256 devices in a mesh: frames: 32 (over z, x), cols: 8 (over y, core).
Axes of the slice: x: 4, y: 4, z: 8, core: 2. Of those that a mesh axis runs over, the one named last changes fastest.
Arguments:
- right_side: float32 [6, 65536], P(None, ('frames', 'cols')), may hold values from -6 to 6
- diag_blocks: float32 [6, 6, 65536], P(None, None, ('frames', 'cols')), may hold values from -0.6 to 24, as said below
- band_blocks: float32 [8, 6, 6, 65536], P(None, None, None, ('frames', 'cols')), may hold values from -0.6 to 0.6
- reach: int32 [65536], P(('frames', 'cols')), may hold values from 1 to 8
- tiles: float32 [32, 8, 8, 384, 384], P('frames', 'cols'), may hold values from -0.09185587 to 0.09185587
- tile_rows: int32 [32, 8, 8], P('frames', 'cols'), may hold values from 0 to 31
- tile_cols: int32 [32, 8, 8], P('frames', 'cols'), may hold values from 0 to 127
- tile_count: int32 [32, 8], P('frames', 'cols'), may hold values from 1 to 8
Outputs:
- solution: float32 [6, 65536], P(None, ('frames', 'cols'))
- residual: float32 [6, 65536], P(None, ('frames', 'cols'))
The draws below stay inside these ranges and needn't reach their ends.
Inputs may be any that keep to these rules, and one draw needn't show every extreme that they name: `diag_blocks`: each block is symmetric, with diagonal entries at least 6 and larger than the sum of its other entries' magnitudes in that row, so each block is positive definite.
All inputs are finite; a program needn't handle non-finite values.
Results may differ from the reference program's by a relative error of at most 0.0003.
Values sent between devices are 32-bit elements; how exact they have to be, the bound alone decides.
No kernel may reach another device: no remote copies, remote signals or barrier semaphores. Data moves between devices by JAX's collectives and lax.ppermute only.
A program may use at most 64 MiB of HBM per device.

```python
import jax
import jax.numpy as jnp
from jax import lax

FR_DEV = 256
BAND = 8
TF = 64
TILES_DEV = 8
ITERS = 4
TILE = 384
KEYFRAMES = 65536
ROW_TILES = 32
COL_TILES = 128
N_FRAMES = 32
N_COLS = 8


def draw_diag_blocks(key, part):
    key_a, key_b = jax.random.split(jax.random.fold_in(key, 11))
    level_diag = jax.random.uniform(key_a, (6, KEYFRAMES), jnp.float32, 6.0, 12.0)
    noise_part = jnp.clip(0.15 * jax.random.normal(key_b, (6, 6, KEYFRAMES), jnp.float32), -0.3, 0.3)
    symmetric = noise_part + jnp.transpose(noise_part, (1, 0, 2))
    identity = jnp.eye(6, dtype=jnp.float32)[:, :, None]
    return symmetric * (1.0 - identity) + identity * level_diag[:, None, :]


def with_ends(values, stream_key, least, largest):
    spot = [jax.random.randint(jax.random.fold_in(stream_key, axis), (), 0, length) for axis, length in enumerate(values.shape)]
    longest = values.shape.index(max(values.shape))
    next_to = spot[:longest] + [(spot[longest] + 1) % values.shape[longest]] + spot[longest + 1:]
    return values.at[tuple(spot)].set(least).at[tuple(next_to)].set(largest)


def block_scale(key, shape, cuts, least, top_value):
    gain = 1.0
    for axis_at, blocks in cuts:
        heights = jax.random.uniform(jax.random.fold_in(jax.random.fold_in(key, 6), axis_at), (blocks,), jnp.float32, least / len(cuts), top_value / len(cuts))
        gain = gain * jnp.repeat(jnp.exp(heights), shape[axis_at] // blocks).reshape((-1,) + (1,) * (len(shape) - 1 - axis_at))
    return gain


def bell_draw(stream_key, shape, width, most, pieces=(), kind=jnp.bfloat16):
    entries = width * jax.random.normal(stream_key, shape, jnp.float32)
    if pieces:
        entries = entries * block_scale(stream_key, shape, pieces, -0.22, 0.18)
    return jnp.clip(entries, -most, most).astype(kind)


def setup_inputs(seed: int = 0) -> dict:
    keys = jax.random.split(jax.random.key(seed), 9)
    right_side = bell_draw(keys[0], (6, KEYFRAMES), 1.0, 6.0, ((1, 256),), jnp.float32)
    diag_blocks = draw_diag_blocks(jax.random.fold_in(keys[8], 71), 0)
    band_blocks = bell_draw(keys[2], (BAND, 6, 6, KEYFRAMES), 0.1, 0.6, ((3, 256),), jnp.float32)
    reach = with_ends(jax.random.randint(keys[3], (KEYFRAMES,), 1, BAND + 1), jax.random.fold_in(keys[3], 1), 1, BAND).astype(jnp.int32)
    tiles = bell_draw(keys[4], (N_FRAMES, N_COLS, TILES_DEV, TILE, TILE), (0.3 / TILE ** 0.5), 0.09185587, ((0, 32), (1, 8)), jnp.float32)
    tile_rows = with_ends(jax.random.randint(keys[5], (N_FRAMES, N_COLS, TILES_DEV), 0, ROW_TILES), jax.random.fold_in(keys[5], 1), 0, ROW_TILES - 1).astype(jnp.int32)
    tile_cols = with_ends(jax.random.randint(keys[6], (N_FRAMES, N_COLS, TILES_DEV), 0, COL_TILES), jax.random.fold_in(keys[6], 1), 0, COL_TILES - 1).astype(jnp.int32)
    tile_count = with_ends(jax.random.randint(keys[7], (N_FRAMES, N_COLS), 1, TILES_DEV + 1), jax.random.fold_in(keys[7], 1), 1, TILES_DEV).astype(jnp.int32)
    return dict(right_side=right_side, diag_blocks=diag_blocks, band_blocks=band_blocks, reach=reach, tiles=tiles, tile_rows=tile_rows, tile_cols=tile_cols, tile_count=tile_count)


def invert_blocks(blocks):
    matrix_rows = [blocks[row_id] for row_id in range(6)]
    inverse = [jnp.zeros_like(blocks[0]).at[row_id].set(1.0) for row_id in range(6)]
    for pivot_id in range(6):
        pivot_value = matrix_rows[pivot_id][pivot_id]
        matrix_rows[pivot_id] = matrix_rows[pivot_id] / pivot_value
        inverse[pivot_id] = inverse[pivot_id] / pivot_value
        for row_id in range(6):
            if row_id != pivot_id:
                factor = matrix_rows[row_id][pivot_id]
                matrix_rows[row_id] = matrix_rows[row_id] - factor * matrix_rows[pivot_id]
                inverse[row_id] = inverse[row_id] - factor * inverse[pivot_id]
    return jnp.stack(inverse)


def precondition(inverse, vector):
    return jnp.einsum("abk,bk->ak", inverse, vector, precision=lax.Precision.HIGHEST)


def band_apply(vector, band_blocks, reach):
    frame_total = vector.shape[1]
    offsets = jnp.arange(1, BAND + 1, dtype=jnp.int32)
    frame_ids = jnp.arange(frame_total, dtype=jnp.int32)
    keep_mask = ((offsets[:, None] <= reach[None, :]) & (frame_ids[None, :] + offsets[:, None] < frame_total)).astype(jnp.float32)
    masked = band_blocks * keep_mask[:, None, None, :]
    padded = jnp.pad(vector, ((0, 0), (0, BAND)))
    result = jnp.zeros_like(vector)
    for offset in range(1, BAND + 1):
        blocks_now = masked[offset - 1]
        result = result + jnp.einsum("abk,bk->ak", blocks_now, padded[:, offset:offset + frame_total], precision=lax.Precision.HIGHEST)
        back_term = jnp.einsum("abk,ak->bk", blocks_now, vector, precision=lax.Precision.HIGHEST)
        result = result.at[:, offset:].add(back_term[:, :frame_total - offset])
    return result


def loop_apply(vector, tiles, tile_rows, tile_cols, tile_count):
    frame_groups, col_groups, slot_total = tile_rows.shape
    total_slots = frame_groups * col_groups * slot_total
    flat_tiles = tiles.reshape(total_slots, TILE, TILE)
    slot_index = jnp.arange(total_slots, dtype=jnp.int32)
    group_id = slot_index // slot_total
    slot_id = slot_index % slot_total
    frame_group = group_id // col_groups
    col_group = group_id % col_groups
    live_flag = (slot_id < tile_count.reshape(-1)[group_id]).astype(jnp.float32)
    row_start = (frame_group * col_groups * FR_DEV + tile_rows.reshape(-1) * TF).astype(jnp.int32)
    col_mid = tile_cols.reshape(-1) * TF
    col_start = (((col_mid // FR_DEV) * col_groups + col_group) * FR_DEV + col_mid % FR_DEV).astype(jnp.int32)

    def one_tile(totals, item):
        tile_now, row_at, col_at, alive_flag = item
        row_part = lax.dynamic_slice_in_dim(vector, row_at, TF, 1).reshape(-1)
        col_part = lax.dynamic_slice_in_dim(vector, col_at, TF, 1).reshape(-1)
        gain_row = (jnp.dot(tile_now, col_part, precision=lax.Precision.HIGHEST) * alive_flag).reshape(6, TF)
        gain_col = (jnp.dot(row_part, tile_now, precision=lax.Precision.HIGHEST) * alive_flag).reshape(6, TF)
        totals = lax.dynamic_update_slice_in_dim(totals, lax.dynamic_slice_in_dim(totals, row_at, TF, 1) + gain_row, row_at, 1)
        totals = lax.dynamic_update_slice_in_dim(totals, lax.dynamic_slice_in_dim(totals, col_at, TF, 1) + gain_col, col_at, 1)
        return totals, None

    result, unused = lax.scan(one_tile, jnp.zeros_like(vector), (flat_tiles, row_start, col_start, live_flag))
    return result


def reference(right_side, diag_blocks, band_blocks, reach, tiles, tile_rows, tile_cols, tile_count):
    inverse = invert_blocks(diag_blocks)

    def apply_system(vector):
        result = jnp.einsum("abk,bk->ak", diag_blocks, vector, precision=lax.Precision.HIGHEST)
        result = result + band_apply(vector, band_blocks, reach)
        return result + loop_apply(vector, tiles, tile_rows, tile_cols, tile_count)

    solution = jnp.zeros_like(right_side)
    residual = right_side
    precond = precondition(inverse, residual)
    direction = precond
    rz_now = jnp.sum(residual * precond)
    for iteration in range(ITERS):
        image_now = apply_system(direction)
        alpha_now = rz_now / jnp.sum(direction * image_now)
        solution = solution + alpha_now * direction
        residual = residual - alpha_now * image_now
        if iteration + 1 < ITERS:
            precond = precondition(inverse, residual)
            rz_next = jnp.sum(residual * precond)
            direction = precond + (rz_next / rz_now) * direction
            rz_now = rz_next
    return solution, residual
```

```python
import jax
import jax.numpy as jnp
from jax import lax
from jax.experimental import pallas as pl
from jax.experimental.pallas import tpu as pltpu
from jax.sharding import PartitionSpec as P


ITERS = 4
BAND = 8
LANES = 128
F32 = jnp.float32
ROWS = ("frames", "cols")


def lane_ids(rows):
    return lax.broadcasted_iota(jnp.int32, (rows, LANES), 1)


def half_turn(x):
    return pltpu.roll(x, 64, 1)


def left(x, by):
    return pltpu.roll(x, (x.shape[1] - by) % x.shape[1], 1) if by % x.shape[1] else x


def right(x, by):
    return pltpu.roll(x, by % x.shape[1], 1) if by % x.shape[1] else x


def store_as_tiles(ref, base, x):
    low = lane_ids(1) < 64
    for u in range(2):
        part = x[:, u * LANES : (u + 1) * LANES]
        turned = half_turn(part)
        for j in range(3):
            lanes = pl.ds(j * LANES, LANES)
            ref[pl.ds(base + 2 * u, 1), lanes] = jnp.where(
                low, part[2 * j : 2 * j + 1], turned[2 * j + 1 : 2 * j + 2]
            )
            ref[pl.ds(base + 2 * u + 1, 1), lanes] = jnp.where(
                low, turned[2 * j : 2 * j + 1], part[2 * j + 1 : 2 * j + 2]
            )


def store_as_natural(ref, t):
    low = lane_ids(1) < 64
    for j in range(3):
        part = t[:, j * LANES : (j + 1) * LANES]
        turned = half_turn(part)
        for u in range(2):
            lanes = pl.ds(u * LANES, LANES)
            ref[pl.ds(2 * j, 1), lanes] = jnp.where(
                low, part[2 * u : 2 * u + 1], turned[2 * u + 1 : 2 * u + 2]
            )
            ref[pl.ds(2 * j + 1, 1), lanes] = jnp.where(
                low, turned[2 * u : 2 * u + 1], part[2 * u + 1 : 2 * u + 2]
            )


def start_kernel(right_ref, diag_ref, band_ref, reach_ref, rows_ref, send_ref, masked_ref, pack):
    reach = reach_ref[...]
    for o in range(BAND):
        keep = (reach > o).astype(F32)
        for a in range(6):
            masked_ref[o * 6 + a] = band_ref[o, a] * keep
    sub = lax.broadcasted_iota(jnp.int32, (6, 256), 0)
    matrix = [diag_ref[a] for a in range(6)]
    inverse = [(sub == a).astype(F32) for a in range(6)]
    for p in range(6):
        pivot = matrix[p][p : p + 1]
        matrix[p] = matrix[p] / pivot
        inverse[p] = inverse[p] / pivot
        for a in range(6):
            if a != p:
                factor = matrix[a][p : p + 1]
                matrix[a] = matrix[a] - factor * matrix[p]
                inverse[a] = inverse[a] - factor * inverse[p]
    residual = right_ref[...]
    first = jnp.concatenate(
        [jnp.sum(inverse[a] * residual, axis=0, keepdims=True) for a in range(6)], axis=0
    )
    store_as_tiles(pack, 0, first)
    store_as_tiles(pack, 4, residual)
    for d in range(4):
        turned = jnp.concatenate(
            [inverse[a][(a + d) % 6 : (a + d) % 6 + 1] for a in range(6)], axis=0
        )
        store_as_tiles(pack, 8 + 4 * d, turned)
    ids = lane_ids(6)
    for j in range(3):
        packed = jnp.zeros((6, LANES), F32)
        for i in range(16):
            block = masked_ref[j * 16 + i, :, LANES : 2 * LANES]
            packed = jnp.where(ids // 8 == i, right(block, i * 8 + 8), packed)
        pack[24:30, j * LANES : (j + 1) * LANES] = packed
    pack[30:32, :] = jnp.zeros((2, 384), F32)
    rows = rows_ref[...]
    pack[30:31, 0:LANES] = ((rows // 4) * 8 + rows % 4).astype(F32)
    whole = pack[...]
    for c in range(8):
        send_ref[c] = whole


def own_edge(edge_ref, row_ref, col):
    last = row_ref[(col + 7) % 8][3:4]
    values = []
    for j in range(3):
        part = last[:, j * LANES : (j + 1) * LANES]
        values += [half_turn(part), part]
    total = jnp.zeros((6, LANES), F32)
    for o in range(BAND):
        z = edge_ref[o * 6] * values[0]
        for a in range(1, 6):
            z = z + edge_ref[o * 6 + a] * values[a]
        total = total + right(z, o + 1)
    total = jnp.where(lane_ids(6) < 8, total, 0.0)
    turned = half_turn(total)
    low = lane_ids(1) < 64
    return jnp.concatenate(
        [jnp.where(low, total[2 * j : 2 * j + 1], turned[2 * j + 1 : 2 * j + 2]) for j in range(3)],
        axis=1,
    )


def send_frames(row_ref, edge_ref, tiles_ref, rows_ref, cols_ref, count_ref, send_ref, edge_out, picked):
    frame = lax.axis_index("frames")
    col = lax.axis_index("cols")
    count = count_ref[0]
    own = row_ref[col]
    sub = lax.broadcasted_iota(jnp.int32, (8, 384), 0)
    chunk = jnp.where(sub < 4, own, 0.0)
    for f in range(32):
        send_ref[f] = chunk
    edge = own_edge(edge_ref, row_ref, col)
    edge_out[...] = jnp.where((sub == 0) & (col > 0), jnp.broadcast_to(edge, (8, 384)), 0.0)
    after = jnp.minimum(frame + 1, 31)
    cross = ((col == 0) & (frame < 31)).astype(F32)
    send_ref[after, 4:5, :] = edge * cross
    picked[...] = jnp.zeros((LANES, 384), F32)
    for s in range(8):
        r = rows_ref[s]
        picked[s : s + 1, :] = row_ref[r // 4, pl.ds(r % 4, 1), :]
    upright = [picked[:, j * LANES : (j + 1) * LANES].T for j in range(3)]
    for s in range(8):
        total = jnp.zeros((1, 384), F32)
        for j in range(3):
            column = upright[j][:, s : s + 1]
            tile = tiles_ref[s, j * LANES : (j + 1) * LANES, :]
            total = total + jnp.sum(tile * column, axis=0, keepdims=True)
        total = total * (s < count).astype(F32)
        q = cols_ref[s]
        send_ref[q // 4, pl.ds(4 + q % 4, 1), :] += total


def first_kernel(
    recv_ref, tiles_ref, rows_ref, cols_ref, count_ref,
    send_ref, edge_out, row_ref, edge_ref, pick_ref, inverse_ref, moment_ref, picked,
):
    col = lax.axis_index("cols")
    sub = lax.broadcasted_iota(jnp.int32, (8, 384), 0)
    moment = jnp.zeros((8, 384), F32)
    for c in range(8):
        both = recv_ref[c, 0:8, :]
        vector = jnp.where(sub < 4, both, 0.0)
        row_ref[c] = vector
        moment = moment + vector * pltpu.roll(both, 4, 0)
        block = [recv_ref[c, 8:16, :], recv_ref[c, 16:24, :]]
        parts = []
        for d in range(4):
            part = block[d // 2]
            part = pltpu.roll(part, 4, 0) if d % 2 else part
            parts.append(jnp.where(sub < 4, part, 0.0))
        parts += [left(parts[2], 256), left(parts[1], 320)]
        for d in range(6):
            inverse_ref[d, c] = parts[d]
    moment_ref[0] = moment[:, 0:128] + moment[:, 128:256] + moment[:, 256:384]
    prev = (col + 7) % 8
    ids = lane_ids(6)
    packed = recv_ref[prev, 24:32, :]
    for j in range(3):
        part = packed[0:6, j * LANES : (j + 1) * LANES]
        for i in range(16):
            edge_ref[j * 16 + i] = jnp.where(ids >= 120, right(part, 120 - i * 8), 0.0)
    lane = lane_ids(1)
    target = jnp.full((1, LANES), -1.0, F32)
    for c in range(8):
        at = lane - 16 * c
        target = jnp.where((at >= 0) & (at < 8), right(recv_ref[c, 30:31, 0:LANES], 16 * c), target)
        target = jnp.where((at >= 8) & (at < 12), (c * 8 + at - 8).astype(F32), target)
        target = jnp.where(at == 12, float(((c + 7) % 8) * 8 + 3), target)
    index = lax.broadcasted_iota(jnp.int32, (64, LANES), 0).astype(F32)
    pick_ref[...] = (index == jnp.broadcast_to(target, (64, LANES))).astype(F32)
    send_frames(row_ref, edge_ref, tiles_ref, rows_ref, cols_ref, count_ref, send_ref, edge_out, picked)


def row_image(recv_ref, pick_ref):
    received = recv_ref[...].reshape(LANES, 384)
    image = jnp.dot(
        pick_ref[...], received, precision=lax.Precision.HIGHEST, preferred_element_type=F32
    )
    return image.reshape(8, 8, 384)


def folded(x):
    x = jnp.sum(x, axis=0)
    return x[:, 0:128] + x[:, 128:256] + x[:, 256:384]


def next_kernel(
    recv_ref, pick_ref, inverse_ref, before_ref, edge_ref, tiles_ref, rows_ref, cols_ref, count_ref,
    send_ref, edge_out, row_ref, image_ref, moment_ref, picked,
):
    col = lax.axis_index("cols")
    image = row_image(recv_ref, pick_ref)
    flat = image.reshape(64, 384)
    vector = inverse_ref[0].reshape(64, 384) * flat
    for d in range(1, 6):
        vector = vector + inverse_ref[d].reshape(64, 384) * left(flat, 64 * d)
    vector = vector.reshape(8, 8, 384)
    row_ref[...] = vector
    moment_ref[0] = folded(before_ref[...] * image)
    moment_ref[1] = folded(vector * image)
    picked[0:64, :] = flat
    image_ref[...] = picked[pl.ds(pl.multiple_of(col * 8, 8), 8), :]
    send_frames(row_ref, edge_ref, tiles_ref, rows_ref, cols_ref, count_ref, send_ref, edge_out, picked)


def band_kernel(row_ref, masked_ref, edge_in, out_ref, natural, sums):
    col = lax.axis_index("cols")
    store_as_natural(natural, row_ref[col])
    lane = lax.broadcasted_iota(jnp.int32, (6, 256), 1)
    vector = natural[0:6, :]
    total = jnp.zeros((6, 256), F32)
    ahead = [jnp.zeros((6, 256), F32) for _ in range(6)]
    for o in range(BAND):
        shifted = jnp.where(lane < 255 - o, left(vector, o + 1), 0.0)
        z = jnp.zeros((6, 256), F32)
        for a in range(6):
            block = masked_ref[o * 6 + a]
            z = z + block * natural[a : a + 1, :]
            ahead[a] = ahead[a] + block * shifted
        total = total + jnp.where(lane > o, right(z, o + 1), 0.0)
    for a in range(6):
        sums[a : a + 1, :] = jnp.sum(ahead[a], axis=0, keepdims=True)
    out_ref[...] = jnp.zeros((8, 384), F32)
    store_as_tiles(out_ref, 0, total + sums[0:6, :])
    out_ref[0:1, :] = out_ref[0:1, :] + edge_in[0:1, :]


def cols_kernel(recv_ref, tiles_ref, row_ref, edge_ref, band_in, cols_ref, count_ref, send_ref, pack):
    frame = lax.axis_index("frames")
    col = lax.axis_index("cols")
    count = count_ref[0]
    total = recv_ref[0]
    for f in range(1, 32):
        total = total + recv_ref[f]
    sub = lax.broadcasted_iota(jnp.int32, (8, 384), 0)
    pack[8:16, :] = jnp.where(sub < 4, pltpu.roll(total, 4, 0) + band_in[...], 0.0)
    after = jnp.minimum(frame + 1, 31)
    here = (col > 0).astype(F32)
    there = ((col == 0) & (frame < 31)).astype(F32)
    start = row_ref[col][0:1] * here + recv_ref[after][0:1] * there
    parts = []
    for j in range(3):
        part = start[:, j * LANES : (j + 1) * LANES]
        parts += [part, half_turn(part)]
    ids = lane_ids(6)
    begin = jnp.concatenate(parts, axis=0)
    sums = [jnp.zeros((6, LANES), F32) for _ in range(6)]
    for o in range(BAND):
        shifted = jnp.where(ids >= 127 - o, left(begin, o + 1), 0.0)
        for a in range(6):
            sums[a] = sums[a] + edge_ref[o * 6 + a] * shifted
    sums = [jnp.sum(x, axis=0, keepdims=True) for x in sums]
    low = lane_ids(1) < 64
    for j in range(3):
        pack[12:13, j * LANES : (j + 1) * LANES] = jnp.where(
            low, half_turn(sums[2 * j]), sums[2 * j + 1]
        )
    for s in range(8):
        q = cols_ref[s]
        piece = recv_ref[q // 4, pl.ds(q % 4, 1), :] * (s < count).astype(F32)
        for j in range(3):
            rows = pl.ds(j * LANES, LANES)
            part = tiles_ref[s, rows, 0:LANES] * piece[:, 0:LANES]
            part = part + tiles_ref[s, rows, LANES : 2 * LANES] * piece[:, LANES : 2 * LANES]
            part = part + tiles_ref[s, rows, 2 * LANES : 384] * piece[:, 2 * LANES : 384]
            pack[s : s + 1, j * LANES : (j + 1) * LANES] = jnp.sum(part.T, axis=0, keepdims=True)
    whole = pack[...]
    for c in range(8):
        send_ref[c] = whole


def moments_kernel(recv_ref, pick_ref, before_ref, m0_ref, m1_ref, m2_ref, m3_ref, send_ref, image_ref, scratch):
    col = lax.axis_index("cols")
    image = row_image(recv_ref, pick_ref)
    scratch[...] = image.reshape(64, 384)
    image_ref[...] = scratch[pl.ds(pl.multiple_of(col * 8, 8), 8), :]
    parts = [m0_ref[0]]
    for ref in (m1_ref, m2_ref, m3_ref):
        parts += [ref[0], ref[1]]
    parts.append(folded(before_ref[...] * image))
    whole = jnp.concatenate([jnp.sum(x, axis=0, keepdims=True) for x in parts], axis=0)
    for f in range(32):
        send_ref[f] = whole


def end_kernel(recv_ref, right_ref, v0, v1, v2, v3, w0, w1, w2, w3, solution_ref, residual_ref, scratch):
    col = lax.axis_index("cols")
    total = recv_ref[0]
    for f in range(1, 32):
        total = total + recv_ref[f]
    sums = jnp.sum(total, axis=1, keepdims=True)
    mu = [jnp.broadcast_to(sums[i : i + 1], (1, LANES)) for i in range(8)]
    zero = jnp.zeros((1, LANES), F32)
    one = zero + 1.0

    def form(left_side, shift):
        value = zero
        for i in range(len(left_side)):
            for k in range(i, len(left_side)):
                term = left_side[i] * left_side[k]
                value = value + (term if i == k else term + term) * mu[i + k + shift]
        return value

    def ratio(top, bottom):
        return jnp.where(top == 0.0, 0.0, top / jnp.where(top == 0.0, one, bottom))

    direction, residual, solution = [one], [one], []
    gamma = mu[0]
    for it in range(ITERS):
        alpha = ratio(gamma, form(direction, 0) + form(direction, 1))
        solution = solution + [zero] * (len(direction) - len(solution))
        solution = [x + alpha * p for x, p in zip(solution, direction)]
        image = [p + q for p, q in zip(direction + [zero], [zero] + direction)]
        residual = residual + [zero] * (len(image) - len(residual))
        residual = [r - alpha * y for r, y in zip(residual, image)]
        if it + 1 < ITERS:
            fresh = form(residual, 0)
            beta = ratio(fresh, gamma)
            direction = direction + [zero] * (len(residual) - len(direction))
            direction = [r + beta * p for r, p in zip(residual, direction)]
            gamma = fresh

    def wide(x):
        return jnp.concatenate([x, x, x], axis=1)

    total = wide(solution[0]) * v0[col]
    for x, ref in zip(solution[1:], (v1, v2, v3)):
        total = total + wide(x) * ref[col]
    store_as_natural(solution_ref, total)
    total = wide(residual[1]) * w0[...]
    for x, ref in zip(residual[2:], (w1, w2, w3)):
        total = total + wide(x) * ref[...]
    store_as_natural(scratch, total)
    residual_ref[...] = scratch[0:6, :] + jnp.concatenate([residual[0]] * 2, axis=1) * right_ref[...]


VM = pl.BlockSpec(memory_space=pltpu.VMEM)
SM = pl.BlockSpec(memory_space=pltpu.SMEM)


def shape(*dims):
    return jax.ShapeDtypeStruct(dims, F32)


def call(kernel, specs, outs, scratch, name):
    return pl.pallas_call(
        kernel,
        in_specs=specs,
        out_specs=[VM] * len(outs),
        out_shape=outs,
        scratch_shapes=[pltpu.VMEM(s, F32) for s in scratch],
        compiler_params=pltpu.CompilerParams(vmem_limit_bytes=24 * 1024 * 1024),
        name=name,
    )


def per_device(right_side, diag_blocks, band_blocks, reach, tiles, tile_rows, tile_cols, tile_count):
    local = tiles.reshape(tiles.shape[2:])
    row_ids = tile_rows.reshape(-1)
    col_ids = tile_cols.reshape(-1)
    count = tile_count.reshape(-1)
    rows_wide = jnp.pad(row_ids, (0, LANES - 8)).reshape(1, LANES)

    def exchange(x, axis):
        return lax.all_to_all(x, axis, 0, 0, tiled=True)

    send, masked = call(
        start_kernel, [VM] * 5, [shape(8, 32, 384), shape(48, 6, 256)], [(32, 384)], "start"
    )(right_side, diag_blocks, band_blocks, reach.reshape(1, -1), rows_wide)
    recv = exchange(send, "cols")
    frames_out = [shape(32, 8, 384), shape(8, 384), shape(8, 8, 384)]
    send, edge, row, edges, pick, inverse, moment = call(
        first_kernel,
        [VM, VM, SM, SM, SM],
        frames_out + [shape(48, 6, LANES), shape(64, LANES), shape(6, 8, 8, 384), shape(1, 8, LANES)],
        [(LANES, 384)],
        "first",
    )(recv, local, row_ids, col_ids, count)
    vectors, images, moments = [row], [], [moment]
    for it in range(ITERS):
        recv = exchange(send, "frames")
        (band,) = call(band_kernel, [VM] * 3, [shape(8, 384)], [(8, 256), (8, 256)], "band")(
            row, masked, edge
        )
        (send,) = call(
            cols_kernel, [VM] * 5 + [SM] * 2, [shape(8, 16, 384)], [(16, 384)], "products"
        )(recv, local, row, edges, band, col_ids, count)
        recv = exchange(send, "cols")
        if it + 1 < ITERS:
            send, edge, row, image, moment = call(
                next_kernel,
                [VM] * 6 + [SM] * 3,
                frames_out + [shape(8, 384), shape(2, 8, LANES)],
                [(LANES, 384)],
                "next",
            )(recv, pick, inverse, row, edges, local, row_ids, col_ids, count)
            vectors.append(row)
            images.append(image)
            moments.append(moment)
    send, image = call(
        moments_kernel, [VM] * 7, [shape(32, 8, LANES), shape(8, 384)], [(64, 384)], "moments"
    )(recv, pick, row, *moments)
    images.append(image)
    recv = exchange(send, "frames")
    return tuple(
        call(end_kernel, [VM] * 10, [shape(6, 256), shape(6, 256)], [(8, 256)], "end")(
            recv, right_side, *vectors, *images
        )
    )


def solution(mesh):
    return jax.shard_map(
        per_device,
        mesh=mesh,
        in_specs=(
            P(None, ROWS),
            P(None, None, ROWS),
            P(None, None, None, ROWS),
            P(ROWS),
            P("frames", "cols", None, None, None),
            P("frames", "cols", None),
            P("frames", "cols", None),
            P("frames", "cols"),
        ),
        out_specs=(P(None, ROWS), P(None, ROWS)),
        check_vma=False,
    )
```

```python
import jax
import jax.numpy as jnp
from jax import lax
from jax.experimental import pallas as pl
from jax.experimental.pallas import tpu as pltpu
from jax.sharding import PartitionSpec as P


ITERS = 4
BAND = 8
LANES = 128
F32 = jnp.float32
ROWS = ("frames", "cols")


def lane_ids(rows):
    return lax.broadcasted_iota(jnp.int32, (rows, LANES), 1)


def half_turn(x):
    return pltpu.roll(x, 64, 1)


def left(x, by):
    return pltpu.roll(x, (x.shape[1] - by) % x.shape[1], 1) if by % x.shape[1] else x


def right(x, by):
    return pltpu.roll(x, by % x.shape[1], 1) if by % x.shape[1] else x


def store_as_tiles(ref, base, x):
    low = lane_ids(1) < 64
    for u in range(2):
        part = x[:, u * LANES : (u + 1) * LANES]
        turned = half_turn(part)
        for j in range(3):
            lanes = pl.ds(j * LANES, LANES)
            ref[pl.ds(base + 2 * u, 1), lanes] = jnp.where(
                low, part[2 * j : 2 * j + 1], turned[2 * j + 1 : 2 * j + 2]
            )
            ref[pl.ds(base + 2 * u + 1, 1), lanes] = jnp.where(
                low, turned[2 * j : 2 * j + 1], part[2 * j + 1 : 2 * j + 2]
            )


def store_as_natural(ref, t):
    low = lane_ids(1) < 64
    for j in range(3):
        part = t[:, j * LANES : (j + 1) * LANES]
        turned = half_turn(part)
        for u in range(2):
            lanes = pl.ds(u * LANES, LANES)
            ref[pl.ds(2 * j, 1), lanes] = jnp.where(
                low, part[2 * u : 2 * u + 1], turned[2 * u + 1 : 2 * u + 2]
            )
            ref[pl.ds(2 * j + 1, 1), lanes] = jnp.where(
                low, turned[2 * u : 2 * u + 1], part[2 * u + 1 : 2 * u + 2]
            )


def start_kernel(
    right_hbm, diag_hbm, band_hbm, reach_hbm, rows_hbm, cols_hbm, tiles_hbm,
    send_ref, masked_ref, rows_ref, cols_ref, tiles_ref,
    right_ref, diag_ref, band_ref, reach_ref, pack, *sems,
):
    copies = [
        pltpu.make_async_copy(source, to, sem)
        for source, to, sem in zip(
            (diag_hbm, right_hbm, reach_hbm, band_hbm, rows_hbm, cols_hbm),
            (diag_ref, right_ref, reach_ref, band_ref, rows_ref, cols_ref),
            sems,
        )
    ]
    copies += [
        pltpu.make_async_copy(tiles_hbm.at[s], tiles_ref.at[s], sems[6 + s]) for s in range(4)
    ]
    for copy in copies:
        copy.start()
    for copy in copies[:2]:
        copy.wait()
    sub = lax.broadcasted_iota(jnp.int32, (6, 256), 0)
    matrix = [diag_ref[a] for a in range(6)]
    inverse = [(sub == a).astype(F32) for a in range(6)]
    for p in range(6):
        pivot = matrix[p][p : p + 1]
        matrix[p] = matrix[p] / pivot
        inverse[p] = inverse[p] / pivot
        for a in range(6):
            if a != p:
                factor = matrix[a][p : p + 1]
                matrix[a] = matrix[a] - factor * matrix[p]
                inverse[a] = inverse[a] - factor * inverse[p]
    residual = right_ref[...]
    first = jnp.concatenate(
        [jnp.sum(inverse[a] * residual, axis=0, keepdims=True) for a in range(6)], axis=0
    )
    store_as_tiles(pack, 0, first)
    store_as_tiles(pack, 4, residual)
    for d in range(4):
        turned = jnp.concatenate(
            [inverse[a][(a + d) % 6 : (a + d) % 6 + 1] for a in range(6)], axis=0
        )
        store_as_tiles(pack, 8 + 4 * d, turned)
    for copy in copies[2:6]:
        copy.wait()
    reach = reach_ref[...]
    for o in range(BAND):
        keep = (reach > o).astype(F32)
        for a in range(6):
            masked_ref[o * 6 + a] = band_ref[a, :, o, :] * keep
    ids = lane_ids(6)
    for j in range(3):
        packed = jnp.zeros((6, LANES), F32)
        for i in range(16):
            block = masked_ref[j * 16 + i, :, LANES : 2 * LANES]
            packed = jnp.where(ids // 8 == i, right(block, i * 8 + 8), packed)
        pack[24:30, j * LANES : (j + 1) * LANES] = packed
    pack[30:32, :] = jnp.zeros((2, 384), F32)
    rows = rows_ref[...]
    pack[30:31, 0:8] = ((rows // 4) * 8 + rows % 4).astype(F32)
    whole = pack[...]
    for c in range(8):
        send_ref[c] = whole
    for copy in copies[6:]:
        copy.wait()


def own_edge(edge_ref, row_ref, col):
    last = row_ref[(col + 7) % 8][3:4]
    values = []
    for j in range(3):
        part = last[:, j * LANES : (j + 1) * LANES]
        values += [half_turn(part), part]
    total = jnp.zeros((6, LANES), F32)
    for o in range(BAND):
        z = edge_ref[o * 6] * values[0]
        for a in range(1, 6):
            z = z + edge_ref[o * 6 + a] * values[a]
        total = total + right(z, o + 1)
    total = jnp.where(lane_ids(6) < 8, total, 0.0)
    turned = half_turn(total)
    low = lane_ids(1) < 64
    return jnp.concatenate(
        [jnp.where(low, total[2 * j : 2 * j + 1], turned[2 * j + 1 : 2 * j + 2]) for j in range(3)],
        axis=1,
    )


def transposed_products(row_ref, tiles_refs, ids_refs, picked):
    rows_ref, _, count_ref = ids_refs
    count = count_ref[0, 0]
    picked[...] = jnp.zeros((LANES, 384), F32)
    for s in range(8):
        r = rows_ref[0, s]
        picked[s : s + 1, :] = row_ref[r // 4, pl.ds(r % 4, 1), :]
    upright = [picked[:, j * LANES : (j + 1) * LANES].T for j in range(3)]
    products = []
    for s in range(8):
        total = jnp.zeros((1, 384), F32)
        for j in range(3):
            column = upright[j][:, s : s + 1]
            tile = tiles_refs[s // 4][s % 4, j * LANES : (j + 1) * LANES, :]
            total = total + jnp.sum(tile * column, axis=0, keepdims=True)
        products.append(total * (s < count).astype(F32))
    return products


def edge_terms(row_ref, edge_ref):
    frame = lax.axis_index("frames")
    col = lax.axis_index("cols")
    edge = own_edge(edge_ref, row_ref, col)
    cross = ((col == 0) & (frame < 31)).astype(F32)
    return edge * (col > 0).astype(F32), edge * cross


def band_terms(row_ref, masked_ref, edge, out_ref, natural, sums):
    col = lax.axis_index("cols")
    store_as_natural(natural, row_ref[col])
    lane = lax.broadcasted_iota(jnp.int32, (6, 256), 1)
    vector = natural[0:6, :]
    total = jnp.zeros((6, 256), F32)
    ahead = [jnp.zeros((6, 256), F32) for _ in range(6)]
    for o in range(BAND):
        shifted = jnp.where(lane < 255 - o, left(vector, o + 1), 0.0)
        z = jnp.zeros((6, 256), F32)
        for a in range(6):
            block = masked_ref[o * 6 + a]
            z = z + block * natural[a : a + 1, :]
            ahead[a] = ahead[a] + block * shifted
        total = total + jnp.where(lane > o, right(z, o + 1), 0.0)
    for a in range(6):
        sums[a : a + 1, :] = jnp.sum(ahead[a], axis=0, keepdims=True)
    out_ref[...] = jnp.zeros((8, 384), F32)
    store_as_tiles(out_ref, 0, total + sums[0:6, :])
    out_ref[0:1, :] = out_ref[0:1, :] + edge


def send_frames(row_ref, edge_ref, masked_ref, tiles_refs, ids_refs, send_ref, band_ref, scratch, copies=()):
    picked, natural, sums = scratch
    col = lax.axis_index("cols")
    sub = lax.broadcasted_iota(jnp.int32, (8, 384), 0)
    chunk = jnp.where(sub < 4, row_ref[col], 0.0)
    for f in range(32):
        send_ref[f] = chunk
    mine, onward = edge_terms(row_ref, edge_ref)
    send_ref[jnp.minimum(lax.axis_index("frames") + 1, 31), 4:5, :] = onward
    band_terms(row_ref, masked_ref, mine, band_ref, natural, sums)
    for copy in copies:
        copy.wait()
    for s, product in enumerate(transposed_products(row_ref, tiles_refs, ids_refs, picked)):
        q = ids_refs[1][0, s]
        send_ref[q // 4, pl.ds(4 + q % 4, 1), :] += product


def send_last(row_ref, edge_ref, masked_ref, tiles_refs, ids_refs, known, send_ref, band_ref, scratch):
    picked, natural, sums, pack = scratch
    col = lax.axis_index("cols")
    mine, onward = edge_terms(row_ref, edge_ref)
    band_terms(row_ref, masked_ref, mine, band_ref, natural, sums)
    own = row_ref[col]
    products = transposed_products(row_ref, tiles_refs, ids_refs, picked)
    for j in range(3):
        lanes = slice(j * LANES, (j + 1) * LANES)
        for s in range(8):
            pack[8 * j + s : 8 * j + s + 1, :] = products[s][:, lanes]
        pack[24 + 4 * j : 28 + 4 * j, :] = own[0:4, lanes]
        pack[36 + j : 37 + j, :] = onward[:, lanes]
    part = own * band_ref[...]
    quad = jnp.sum(part[:, 0:128] + part[:, 128:256] + part[:, 256:384], axis=0, keepdims=True)
    part = own[0:1] * mine
    quad = quad + part[:, 0:128] + part[:, 128:256] + part[:, 256:384]
    rows = [jnp.sum(x, axis=0, keepdims=True) for x in known] + [quad]
    lane = lax.broadcasted_iota(jnp.int32, (8, LANES), 1)
    sub = lax.broadcasted_iota(jnp.int32, (8, LANES), 0)
    totals = jnp.sum(jnp.concatenate(rows, axis=0), axis=1, keepdims=True)
    misc = jnp.sum(jnp.where(lane == sub + 8, totals, 0.0), axis=0, keepdims=True)
    for s in range(8):
        misc = jnp.where(lane_ids(1) == s, ids_refs[1][0, s].astype(F32), misc)
    pack[39:40, :] = misc
    whole = pack[...]
    for f in range(32):
        send_ref[f] = whole


def first_kernel(
    recv_ref, masked_ref, tiles_hbm, early_ref, rows_ref, cols_ref, count_ref,
    send_ref, band_ref, row_ref, edge_ref, pick_ref, inverse_ref, moment_ref, late_ref,
    picked, natural, sums, *sems,
):
    copies = [
        pltpu.make_async_copy(tiles_hbm.at[4 + s], late_ref.at[s], sems[s]) for s in range(4)
    ]
    for copy in copies:
        copy.start()
    col = lax.axis_index("cols")
    sub = lax.broadcasted_iota(jnp.int32, (8, 384), 0)
    moment = jnp.zeros((8, 384), F32)
    for c in range(8):
        both = recv_ref[c, 0:8, :]
        vector = jnp.where(sub < 4, both, 0.0)
        row_ref[c] = vector
        moment = moment + vector * pltpu.roll(both, 4, 0)
        block = [recv_ref[c, 8:16, :], recv_ref[c, 16:24, :]]
        parts = []
        for d in range(4):
            part = block[d // 2]
            part = pltpu.roll(part, 4, 0) if d % 2 else part
            parts.append(jnp.where(sub < 4, part, 0.0))
        parts += [left(parts[2], 256), left(parts[1], 320)]
        for d in range(6):
            inverse_ref[d, c] = parts[d]
    moment_ref[0] = moment[:, 0:128] + moment[:, 128:256] + moment[:, 256:384]
    prev = (col + 7) % 8
    ids = lane_ids(6)
    packed = recv_ref[prev, 24:32, :]
    for j in range(3):
        part = packed[0:6, j * LANES : (j + 1) * LANES]
        for i in range(16):
            edge_ref[j * 16 + i] = jnp.where(ids >= 120, right(part, 120 - i * 8), 0.0)
    lane = lane_ids(1)
    target = jnp.full((1, LANES), -1.0, F32)
    for c in range(8):
        at = lane - 16 * c
        target = jnp.where((at >= 0) & (at < 8), right(recv_ref[c, 30:31, 0:LANES], 16 * c), target)
        target = jnp.where((at >= 8) & (at < 12), (c * 8 + at - 8).astype(F32), target)
        target = jnp.where(at == 12, float(((c + 7) % 8) * 8 + 3), target)
    index = lax.broadcasted_iota(jnp.int32, (64, LANES), 0).astype(F32)
    pick_ref[...] = (index == jnp.broadcast_to(target, (64, LANES))).astype(F32)
    ids_refs = (rows_ref, cols_ref, count_ref)
    scratch = (picked, natural, sums)
    tiles_refs = (early_ref, late_ref)
    send_frames(
        row_ref, edge_ref, masked_ref, tiles_refs, ids_refs, send_ref, band_ref, scratch, copies
    )


def row_image(recv_ref, pick_ref):
    received = recv_ref[...].reshape(LANES, 384)
    image = jnp.dot(
        pick_ref[...], received, precision=lax.Precision.HIGHEST, preferred_element_type=F32
    )
    return image.reshape(8, 8, 384)


def folded(x):
    x = jnp.sum(x, axis=0)
    return x[:, 0:128] + x[:, 128:256] + x[:, 256:384]


def advance(recv_ref, pick_ref, inverse_ref, before_ref, row_ref, image_ref, moment_ref, picked):
    col = lax.axis_index("cols")
    image = row_image(recv_ref, pick_ref)
    flat = image.reshape(64, 384)
    vector = inverse_ref[0].reshape(64, 384) * flat
    for d in range(1, 6):
        vector = vector + inverse_ref[d].reshape(64, 384) * left(flat, 64 * d)
    vector = vector.reshape(8, 8, 384)
    row_ref[...] = vector
    moments = [folded(before_ref[...] * image), folded(vector * image)]
    if moment_ref is not None:
        moment_ref[0], moment_ref[1] = moments
    picked[0:64, :] = flat
    image_ref[...] = picked[pl.ds(pl.multiple_of(col * 8, 8), 8), :]
    return moments


def next_kernel(
    recv_ref, pick_ref, inverse_ref, before_ref, edge_ref, masked_ref, early_ref, late_ref, rows_ref, cols_ref, count_ref,
    send_ref, band_ref, row_ref, image_ref, moment_ref, *scratch,
):
    advance(recv_ref, pick_ref, inverse_ref, before_ref, row_ref, image_ref, moment_ref, scratch[0])
    ids_refs = (rows_ref, cols_ref, count_ref)
    tiles_refs = (early_ref, late_ref)
    send_frames(row_ref, edge_ref, masked_ref, tiles_refs, ids_refs, send_ref, band_ref, scratch)


def last_kernel(
    recv_ref, pick_ref, inverse_ref, before_ref, edge_ref, masked_ref, early_ref, late_ref, rows_ref, cols_ref, count_ref,
    m0_ref, m1_ref, m2_ref, send_ref, band_ref, row_ref, image_ref, *scratch,
):
    moments = advance(recv_ref, pick_ref, inverse_ref, before_ref, row_ref, image_ref, None, scratch[0])
    known = [m0_ref[0], m1_ref[0], m1_ref[1], m2_ref[0], m2_ref[1]] + moments
    ids_refs = (rows_ref, cols_ref, count_ref)
    tiles_refs = (early_ref, late_ref)
    send_last(row_ref, edge_ref, masked_ref, tiles_refs, ids_refs, known, send_ref, band_ref, scratch)


def onward_terms(edge_ref, start):
    parts = []
    for j in range(3):
        part = start[:, j * LANES : (j + 1) * LANES]
        parts += [part, half_turn(part)]
    ids = lane_ids(6)
    begin = jnp.concatenate(parts, axis=0)
    sums = [jnp.zeros((6, LANES), F32) for _ in range(6)]
    for o in range(BAND):
        shifted = jnp.where(ids >= 127 - o, left(begin, o + 1), 0.0)
        for a in range(6):
            sums[a] = sums[a] + edge_ref[o * 6 + a] * shifted
    sums = [jnp.sum(x, axis=0, keepdims=True) for x in sums]
    low = lane_ids(1) < 64
    return jnp.concatenate(
        [jnp.where(low, half_turn(sums[2 * j]), sums[2 * j + 1]) for j in range(3)], axis=1
    )


def tile_products(tiles_refs, piece_of, count, pack):
    for s in range(8):
        piece = piece_of(s) * (s < count).astype(F32)
        for j in range(3):
            rows = pl.ds(j * LANES, LANES)
            tile = tiles_refs[s // 4]
            part = tile[s % 4, rows, 0:LANES] * piece[:, 0:LANES]
            part = part + tile[s % 4, rows, LANES : 2 * LANES] * piece[:, LANES : 2 * LANES]
            part = part + tile[s % 4, rows, 2 * LANES : 384] * piece[:, 2 * LANES : 384]
            pack[s : s + 1, j * LANES : (j + 1) * LANES] = jnp.sum(part.T, axis=0, keepdims=True)


def cols_kernel(recv_ref, early_ref, late_ref, row_ref, edge_ref, band_ref, cols_ref, count_ref, send_ref, pack):
    frame = lax.axis_index("frames")
    col = lax.axis_index("cols")
    total = recv_ref[0]
    for f in range(1, 32):
        total = total + recv_ref[f]
    sub = lax.broadcasted_iota(jnp.int32, (8, 384), 0)
    pack[8:16, :] = jnp.where(sub < 4, pltpu.roll(total, 4, 0) + band_ref[...], 0.0)
    here = (col > 0).astype(F32)
    there = ((col == 0) & (frame < 31)).astype(F32)
    start = row_ref[col][0:1] * here + recv_ref[jnp.minimum(frame + 1, 31)][0:1] * there
    pack[12:13, :] = onward_terms(edge_ref, start)

    def piece_of(s):
        q = cols_ref[0, s]
        return recv_ref[q // 4, pl.ds(q % 4, 1), :]

    tile_products((early_ref, late_ref), piece_of, count_ref[0, 0], pack)
    whole = pack[...]
    for c in range(8):
        send_ref[c] = whole


def finish_kernel(
    recv_ref, early_ref, late_ref, row_ref, edge_ref, band_ref, cols_ref, count_ref, send_ref, known_ref, pack
):
    frame = lax.axis_index("frames")
    col = lax.axis_index("cols")
    lane = lane_ids(1)
    misc = [recv_ref[f, 39:40, :] for f in range(32)]
    total = misc[0]
    for x in misc[1:]:
        total = total + x
    known_ref[...] = jnp.broadcast_to(total, (8, LANES))
    halves = []
    for h in range(2):
        tags = jnp.zeros((1, LANES), F32)
        for i in range(16):
            tags = jnp.where(lane // 8 == i, right(misc[16 * h + i], 8 * i), tags)
        halves.append(tags)
    tags = jnp.concatenate(halves, axis=1)
    products = jnp.concatenate(
        [recv_ref[:, 8 * j : 8 * j + 8, :].reshape(256, LANES) for j in range(3)], axis=1
    )

    def dot(a, b):
        return jnp.dot(a, b, precision=lax.Precision.HIGHEST, preferred_element_type=F32)

    at = lax.broadcasted_iota(jnp.int32, (256, 256), 0)
    wanted = ((at // 8) * 4 + at % 4).astype(F32)
    sums = dot((wanted == jnp.broadcast_to(tags, (256, 256))).astype(F32), products)
    low = lax.broadcasted_iota(jnp.int32, (8, LANES), 0) < 4
    quad = jnp.zeros((8, LANES), F32)
    for f in range(32):
        here = sums[8 * f : 8 * f + 8]
        quad = quad + jnp.where(low, here[:, 0:128], here[:, 128:256]) * recv_ref[f, 24:32, :]
        quad = quad + jnp.where(low, here[:, 256:384] * recv_ref[f, 32:40, :], 0.0)
    quad = jnp.sum(quad, axis=0, keepdims=True)
    for f in range(31):
        for j in range(3):
            quad = quad + recv_ref[f, 36 + j : 37 + j, :] * recv_ref[f + 1, 24 + 4 * j : 25 + 4 * j, :]
    quad = quad + quad + jnp.where(lane == 15, total, 0.0)

    sub = lax.broadcasted_iota(jnp.int32, (8, 256), 0)
    mine = dot((jnp.broadcast_to(tags, (8, 256)) == (4 * frame + sub % 4).astype(F32)).astype(F32), products)
    sub = lax.broadcasted_iota(jnp.int32, (8, 384), 0)
    pack[8:16, :] = jnp.where(sub < 4, mine + band_ref[...], 0.0)
    before = jnp.maximum(frame - 1, 0)
    for j in range(3):
        lanes = slice(j * LANES, (j + 1) * LANES)
        edge = recv_ref[before, 36 + j : 37 + j, :] * (frame > 0).astype(F32)
        pack[8:9, lanes] = pack[8:9, lanes] + edge
    here = (col > 0).astype(F32)
    there = ((col == 0) & (frame < 31)).astype(F32)
    after = jnp.minimum(frame + 1, 31)

    def row_of(f, i):
        return jnp.concatenate([recv_ref[f, pl.ds(24 + 4 * j + i, 1), :] for j in range(3)], axis=1)

    pack[12:13, :] = onward_terms(edge_ref, row_ref[col][0:1] * here + row_of(after, 0) * there)
    pack[13:14, 0:LANES] = quad

    def piece_of(s):
        q = cols_ref[0, s]
        return row_of(q // 4, q % 4)

    tile_products((early_ref, late_ref), piece_of, count_ref[0, 0], pack)
    whole = pack[...]
    for c in range(8):
        send_ref[c] = whole


def end_kernel(
    recv_ref, pick_ref, known_ref, right_ref, v0, v1, v2, v3, w0, w1, w2, solution_ref, residual_ref, scratch
):
    col = lax.axis_index("cols")
    last = jnp.dot(
        pick_ref[pl.ds(pl.multiple_of(col * 8, 8), 8), :],
        recv_ref[...].reshape(LANES, 384),
        precision=lax.Precision.HIGHEST,
        preferred_element_type=F32,
    )
    total = recv_ref[0, 13:14, 0:LANES]
    for c in range(1, 8):
        total = total + recv_ref[c, 13:14, 0:LANES]
    known = known_ref[0:1, :]
    mu = [jnp.broadcast_to(known[:, 8 + i : 9 + i], (1, LANES)) for i in range(7)]
    mu.append(jnp.broadcast_to(jnp.sum(total, axis=1, keepdims=True), (1, LANES)))
    zero = jnp.zeros((1, LANES), F32)
    one = zero + 1.0

    def form(left_side, shift):
        value = zero
        for i in range(len(left_side)):
            for k in range(i, len(left_side)):
                term = left_side[i] * left_side[k]
                value = value + (term if i == k else term + term) * mu[i + k + shift]
        return value

    def ratio(top, bottom):
        return jnp.where(top == 0.0, 0.0, top / jnp.where(top == 0.0, one, bottom))

    direction, residual, solution = [one], [one], []
    gamma = mu[0]
    for it in range(ITERS):
        alpha = ratio(gamma, form(direction, 0) + form(direction, 1))
        solution = solution + [zero] * (len(direction) - len(solution))
        solution = [x + alpha * p for x, p in zip(solution, direction)]
        image = [p + q for p, q in zip(direction + [zero], [zero] + direction)]
        residual = residual + [zero] * (len(image) - len(residual))
        residual = [r - alpha * y for r, y in zip(residual, image)]
        if it + 1 < ITERS:
            fresh = form(residual, 0)
            beta = ratio(fresh, gamma)
            direction = direction + [zero] * (len(residual) - len(direction))
            direction = [r + beta * p for r, p in zip(residual, direction)]
            gamma = fresh

    def wide(x):
        return jnp.concatenate([x, x, x], axis=1)

    total = wide(solution[0]) * v0[col]
    for x, ref in zip(solution[1:], (v1, v2, v3)):
        total = total + wide(x) * ref[col]
    store_as_natural(solution_ref, total)
    total = wide(residual[4]) * last
    for x, ref in zip(residual[1:4], (w0, w1, w2)):
        total = total + wide(x) * ref[...]
    store_as_natural(scratch, total)
    residual_ref[...] = scratch[0:6, :] + jnp.concatenate([residual[0]] * 2, axis=1) * right_ref[...]


VM = pl.BlockSpec(memory_space=pltpu.VMEM)
SM = pl.BlockSpec(memory_space=pltpu.SMEM)
HB = pl.BlockSpec(memory_space=pltpu.HBM)


def shape(*dims, kind=F32):
    return jax.ShapeDtypeStruct(dims, kind)


def call(kernel, specs, outs, scratch, name):
    return pl.pallas_call(
        kernel,
        in_specs=specs,
        out_specs=[VM] * len(outs),
        out_shape=outs,
        scratch_shapes=[pltpu.VMEM(s, F32) if isinstance(s, tuple) else s for s in scratch],
        compiler_params=pltpu.CompilerParams(vmem_limit_bytes=24 * 1024 * 1024),
        name=name,
    )


def per_device(right_side, diag_blocks, band_blocks, reach, tiles, tile_rows, tile_cols, tile_count):
    def exchange(x, axis):
        return lax.all_to_all(x, axis, 0, 0, tiled=True)

    def in_hbm(x):
        return pltpu.with_memory_space_constraint(x, pltpu.HBM)

    sem = pltpu.SemaphoreType.DMA(())
    stored = in_hbm(tiles.reshape(tiles.shape[2:]))
    inputs = (right_side, diag_blocks, jnp.transpose(band_blocks, (1, 2, 0, 3)), reach.reshape(1, -1))
    inputs += (tile_rows.reshape(1, 8), tile_cols.reshape(1, 8))
    send, masked, *ids, early = call(
        start_kernel,
        [HB] * 7,
        [shape(8, 32, 384), shape(48, 6, 256)]
        + [shape(1, 8, kind=jnp.int32)] * 2
        + [shape(4, 384, 384)],
        [(6, 256), (6, 6, 256), (6, 6, 8, 256), pltpu.VMEM((1, 256), jnp.int32), (32, 384)]
        + [sem] * 10,
        "start",
    )(*[in_hbm(x) for x in inputs], stored)
    ids.append(tile_count)
    recv = exchange(send, "cols")
    frames_out = [shape(32, 8, 384), shape(8, 384), shape(8, 8, 384)]
    scratch = [(LANES, 384), (8, 256), (8, 256)]
    send, band, row, edges, pick, inverse, moment, late = call(
        first_kernel,
        [VM] * 2 + [HB, VM] + [SM] * 3,
        frames_out
        + [shape(48, 6, LANES), shape(64, LANES), shape(6, 8, 8, 384), shape(1, 8, LANES)]
        + [shape(4, 384, 384)],
        scratch + [sem] * 4,
        "first",
    )(recv, masked, stored, early, *ids)
    vectors, images, moments = [row], [], [moment]
    for it in range(ITERS - 1):
        recv = exchange(send, "frames")
        (send,) = call(
            cols_kernel, [VM] * 6 + [SM] * 2, [shape(8, 16, 384)], [(16, 384)], "products"
        )(recv, early, late, row, edges, band, *ids[1:])
        recv = exchange(send, "cols")
        given = (recv, pick, inverse, row, edges, masked, early, late, *ids)
        if it + 2 < ITERS:
            send, band, row, image, moment = call(
                next_kernel,
                [VM] * 8 + [SM] * 3,
                frames_out + [shape(8, 384), shape(2, 8, LANES)],
                scratch,
                "next",
            )(*given)
            moments.append(moment)
        else:
            send, band, row, image = call(
                last_kernel,
                [VM] * 8 + [SM] * 3 + [VM] * 3,
                [shape(32, 40, LANES), shape(8, 384), shape(8, 8, 384), shape(8, 384)],
                scratch + [(40, LANES)],
                "last",
            )(*given, *moments)
        vectors.append(row)
        images.append(image)
    recv = exchange(send, "frames")
    send, known = call(
        finish_kernel, [VM] * 6 + [SM] * 2, [shape(8, 16, 384), shape(8, LANES)], [(16, 384)], "finish"
    )(recv, early, late, row, edges, band, *ids[1:])
    recv = exchange(send, "cols")
    return tuple(
        call(end_kernel, [VM] * 11, [shape(6, 256), shape(6, 256)], [(8, 256)], "end")(
            recv, pick, known, right_side, *vectors, *images
        )
    )


def solution(mesh):
    return jax.shard_map(
        per_device,
        mesh=mesh,
        in_specs=(
            P(None, ROWS),
            P(None, None, ROWS),
            P(None, None, None, ROWS),
            P(ROWS),
            P("frames", "cols", None, None, None),
            P("frames", "cols", None),
            P("frames", "cols", None),
            P("frames", "cols"),
        ),
        out_specs=(P(None, ROWS), P(None, ROWS)),
        check_vma=False,
    )
```

```python
import jax
import jax.numpy as jnp
from jax import lax
from jax.experimental import pallas as pl
from jax.experimental.pallas import tpu as pltpu
from jax.sharding import PartitionSpec as P


ITERS = 4
BAND = 8
LANES = 128
F32 = jnp.float32
ROWS = ("frames", "cols")
EARLY = 3


def lane_ids(rows):
    return lax.broadcasted_iota(jnp.int32, (rows, LANES), 1)


def half_turn(x):
    return pltpu.roll(x, 64, 1)


def left(x, by):
    return pltpu.roll(x, (x.shape[1] - by) % x.shape[1], 1) if by % x.shape[1] else x


def right(x, by):
    return pltpu.roll(x, by % x.shape[1], 1) if by % x.shape[1] else x


def store_as_tiles(ref, base, x):
    low = lane_ids(1) < 64
    for u in range(2):
        part = x[:, u * LANES : (u + 1) * LANES]
        turned = half_turn(part)
        for j in range(3):
            lanes = pl.ds(j * LANES, LANES)
            ref[pl.ds(base + 2 * u, 1), lanes] = jnp.where(
                low, part[2 * j : 2 * j + 1], turned[2 * j + 1 : 2 * j + 2]
            )
            ref[pl.ds(base + 2 * u + 1, 1), lanes] = jnp.where(
                low, turned[2 * j : 2 * j + 1], part[2 * j + 1 : 2 * j + 2]
            )


def store_as_natural(ref, t):
    low = lane_ids(1) < 64
    for j in range(3):
        part = t[:, j * LANES : (j + 1) * LANES]
        turned = half_turn(part)
        for u in range(2):
            lanes = pl.ds(u * LANES, LANES)
            ref[pl.ds(2 * j, 1), lanes] = jnp.where(
                low, part[2 * u : 2 * u + 1], turned[2 * u + 1 : 2 * u + 2]
            )
            ref[pl.ds(2 * j + 1, 1), lanes] = jnp.where(
                low, turned[2 * u : 2 * u + 1], part[2 * u + 1 : 2 * u + 2]
            )


def start_kernel(
    right_hbm, diag_hbm, band_hbm, reach_hbm, rows_hbm, cols_hbm, tiles_hbm,
    send_ref, masked_ref, extra_ref, rows_ref, cols_ref, tiles_ref,
    right_ref, diag_ref, band_ref, reach_ref, pack, lines, *sems,
):
    copies = [
        pltpu.make_async_copy(source, to, sem)
        for source, to, sem in zip(
            (diag_hbm, right_hbm, reach_hbm, band_hbm, rows_hbm, cols_hbm),
            (diag_ref, right_ref, reach_ref, band_ref, rows_ref, cols_ref),
            sems,
        )
    ]
    copies += [
        pltpu.make_async_copy(tiles_hbm.at[s], tiles_ref.at[s], sems[6 + s]) for s in range(EARLY)
    ]
    for copy in copies:
        copy.start()
    for copy in copies[:2]:
        copy.wait()
    sub = lax.broadcasted_iota(jnp.int32, (6, 256), 0)
    matrix = [diag_ref[a] for a in range(6)]
    inverse = [(sub == a).astype(F32) for a in range(6)]
    for p in range(6):
        pivot = matrix[p][p : p + 1]
        matrix[p] = matrix[p] / pivot
        inverse[p] = inverse[p] / pivot
        for a in range(6):
            if a != p:
                factor = matrix[a][p : p + 1]
                matrix[a] = matrix[a] - factor * matrix[p]
                inverse[a] = inverse[a] - factor * inverse[p]
    residual = right_ref[...]
    first = jnp.concatenate(
        [jnp.sum(inverse[a] * residual, axis=0, keepdims=True) for a in range(6)], axis=0
    )
    store_as_tiles(pack, 0, first)
    for j in range(3):
        lines[4 * j : 4 * j + 4, :] = pack[0:4, j * LANES : (j + 1) * LANES]
    for d in range(4):
        turned = jnp.concatenate(
            [inverse[a][(a + d) % 6 : (a + d) % 6 + 1] for a in range(6)], axis=0
        )
        store_as_tiles(pack, 0, turned)
        for j in range(3):
            at = (3 * d + j) * 4
            extra_ref[at : at + 4, :] = pack[0:4, j * LANES : (j + 1) * LANES]
    product = first * residual
    product = jnp.sum(product[:, 0:LANES] + product[:, LANES:256], axis=0, keepdims=True)
    product = jnp.sum(product, axis=1, keepdims=True)
    extra_ref[48:49, :] = jnp.where(lane_ids(1) == 8, product, 0.0)
    for copy in copies[2:6]:
        copy.wait()
    reach = reach_ref[...]
    for o in range(BAND):
        keep = (reach > o).astype(F32)
        for a in range(6):
            masked_ref[o * 6 + a] = band_ref[a, :, o, :] * keep
    ids = lane_ids(6)
    for j in range(3):
        packed = jnp.zeros((6, LANES), F32)
        for i in range(16):
            block = masked_ref[j * 16 + i, :, LANES : 2 * LANES]
            packed = jnp.where(ids // 8 == i, right(block, i * 8 + 8), packed)
        lines[12 + 6 * j : 18 + 6 * j, :] = packed
    lines[30:32, :] = jnp.zeros((2, LANES), F32)
    whole = lines[...]
    for c in range(8):
        send_ref[c] = whole
    for copy in copies[6:]:
        copy.wait()


def own_edge(edge_ref, row_ref, col):
    last = row_ref[(col + 7) % 8][3:4]
    values = []
    for j in range(3):
        part = last[:, j * LANES : (j + 1) * LANES]
        values += [half_turn(part), part]
    total = jnp.zeros((6, LANES), F32)
    for o in range(BAND):
        z = edge_ref[o * 6] * values[0]
        for a in range(1, 6):
            z = z + edge_ref[o * 6 + a] * values[a]
        total = total + right(z, o + 1)
    total = jnp.where(lane_ids(6) < 8, total, 0.0)
    turned = half_turn(total)
    low = lane_ids(1) < 64
    return jnp.concatenate(
        [jnp.where(low, total[2 * j : 2 * j + 1], turned[2 * j + 1 : 2 * j + 2]) for j in range(3)],
        axis=1,
    )


def slot_of(tiles_refs, s):
    return tiles_refs[0].at[s] if s < EARLY else tiles_refs[1].at[s - EARLY]


def transposed_products(row_ref, tiles_refs, ids_refs, picked, copies=()):
    rows_ref, _, count_ref = ids_refs
    count = count_ref[0, 0]
    picked[...] = jnp.zeros((LANES, 384), F32)
    for s in range(8):
        r = rows_ref[0, s]
        picked[s : s + 1, :] = row_ref[r // 4, pl.ds(r % 4, 1), :]
    upright = [picked[:, j * LANES : (j + 1) * LANES].T for j in range(3)]
    products = []
    for s in range(8):
        if copies and s >= EARLY:
            copies[s - EARLY].wait()
        total = jnp.zeros((1, 384), F32)
        for j in range(3):
            column = upright[j][:, s : s + 1]
            tile = slot_of(tiles_refs, s)[j * LANES : (j + 1) * LANES, :]
            total = total + jnp.sum(tile * column, axis=0, keepdims=True)
        products.append(total * (s < count).astype(F32))
    return products


def edge_terms(row_ref, edge_ref):
    frame = lax.axis_index("frames")
    col = lax.axis_index("cols")
    edge = own_edge(edge_ref, row_ref, col)
    cross = ((col == 0) & (frame < 31)).astype(F32)
    return edge * (col > 0).astype(F32), edge * cross


def band_terms(row_ref, masked_ref, edge, out_ref, natural, sums):
    col = lax.axis_index("cols")
    store_as_natural(natural, row_ref[col])
    lane = lax.broadcasted_iota(jnp.int32, (6, 256), 1)
    vector = natural[0:6, :]
    total = jnp.zeros((6, 256), F32)
    ahead = [jnp.zeros((6, 256), F32) for _ in range(6)]
    for o in range(BAND):
        shifted = jnp.where(lane < 255 - o, left(vector, o + 1), 0.0)
        z = jnp.zeros((6, 256), F32)
        for a in range(6):
            block = masked_ref[o * 6 + a]
            z = z + block * natural[a : a + 1, :]
            ahead[a] = ahead[a] + block * shifted
        total = total + jnp.where(lane > o, right(z, o + 1), 0.0)
    for a in range(6):
        sums[a : a + 1, :] = jnp.sum(ahead[a], axis=0, keepdims=True)
    out_ref[...] = jnp.zeros((8, 384), F32)
    store_as_tiles(out_ref, 0, total + sums[0:6, :])
    out_ref[0:1, :] = out_ref[0:1, :] + edge


def send_frames(row_ref, edge_ref, masked_ref, tiles_refs, ids_refs, send_ref, band_ref, scratch, copies=()):
    picked, natural, sums = scratch
    col = lax.axis_index("cols")
    sub = lax.broadcasted_iota(jnp.int32, (8, 384), 0)
    chunk = jnp.where(sub < 4, row_ref[col], 0.0)
    for f in range(32):
        send_ref[f] = chunk
    mine, onward = edge_terms(row_ref, edge_ref)
    send_ref[jnp.minimum(lax.axis_index("frames") + 1, 31), 4:5, :] = onward
    band_terms(row_ref, masked_ref, mine, band_ref, natural, sums)
    for s, product in enumerate(transposed_products(row_ref, tiles_refs, ids_refs, picked, copies)):
        q = ids_refs[1][0, s]
        send_ref[q // 4, pl.ds(4 + q % 4, 1), :] += product


def send_last(row_ref, edge_ref, masked_ref, tiles_refs, ids_refs, known, send_ref, band_ref, scratch):
    picked, natural, sums, pack = scratch
    col = lax.axis_index("cols")
    mine, onward = edge_terms(row_ref, edge_ref)
    band_terms(row_ref, masked_ref, mine, band_ref, natural, sums)
    own = row_ref[col]
    products = transposed_products(row_ref, tiles_refs, ids_refs, picked)
    for j in range(3):
        lanes = slice(j * LANES, (j + 1) * LANES)
        for s in range(8):
            pack[8 * j + s : 8 * j + s + 1, :] = products[s][:, lanes]
        pack[24 + 4 * j : 28 + 4 * j, :] = own[0:4, lanes]
        pack[36 + j : 37 + j, :] = onward[:, lanes]
    part = own * band_ref[...]
    quad = jnp.sum(part[:, 0:128] + part[:, 128:256] + part[:, 256:384], axis=0, keepdims=True)
    part = own[0:1] * mine
    quad = quad + part[:, 0:128] + part[:, 128:256] + part[:, 256:384]
    rows = [jnp.sum(x, axis=0, keepdims=True) for x in known] + [quad]
    lane = lax.broadcasted_iota(jnp.int32, (8, LANES), 1)
    sub = lax.broadcasted_iota(jnp.int32, (8, LANES), 0)
    totals = jnp.sum(jnp.concatenate(rows, axis=0), axis=1, keepdims=True)
    misc = jnp.sum(jnp.where(lane == sub + 8, totals, 0.0), axis=0, keepdims=True)
    for s in range(8):
        misc = jnp.where(lane_ids(1) == s, ids_refs[1][0, s].astype(F32), misc)
    pack[39:40, :] = misc
    whole = pack[...]
    for f in range(32):
        send_ref[f] = whole


def first_kernel(
    recv_ref, masked_ref, tiles_hbm, early_ref, rows_ref, cols_ref, count_ref,
    send_ref, band_ref, row_ref, edge_ref, late_ref, picked, natural, sums, *sems,
):
    copies = [
        pltpu.make_async_copy(tiles_hbm.at[EARLY + s], late_ref.at[s], sems[s])
        for s in range(8 - EARLY)
    ]
    for copy in copies:
        copy.start()
    col = lax.axis_index("cols")
    row_ref[...] = jnp.zeros((8, 8, 384), F32)
    for c in range(8):
        for j in range(3):
            row_ref[c, 0:4, j * LANES : (j + 1) * LANES] = recv_ref[c, 4 * j : 4 * j + 4, :]
    prev = (col + 7) % 8
    ids = lane_ids(6)
    for j in range(3):
        part = recv_ref[prev, 12 + 6 * j : 18 + 6 * j, :]
        for i in range(16):
            edge_ref[j * 16 + i] = jnp.where(ids >= 120, right(part, 120 - i * 8), 0.0)
    scratch = (picked, natural, sums)
    send_frames(
        row_ref, edge_ref, masked_ref, (early_ref, late_ref), (rows_ref, cols_ref, count_ref),
        send_ref, band_ref, scratch, copies,
    )


def unpack(recv_ref, pick_ref, inverse_ref):
    lane = lane_ids(1)
    target = jnp.full((1, LANES), -1.0, F32)
    for c in range(8):
        target = jnp.where(lane // 8 == c, right(recv_ref[c, 39:40, :], 8 * c), target)
    index = lax.broadcasted_iota(jnp.int32, (64, LANES), 0).astype(F32)
    found = (index == jnp.broadcast_to(target, (64, LANES))).astype(F32)
    pick_ref[...] = jnp.where(lax.broadcasted_iota(jnp.int32, (64, LANES), 1) < 64, found, 0.0)
    low = lax.broadcasted_iota(jnp.int32, (8, LANES), 0) < 4
    for c in range(8):
        parts = []
        for g in range(12):
            part = recv_ref[c, 40 + 8 * (g // 2) : 48 + 8 * (g // 2), :]
            part = pltpu.roll(part, 4, 0) if g % 2 else part
            parts.append(jnp.where(low, part, 0.0))
        parts = [jnp.concatenate(parts[3 * d : 3 * d + 3], axis=1) for d in range(4)]
        parts += [left(parts[2], 256), left(parts[1], 320)]
        for d in range(6):
            inverse_ref[d, c] = parts[d]


def row_image(recv_ref, pick_ref):
    products = jnp.concatenate(
        [recv_ref[:, 8 * j : 8 * j + 8, :].reshape(64, LANES) for j in range(3)], axis=1
    )
    image = jnp.dot(
        pick_ref[:, 0:64], products, precision=lax.Precision.HIGHEST, preferred_element_type=F32
    )
    sub = lax.broadcasted_iota(jnp.int32, (8, LANES), 0)
    rows = []
    for c in range(8):
        one, two = recv_ref[c, 24:32, :], recv_ref[c, 32:40, :]
        after = recv_ref[(c + 1) % 8, 32:40, :]
        parts = [one, pltpu.roll(one, 4, 0), two]
        onward = [pltpu.roll(after, 7 - j, 0) for j in range(3)]
        parts = [
            jnp.where(sub < 4, x, 0.0) + jnp.where(sub == 3, y, 0.0) for x, y in zip(parts, onward)
        ]
        rows.append(image[8 * c : 8 * c + 8] + jnp.concatenate(parts, axis=1))
    return jnp.concatenate(rows, axis=0).reshape(8, 8, 384)


def folded(x):
    x = jnp.sum(x, axis=0)
    return x[:, 0:128] + x[:, 128:256] + x[:, 256:384]


def advance(recv_ref, pick_ref, inverse_ref, before_ref, row_ref, image_ref, moment_ref, picked):
    col = lax.axis_index("cols")
    image = row_image(recv_ref, pick_ref)
    flat = image.reshape(64, 384)
    vector = inverse_ref[0].reshape(64, 384) * flat
    for d in range(1, 6):
        vector = vector + inverse_ref[d].reshape(64, 384) * left(flat, 64 * d)
    vector = vector.reshape(8, 8, 384)
    row_ref[...] = vector
    moments = [folded(before_ref[...] * image), folded(vector * image)]
    if moment_ref is not None:
        moment_ref[0], moment_ref[1] = moments
    picked[0:64, :] = flat
    image_ref[...] = picked[pl.ds(pl.multiple_of(col * 8, 8), 8), :]
    return moments


def second_kernel(
    recv_ref, before_ref, edge_ref, masked_ref, early_ref, late_ref, rows_ref, cols_ref, count_ref,
    send_ref, band_ref, row_ref, image_ref, moment_ref, pick_ref, inverse_ref, *scratch,
):
    unpack(recv_ref, pick_ref, inverse_ref)
    total = recv_ref[0, 39:40, :]
    for c in range(1, 8):
        total = total + recv_ref[c, 39:40, :]
    sub = lax.broadcasted_iota(jnp.int32, (8, LANES), 0)
    lane = lax.broadcasted_iota(jnp.int32, (8, LANES), 1)
    moment_ref[2] = jnp.where((sub == 0) & (lane == 8), jnp.broadcast_to(total, (8, LANES)), 0.0)
    advance(recv_ref, pick_ref, inverse_ref, before_ref, row_ref, image_ref, moment_ref, scratch[0])
    ids_refs = (rows_ref, cols_ref, count_ref)
    tiles_refs = (early_ref, late_ref)
    send_frames(row_ref, edge_ref, masked_ref, tiles_refs, ids_refs, send_ref, band_ref, scratch)


def next_kernel(
    recv_ref, before_ref, edge_ref, masked_ref, early_ref, late_ref, rows_ref, cols_ref, count_ref,
    pick_ref, inverse_ref, send_ref, band_ref, row_ref, image_ref, moment_ref, *scratch,
):
    advance(recv_ref, pick_ref, inverse_ref, before_ref, row_ref, image_ref, moment_ref, scratch[0])
    ids_refs = (rows_ref, cols_ref, count_ref)
    tiles_refs = (early_ref, late_ref)
    send_frames(row_ref, edge_ref, masked_ref, tiles_refs, ids_refs, send_ref, band_ref, scratch)


def last_kernel(
    recv_ref, before_ref, edge_ref, masked_ref, early_ref, late_ref, rows_ref, cols_ref, count_ref,
    pick_ref, inverse_ref, m1_ref, m2_ref, send_ref, band_ref, row_ref, image_ref, *scratch,
):
    moments = advance(recv_ref, pick_ref, inverse_ref, before_ref, row_ref, image_ref, None, scratch[0])
    known = [m1_ref[2], m1_ref[0], m1_ref[1], m2_ref[0], m2_ref[1]] + moments
    ids_refs = (rows_ref, cols_ref, count_ref)
    tiles_refs = (early_ref, late_ref)
    send_last(row_ref, edge_ref, masked_ref, tiles_refs, ids_refs, known, send_ref, band_ref, scratch)


def onward_terms(edge_ref, start):
    parts = []
    for j in range(3):
        part = start[:, j * LANES : (j + 1) * LANES]
        parts += [part, half_turn(part)]
    ids = lane_ids(6)
    begin = jnp.concatenate(parts, axis=0)
    sums = [jnp.zeros((6, LANES), F32) for _ in range(6)]
    for o in range(BAND):
        shifted = jnp.where(ids >= 127 - o, left(begin, o + 1), 0.0)
        for a in range(6):
            sums[a] = sums[a] + edge_ref[o * 6 + a] * shifted
    sums = [jnp.sum(x, axis=0, keepdims=True) for x in sums]
    low = lane_ids(1) < 64
    return jnp.concatenate(
        [jnp.where(low, half_turn(sums[2 * j]), sums[2 * j + 1]) for j in range(3)], axis=1
    )


def tile_products(tiles_refs, piece_of, count, pack):
    for s in range(8):
        piece = piece_of(s) * (s < count).astype(F32)
        for j in range(3):
            rows = pl.ds(j * LANES, LANES)
            tile = slot_of(tiles_refs, s)
            part = tile[rows, 0:LANES] * piece[:, 0:LANES]
            part = part + tile[rows, LANES : 2 * LANES] * piece[:, LANES : 2 * LANES]
            part = part + tile[rows, 2 * LANES : 384] * piece[:, 2 * LANES : 384]
            pack[8 * j + s : 8 * j + s + 1, :] = jnp.sum(part.T, axis=0, keepdims=True)


def cols_kernel(recv_ref, early_ref, late_ref, row_ref, edge_ref, band_ref, cols_ref, count_ref, *rest):
    extra_ref, rows_ref = rest[:2] if len(rest) == 4 else (None, None)
    send_ref, pack = rest[-2:]
    frame = lax.axis_index("frames")
    col = lax.axis_index("cols")
    total = recv_ref[0]
    for f in range(1, 32):
        total = total + recv_ref[f]
    terms = pltpu.roll(total, 4, 0) + band_ref[...]
    here = (col > 0).astype(F32)
    there = ((col == 0) & (frame < 31)).astype(F32)
    start = row_ref[col][0:1] * here + recv_ref[jnp.minimum(frame + 1, 31)][0:1] * there
    onward = onward_terms(edge_ref, start)
    for j in range(3):
        lanes = slice(j * LANES, (j + 1) * LANES)
        pack[24 + 4 * j : 28 + 4 * j, :] = terms[0:4, lanes]
        pack[36 + j : 37 + j, :] = onward[:, lanes]
    misc = jnp.zeros((1, LANES), F32)
    if extra_ref is not None:
        misc = extra_ref[48:49, :]
        for s in range(8):
            r = rows_ref[0, s]
            misc = jnp.where(lane_ids(1) == s, ((r // 4) * 8 + r % 4).astype(F32), misc)
    pack[39:40, :] = misc

    def piece_of(s):
        q = cols_ref[0, s]
        return recv_ref[q // 4, pl.ds(q % 4, 1), :]

    tile_products((early_ref, late_ref), piece_of, count_ref[0, 0], pack)
    whole = pack[...]
    for c in range(8):
        send_ref[c, 0:40, :] = whole
        if extra_ref is not None:
            send_ref[c, 40:88, :] = extra_ref[0:48, :]


def finish_kernel(
    recv_ref, early_ref, late_ref, row_ref, edge_ref, band_ref, cols_ref, count_ref, rows_ref,
    send_ref, known_ref, mine_ref, pack,
):
    frame = lax.axis_index("frames")
    col = lax.axis_index("cols")
    lane = lane_ids(1)
    misc = [recv_ref[f, 39:40, :] for f in range(32)]
    total = misc[0]
    for x in misc[1:]:
        total = total + x
    known_ref[...] = jnp.broadcast_to(total, (8, LANES))
    halves = []
    for h in range(2):
        tags = jnp.zeros((1, LANES), F32)
        for i in range(16):
            tags = jnp.where(lane // 8 == i, right(misc[16 * h + i], 8 * i), tags)
        halves.append(tags)
    tags = jnp.concatenate(halves, axis=1)
    products = jnp.concatenate(
        [recv_ref[:, 8 * j : 8 * j + 8, :].reshape(256, LANES) for j in range(3)], axis=1
    )

    def dot(a, b):
        return jnp.dot(a, b, precision=lax.Precision.HIGHEST, preferred_element_type=F32)

    at = lax.broadcasted_iota(jnp.int32, (256, 256), 0)
    wanted = ((at // 8) * 4 + at % 4).astype(F32)
    sums = dot((wanted == jnp.broadcast_to(tags, (256, 256))).astype(F32), products)
    low = lax.broadcasted_iota(jnp.int32, (8, LANES), 0) < 4
    quad = jnp.zeros((8, LANES), F32)
    for f in range(32):
        here = sums[8 * f : 8 * f + 8]
        quad = quad + jnp.where(low, here[:, 0:128], here[:, 128:256]) * recv_ref[f, 24:32, :]
        quad = quad + jnp.where(low, here[:, 256:384] * recv_ref[f, 32:40, :], 0.0)
    quad = jnp.sum(quad, axis=0, keepdims=True)
    for f in range(31):
        for j in range(3):
            quad = quad + recv_ref[f, 36 + j : 37 + j, :] * recv_ref[f + 1, 24 + 4 * j : 25 + 4 * j, :]
    quad = quad + quad + jnp.where(lane == 15, total, 0.0)

    sub = lax.broadcasted_iota(jnp.int32, (8, 256), 0)
    mine = dot((jnp.broadcast_to(tags, (8, 256)) == (4 * frame + sub % 4).astype(F32)).astype(F32), products)
    mine_ref[...] = mine + band_ref[...]
    before = jnp.maximum(frame - 1, 0)
    for j in range(3):
        lanes = slice(j * LANES, (j + 1) * LANES)
        edge = recv_ref[before, 36 + j : 37 + j, :] * (frame > 0).astype(F32)
        mine_ref[0:1, lanes] = mine_ref[0:1, lanes] + edge
    here = (col > 0).astype(F32)
    there = ((col == 0) & (frame < 31)).astype(F32)
    after = jnp.minimum(frame + 1, 31)

    def row_of(f, i):
        return jnp.concatenate([recv_ref[f, pl.ds(24 + 4 * j + i, 1), :] for j in range(3)], axis=1)

    onward = onward_terms(edge_ref, row_ref[col][0:1] * here + row_of(after, 0) * there)
    empty = jnp.where(lax.broadcasted_iota(jnp.int32, (16, LANES), 0) == 12, quad, 0.0)
    for c in range(8):
        send_ref[c] = empty
    for j in range(3):
        send_ref[(col + 7) % 8, 4 * j + 3 : 4 * j + 4, :] = onward[:, j * LANES : (j + 1) * LANES]

    def piece_of(s):
        q = cols_ref[0, s]
        return row_of(q // 4, q % 4)

    tile_products((early_ref, late_ref), piece_of, count_ref[0, 0], pack)
    for s in range(8):
        r = rows_ref[0, s]
        for j in range(3):
            send_ref[r // 4, pl.ds(4 * j + r % 4, 1), :] += pack[8 * j + s : 8 * j + s + 1, :]


def end_kernel(
    recv_ref, mine_ref, known_ref, right_ref, v0, v1, v2, v3, w0, w1, w2, solution_ref, residual_ref, scratch
):
    col = lax.axis_index("cols")
    total = recv_ref[0]
    for c in range(1, 8):
        total = total + recv_ref[c]
    parts = [total[0:8], pltpu.roll(total[0:8], 4, 0), total[8:16]]
    last = jnp.concatenate(parts, axis=1) + mine_ref[...]
    known = known_ref[0:1, :]
    mu = [jnp.broadcast_to(known[:, 8 + i : 9 + i], (1, LANES)) for i in range(7)]
    mu.append(jnp.broadcast_to(jnp.sum(total[12:13], axis=1, keepdims=True), (1, LANES)))
    zero = jnp.zeros((1, LANES), F32)
    one = zero + 1.0

    def form(left_side, shift):
        value = zero
        for i in range(len(left_side)):
            for k in range(i, len(left_side)):
                term = left_side[i] * left_side[k]
                value = value + (term if i == k else term + term) * mu[i + k + shift]
        return value

    def ratio(top, bottom):
        return jnp.where(top == 0.0, 0.0, top / jnp.where(top == 0.0, one, bottom))

    direction, residual, solution = [one], [one], []
    gamma = mu[0]
    for it in range(ITERS):
        alpha = ratio(gamma, form(direction, 0) + form(direction, 1))
        solution = solution + [zero] * (len(direction) - len(solution))
        solution = [x + alpha * p for x, p in zip(solution, direction)]
        image = [p + q for p, q in zip(direction + [zero], [zero] + direction)]
        residual = residual + [zero] * (len(image) - len(residual))
        residual = [r - alpha * y for r, y in zip(residual, image)]
        if it + 1 < ITERS:
            fresh = form(residual, 0)
            beta = ratio(fresh, gamma)
            direction = direction + [zero] * (len(residual) - len(direction))
            direction = [r + beta * p for r, p in zip(residual, direction)]
            gamma = fresh

    def wide(x):
        return jnp.concatenate([x, x, x], axis=1)

    total = wide(solution[0]) * v0[col]
    for x, ref in zip(solution[1:], (v1, v2, v3)):
        total = total + wide(x) * ref[col]
    store_as_natural(solution_ref, total)
    total = wide(residual[4]) * last
    for x, ref in zip(residual[1:4], (w0, w1, w2)):
        total = total + wide(x) * ref[...]
    store_as_natural(scratch, total)
    residual_ref[...] = scratch[0:6, :] + jnp.concatenate([residual[0]] * 2, axis=1) * right_ref[...]


VM = pl.BlockSpec(memory_space=pltpu.VMEM)
SM = pl.BlockSpec(memory_space=pltpu.SMEM)
HB = pl.BlockSpec(memory_space=pltpu.HBM)


def shape(*dims, kind=F32):
    return jax.ShapeDtypeStruct(dims, kind)


def call(kernel, specs, outs, scratch, name):
    return pl.pallas_call(
        kernel,
        in_specs=specs,
        out_specs=[VM] * len(outs),
        out_shape=outs,
        scratch_shapes=[pltpu.VMEM(s, F32) if isinstance(s, tuple) else s for s in scratch],
        compiler_params=pltpu.CompilerParams(vmem_limit_bytes=24 * 1024 * 1024),
        name=name,
    )


def per_device(right_side, diag_blocks, band_blocks, reach, tiles, tile_rows, tile_cols, tile_count):
    def exchange(x, axis):
        return lax.all_to_all(x, axis, 0, 0, tiled=True)

    def in_hbm(x):
        return pltpu.with_memory_space_constraint(x, pltpu.HBM)

    sem = pltpu.SemaphoreType.DMA(())
    stored = in_hbm(tiles.reshape(tiles.shape[2:]))
    inputs = (right_side, diag_blocks, jnp.transpose(band_blocks, (1, 2, 0, 3)), reach.reshape(1, -1))
    inputs += (tile_rows.reshape(1, 8), tile_cols.reshape(1, 8))
    send, masked, extra, *ids, early = call(
        start_kernel,
        [HB] * 7,
        [shape(8, 32, LANES), shape(48, 6, 256), shape(56, LANES)]
        + [shape(1, 8, kind=jnp.int32)] * 2
        + [shape(EARLY, 384, 384)],
        [(6, 256), (6, 6, 256), (6, 6, 8, 256), pltpu.VMEM((1, 256), jnp.int32), (8, 384), (32, LANES)]
        + [sem] * (6 + EARLY),
        "start",
    )(*[in_hbm(x) for x in inputs], stored)
    ids.append(tile_count)
    recv = exchange(send, "cols")
    frames_out = [shape(32, 8, 384), shape(8, 384), shape(8, 8, 384)]
    scratch = [(LANES, 384), (8, 256), (8, 256)]
    send, band, row, edges, late = call(
        first_kernel,
        [VM] * 2 + [HB, VM] + [SM] * 3,
        frames_out + [shape(48, 6, LANES), shape(8 - EARLY, 384, 384)],
        scratch + [sem] * (8 - EARLY),
        "first",
    )(recv, masked, stored, early, *ids)
    vectors, images, moments = [row], [], []
    for it in range(ITERS - 1):
        recv = exchange(send, "frames")
        (send,) = call(
            cols_kernel,
            [VM] * 6 + [SM] * 2 + ([VM, SM] if it == 0 else []),
            [shape(8, 88 if it == 0 else 40, LANES)],
            [(40, LANES)],
            "products",
        )(recv, early, late, row, edges, band, *ids[1:], *((extra, ids[0]) if it == 0 else ()))
        recv = exchange(send, "cols")
        given = (recv, row, edges, masked, early, late, *ids)
        specs = [VM] * 6 + [SM] * 3
        if it == 0:
            send, band, row, image, moment, pick, inverse = call(
                second_kernel,
                specs,
                frames_out
                + [shape(8, 384), shape(3, 8, LANES), shape(64, LANES), shape(6, 8, 8, 384)],
                scratch,
                "second",
            )(*given)
            moments.append(moment)
        elif it + 2 < ITERS:
            send, band, row, image, moment = call(
                next_kernel,
                specs + [VM] * 2,
                frames_out + [shape(8, 384), shape(2, 8, LANES)],
                scratch,
                "next",
            )(*given, pick, inverse)
            moments.append(moment)
        else:
            send, band, row, image = call(
                last_kernel,
                specs + [VM] * 4,
                [shape(32, 40, LANES), shape(8, 384), shape(8, 8, 384), shape(8, 384)],
                scratch + [(40, LANES)],
                "last",
            )(*given, pick, inverse, *moments)
        vectors.append(row)
        images.append(image)
    recv = exchange(send, "frames")
    send, known, mine = call(
        finish_kernel,
        [VM] * 6 + [SM] * 3,
        [shape(8, 16, LANES), shape(8, LANES), shape(8, 384)],
        [(24, LANES)],
        "finish",
    )(recv, early, late, row, edges, band, *ids[1:], ids[0])
    recv = exchange(send, "cols")
    return tuple(
        call(end_kernel, [VM] * 11, [shape(6, 256), shape(6, 256)], [(8, 256)], "end")(
            recv, mine, known, right_side, *vectors, *images
        )
    )


def solution(mesh):
    return jax.shard_map(
        per_device,
        mesh=mesh,
        in_specs=(
            P(None, ROWS),
            P(None, None, ROWS),
            P(None, None, None, ROWS),
            P(ROWS),
            P("frames", "cols", None, None, None),
            P("frames", "cols", None),
            P("frames", "cols", None),
            P("frames", "cols"),
        ),
        out_specs=(P(None, ROWS), P(None, ROWS)),
        check_vma=False,
    )
```

```python
import jax
import jax.numpy as jnp
from jax import lax
from jax.experimental import pallas as pl
from jax.experimental.pallas import tpu as pltpu
from jax.sharding import PartitionSpec as P


ITERS = 4
BAND = 8
LANES = 128
F32 = jnp.float32
ROWS = ("frames", "cols")
EARLY = 4


def lane_ids(rows):
    return lax.broadcasted_iota(jnp.int32, (rows, LANES), 1)


def half_turn(x):
    return pltpu.roll(x, 64, 1)


def left(x, by):
    return pltpu.roll(x, (x.shape[1] - by) % x.shape[1], 1) if by % x.shape[1] else x


def right(x, by):
    return pltpu.roll(x, by % x.shape[1], 1) if by % x.shape[1] else x


def store_as_tiles(ref, base, x):
    low = lane_ids(1) < 64
    for u in range(2):
        part = x[:, u * LANES : (u + 1) * LANES]
        turned = half_turn(part)
        for j in range(3):
            lanes = pl.ds(j * LANES, LANES)
            ref[pl.ds(base + 2 * u, 1), lanes] = jnp.where(
                low, part[2 * j : 2 * j + 1], turned[2 * j + 1 : 2 * j + 2]
            )
            ref[pl.ds(base + 2 * u + 1, 1), lanes] = jnp.where(
                low, turned[2 * j : 2 * j + 1], part[2 * j + 1 : 2 * j + 2]
            )


def store_as_natural(ref, t):
    low = lane_ids(1) < 64
    for j in range(3):
        part = t[:, j * LANES : (j + 1) * LANES]
        turned = half_turn(part)
        for u in range(2):
            lanes = pl.ds(u * LANES, LANES)
            ref[pl.ds(2 * j, 1), lanes] = jnp.where(
                low, part[2 * u : 2 * u + 1], turned[2 * u + 1 : 2 * u + 2]
            )
            ref[pl.ds(2 * j + 1, 1), lanes] = jnp.where(
                low, turned[2 * u : 2 * u + 1], part[2 * u + 1 : 2 * u + 2]
            )


def start_kernel(
    right_hbm, diag_hbm, band_hbm, reach_hbm, rows_hbm, cols_hbm,
    send_ref, masked_ref, extra_ref, rows_ref, cols_ref,
    right_ref, diag_ref, band_ref, reach_ref, pack, lines, *sems,
):
    copies = [
        pltpu.make_async_copy(source, to, sem)
        for source, to, sem in zip(
            (diag_hbm, right_hbm, reach_hbm, band_hbm, rows_hbm, cols_hbm),
            (diag_ref, right_ref, reach_ref, band_ref, rows_ref, cols_ref),
            sems,
        )
    ]
    for copy in copies:
        copy.start()
    for copy in copies[:2]:
        copy.wait()
    sub = lax.broadcasted_iota(jnp.int32, (6, 256), 0)
    matrix = [diag_ref[a] for a in range(6)]
    inverse = [(sub == a).astype(F32) for a in range(6)]
    for p in range(6):
        pivot = matrix[p][p : p + 1]
        matrix[p] = matrix[p] / pivot
        inverse[p] = inverse[p] / pivot
        for a in range(6):
            if a != p:
                factor = matrix[a][p : p + 1]
                matrix[a] = matrix[a] - factor * matrix[p]
                inverse[a] = inverse[a] - factor * inverse[p]
    residual = right_ref[...]
    first = jnp.concatenate(
        [jnp.sum(inverse[a] * residual, axis=0, keepdims=True) for a in range(6)], axis=0
    )
    store_as_tiles(pack, 0, first)
    for j in range(3):
        lines[4 * j : 4 * j + 4, :] = pack[0:4, j * LANES : (j + 1) * LANES]
    for d in range(4):
        turned = jnp.concatenate(
            [inverse[a][(a + d) % 6 : (a + d) % 6 + 1] for a in range(6)], axis=0
        )
        store_as_tiles(pack, 0, turned)
        for j in range(3):
            at = (3 * d + j) * 4
            extra_ref[at : at + 4, :] = pack[0:4, j * LANES : (j + 1) * LANES]
    product = first * residual
    product = jnp.sum(product[:, 0:LANES] + product[:, LANES:256], axis=0, keepdims=True)
    product = jnp.sum(product, axis=1, keepdims=True)
    extra_ref[48:49, :] = jnp.where(lane_ids(1) == 8, product, 0.0)
    for copy in copies[2:6]:
        copy.wait()
    reach = reach_ref[...]
    for o in range(BAND):
        keep = (reach > o).astype(F32)
        for a in range(6):
            masked_ref[o * 6 + a] = band_ref[a, :, o, :] * keep
    ids = lane_ids(6)
    for j in range(3):
        packed = jnp.zeros((6, LANES), F32)
        for i in range(16):
            block = masked_ref[j * 16 + i, :, LANES : 2 * LANES]
            packed = jnp.where(ids // 8 == i, right(block, i * 8 + 8), packed)
        lines[12 + 6 * j : 18 + 6 * j, :] = packed
    lines[30:32, :] = jnp.zeros((2, LANES), F32)
    whole = lines[...]
    for c in range(8):
        send_ref[c] = whole


def load_kernel(tiles_hbm, tiles_ref, *sems):
    copies = [pltpu.make_async_copy(tiles_hbm.at[s], tiles_ref.at[s], sems[s]) for s in range(EARLY)]
    for copy in copies:
        copy.start()
    for copy in copies:
        copy.wait()


def own_edge(edge_ref, row_ref, col):
    last = row_ref[(col + 7) % 8][3:4]
    values = []
    for j in range(3):
        part = last[:, j * LANES : (j + 1) * LANES]
        values += [half_turn(part), part]
    total = jnp.zeros((6, LANES), F32)
    for o in range(BAND):
        z = edge_ref[o * 6] * values[0]
        for a in range(1, 6):
            z = z + edge_ref[o * 6 + a] * values[a]
        total = total + right(z, o + 1)
    total = jnp.where(lane_ids(6) < 8, total, 0.0)
    turned = half_turn(total)
    low = lane_ids(1) < 64
    return jnp.concatenate(
        [jnp.where(low, total[2 * j : 2 * j + 1], turned[2 * j + 1 : 2 * j + 2]) for j in range(3)],
        axis=1,
    )


def bfloat16_parts(x):
    high = x.astype(jnp.bfloat16)
    rest = x - high.astype(F32)
    middle = rest.astype(jnp.bfloat16)
    return high, middle, (rest - middle.astype(F32)).astype(jnp.bfloat16)


def select_sum(pick, x):
    pick = pick.astype(jnp.bfloat16)
    high, middle, low = [
        jnp.dot(pick, part, preferred_element_type=F32) for part in bfloat16_parts(x)
    ]
    return low + middle + high


def slot_of(tiles_refs, s):
    return tiles_refs[0].at[s] if s < EARLY else tiles_refs[1].at[s - EARLY]


def transposed_products(row_ref, tiles_refs, ids_refs, picked, spread, copies=()):
    rows_ref, _, count_ref = ids_refs
    count = count_ref[0, 0]
    picked[...] = jnp.zeros((LANES, 384), F32)
    for s in range(8):
        r = rows_ref[0, s]
        picked[s : s + 1, :] = row_ref[r // 4, pl.ds(r % 4, 1), :]
    for i, part in enumerate(bfloat16_parts(picked[4:8, :])):
        picked[8 + 4 * i : 12 + 4 * i, :] = part.astype(F32)
    upright = [picked[:, j * LANES : (j + 1) * LANES].T for j in range(3)]
    at = lax.broadcasted_iota(jnp.int32, (LANES, 512), 0)
    to = lax.broadcasted_iota(jnp.int32, (LANES, 512), 1)
    ones = ((at >= 8) & (at < 20) & (at % 4 == to // LANES)).astype(jnp.bfloat16)
    for j in range(3):
        spread[j * LANES : (j + 1) * LANES, :] = jnp.dot(
            upright[j].astype(jnp.bfloat16), ones, preferred_element_type=F32
        )
    products = []
    for s in range(8):
        if copies and s >= EARLY:
            copies[s - EARLY].wait()
        tile = slot_of(tiles_refs, s)
        sums = [[None] * 3, [None] * 3]
        for i in range(48):
            if s < 4:
                column = upright[i // 16][8 * (i % 16) : 8 * (i % 16) + 8, s : s + 1]
                column = jnp.broadcast_to(column, (8, LANES))
            else:
                column = spread[8 * i : 8 * i + 8, (s - 4) * LANES : (s - 3) * LANES]
            for j in range(3):
                part = tile[8 * i : 8 * i + 8, j * LANES : (j + 1) * LANES] * column
                before = sums[i % 2][j]
                sums[i % 2][j] = part if before is None else before + part
        total = jnp.concatenate(
            [jnp.sum(x + y, axis=0, keepdims=True) for x, y in zip(*sums)], axis=1
        )
        products.append(total * (s < count).astype(F32))
    return products


def edge_terms(row_ref, edge_ref):
    frame = lax.axis_index("frames")
    col = lax.axis_index("cols")
    edge = own_edge(edge_ref, row_ref, col)
    cross = ((col == 0) & (frame < 31)).astype(F32)
    return edge * (col > 0).astype(F32), edge * cross


def band_terms(row_ref, masked_ref, edge, out_ref, natural, sums):
    col = lax.axis_index("cols")
    store_as_natural(natural, row_ref[col])
    lane = lax.broadcasted_iota(jnp.int32, (6, 256), 1)
    vector = natural[0:6, :]
    total = jnp.zeros((6, 256), F32)
    ahead = [jnp.zeros((6, 256), F32) for _ in range(6)]
    for o in range(BAND):
        shifted = jnp.where(lane < 255 - o, left(vector, o + 1), 0.0)
        z = jnp.zeros((6, 256), F32)
        for a in range(6):
            block = masked_ref[o * 6 + a]
            z = z + block * natural[a : a + 1, :]
            ahead[a] = ahead[a] + block * shifted
        total = total + jnp.where(lane > o, right(z, o + 1), 0.0)
    for a in range(6):
        sums[a : a + 1, :] = jnp.sum(ahead[a], axis=0, keepdims=True)
    out_ref[...] = jnp.zeros((8, 384), F32)
    store_as_tiles(out_ref, 0, total + sums[0:6, :])
    out_ref[0:1, :] = out_ref[0:1, :] + edge


def send_frames(row_ref, edge_ref, masked_ref, tiles_refs, ids_refs, send_ref, band_ref, scratch, copies=()):
    picked, natural, sums, spread = scratch
    col = lax.axis_index("cols")
    sub = lax.broadcasted_iota(jnp.int32, (8, 384), 0)
    chunk = jnp.where(sub < 4, row_ref[col], 0.0)
    for f in range(32):
        send_ref[f] = chunk
    mine, onward = edge_terms(row_ref, edge_ref)
    send_ref[jnp.minimum(lax.axis_index("frames") + 1, 31), 4:5, :] = onward
    band_terms(row_ref, masked_ref, mine, band_ref, natural, sums)
    for s, product in enumerate(transposed_products(row_ref, tiles_refs, ids_refs, picked, spread, copies)):
        q = ids_refs[1][0, s]
        send_ref[q // 4, pl.ds(4 + q % 4, 1), :] += product


def send_last(row_ref, edge_ref, masked_ref, tiles_refs, ids_refs, known, send_ref, band_ref, scratch):
    picked, natural, sums, spread, pack = scratch
    col = lax.axis_index("cols")
    mine, onward = edge_terms(row_ref, edge_ref)
    band_terms(row_ref, masked_ref, mine, band_ref, natural, sums)
    own = row_ref[col]
    products = transposed_products(row_ref, tiles_refs, ids_refs, picked, spread)
    for j in range(3):
        lanes = slice(j * LANES, (j + 1) * LANES)
        for s in range(8):
            pack[8 * j + s : 8 * j + s + 1, :] = products[s][:, lanes]
        pack[24 + 4 * j : 28 + 4 * j, :] = own[0:4, lanes]
        pack[36 + j : 37 + j, :] = onward[:, lanes]
    part = own * band_ref[...]
    quad = jnp.sum(part[:, 0:128] + part[:, 128:256] + part[:, 256:384], axis=0, keepdims=True)
    part = own[0:1] * mine
    quad = quad + part[:, 0:128] + part[:, 128:256] + part[:, 256:384]
    rows = [jnp.sum(x, axis=0, keepdims=True) for x in known] + [quad]
    lane = lax.broadcasted_iota(jnp.int32, (8, LANES), 1)
    sub = lax.broadcasted_iota(jnp.int32, (8, LANES), 0)
    totals = jnp.sum(jnp.concatenate(rows, axis=0), axis=1, keepdims=True)
    misc = jnp.sum(jnp.where(lane == sub + 8, totals, 0.0), axis=0, keepdims=True)
    for s in range(8):
        misc = jnp.where(lane_ids(1) == s, ids_refs[1][0, s].astype(F32), misc)
    pack[39:40, :] = misc
    whole = pack[...]
    for f in range(32):
        send_ref[f] = whole


def first_kernel(
    recv_ref, masked_ref, tiles_hbm, early_ref, rows_ref, cols_ref, count_ref,
    send_ref, band_ref, row_ref, edge_ref, late_ref, picked, natural, sums, spread, *sems,
):
    copies = [
        pltpu.make_async_copy(tiles_hbm.at[EARLY + s], late_ref.at[s], sems[s])
        for s in range(8 - EARLY)
    ]
    for copy in copies:
        copy.start()
    col = lax.axis_index("cols")
    row_ref[...] = jnp.zeros((8, 8, 384), F32)
    for c in range(8):
        for j in range(3):
            row_ref[c, 0:4, j * LANES : (j + 1) * LANES] = recv_ref[c, 4 * j : 4 * j + 4, :]
    prev = (col + 7) % 8
    ids = lane_ids(6)
    for j in range(3):
        part = recv_ref[prev, 12 + 6 * j : 18 + 6 * j, :]
        for i in range(16):
            edge_ref[j * 16 + i] = jnp.where(ids >= 120, right(part, 120 - i * 8), 0.0)
    scratch = (picked, natural, sums, spread)
    send_frames(
        row_ref, edge_ref, masked_ref, (early_ref, late_ref), (rows_ref, cols_ref, count_ref),
        send_ref, band_ref, scratch, copies,
    )


def unpack(recv_ref, pick_ref, inverse_ref):
    lane = lane_ids(1)
    target = jnp.full((1, LANES), -1.0, F32)
    for c in range(8):
        target = jnp.where(lane // 8 == c, right(recv_ref[c, 39:40, :], 8 * c), target)
    index = lax.broadcasted_iota(jnp.int32, (64, LANES), 0).astype(F32)
    found = (index == jnp.broadcast_to(target, (64, LANES))).astype(F32)
    pick_ref[...] = jnp.where(lax.broadcasted_iota(jnp.int32, (64, LANES), 1) < 64, found, 0.0)
    low = lax.broadcasted_iota(jnp.int32, (8, LANES), 0) < 4
    for c in range(8):
        parts = []
        for g in range(12):
            part = recv_ref[c, 40 + 8 * (g // 2) : 48 + 8 * (g // 2), :]
            part = pltpu.roll(part, 4, 0) if g % 2 else part
            parts.append(jnp.where(low, part, 0.0))
        parts = [jnp.concatenate(parts[3 * d : 3 * d + 3], axis=1) for d in range(4)]
        parts += [left(parts[2], 256), left(parts[1], 320)]
        for d in range(6):
            inverse_ref[d, c] = parts[d]


def row_image(recv_ref, pick_ref):
    products = jnp.concatenate(
        [recv_ref[:, 8 * j : 8 * j + 8, :].reshape(64, LANES) for j in range(3)], axis=1
    )
    image = select_sum(pick_ref[:, 0:64], products)
    sub = lax.broadcasted_iota(jnp.int32, (8, LANES), 0)
    rows = []
    for c in range(8):
        one, two = recv_ref[c, 24:32, :], recv_ref[c, 32:40, :]
        after = recv_ref[(c + 1) % 8, 32:40, :]
        parts = [one, pltpu.roll(one, 4, 0), two]
        onward = [pltpu.roll(after, 7 - j, 0) for j in range(3)]
        parts = [
            jnp.where(sub < 4, x, 0.0) + jnp.where(sub == 3, y, 0.0) for x, y in zip(parts, onward)
        ]
        rows.append(image[8 * c : 8 * c + 8] + jnp.concatenate(parts, axis=1))
    return jnp.concatenate(rows, axis=0).reshape(8, 8, 384)


def folded(x):
    x = jnp.sum(x, axis=0)
    return x[:, 0:128] + x[:, 128:256] + x[:, 256:384]


def advance(recv_ref, pick_ref, inverse_ref, before_ref, row_ref, image_ref, moment_ref, picked):
    col = lax.axis_index("cols")
    image = row_image(recv_ref, pick_ref)
    flat = image.reshape(64, 384)
    vector = inverse_ref[0].reshape(64, 384) * flat
    for d in range(1, 6):
        vector = vector + inverse_ref[d].reshape(64, 384) * left(flat, 64 * d)
    vector = vector.reshape(8, 8, 384)
    row_ref[...] = vector
    moments = [folded(before_ref[...] * image), folded(vector * image)]
    if moment_ref is not None:
        moment_ref[0], moment_ref[1] = moments
    picked[0:64, :] = flat
    image_ref[...] = picked[pl.ds(pl.multiple_of(col * 8, 8), 8), :]
    return moments


def second_kernel(
    recv_ref, before_ref, edge_ref, masked_ref, early_ref, late_ref, rows_ref, cols_ref, count_ref,
    send_ref, band_ref, row_ref, image_ref, moment_ref, pick_ref, inverse_ref, *scratch,
):
    unpack(recv_ref, pick_ref, inverse_ref)
    total = recv_ref[0, 39:40, :]
    for c in range(1, 8):
        total = total + recv_ref[c, 39:40, :]
    sub = lax.broadcasted_iota(jnp.int32, (8, LANES), 0)
    lane = lax.broadcasted_iota(jnp.int32, (8, LANES), 1)
    moment_ref[2] = jnp.where((sub == 0) & (lane == 8), jnp.broadcast_to(total, (8, LANES)), 0.0)
    advance(recv_ref, pick_ref, inverse_ref, before_ref, row_ref, image_ref, moment_ref, scratch[0])
    ids_refs = (rows_ref, cols_ref, count_ref)
    tiles_refs = (early_ref, late_ref)
    send_frames(row_ref, edge_ref, masked_ref, tiles_refs, ids_refs, send_ref, band_ref, scratch)


def next_kernel(
    recv_ref, before_ref, edge_ref, masked_ref, early_ref, late_ref, rows_ref, cols_ref, count_ref,
    pick_ref, inverse_ref, send_ref, band_ref, row_ref, image_ref, moment_ref, *scratch,
):
    advance(recv_ref, pick_ref, inverse_ref, before_ref, row_ref, image_ref, moment_ref, scratch[0])
    ids_refs = (rows_ref, cols_ref, count_ref)
    tiles_refs = (early_ref, late_ref)
    send_frames(row_ref, edge_ref, masked_ref, tiles_refs, ids_refs, send_ref, band_ref, scratch)


def last_kernel(
    recv_ref, before_ref, edge_ref, masked_ref, early_ref, late_ref, rows_ref, cols_ref, count_ref,
    pick_ref, inverse_ref, m1_ref, m2_ref, send_ref, band_ref, row_ref, image_ref, *scratch,
):
    moments = advance(recv_ref, pick_ref, inverse_ref, before_ref, row_ref, image_ref, None, scratch[0])
    known = [m1_ref[2], m1_ref[0], m1_ref[1], m2_ref[0], m2_ref[1]] + moments
    ids_refs = (rows_ref, cols_ref, count_ref)
    tiles_refs = (early_ref, late_ref)
    send_last(row_ref, edge_ref, masked_ref, tiles_refs, ids_refs, known, send_ref, band_ref, scratch)


def onward_terms(edge_ref, start):
    parts = []
    for j in range(3):
        part = start[:, j * LANES : (j + 1) * LANES]
        parts += [part, half_turn(part)]
    ids = lane_ids(6)
    begin = jnp.concatenate(parts, axis=0)
    sums = [jnp.zeros((6, LANES), F32) for _ in range(6)]
    for o in range(BAND):
        shifted = jnp.where(ids >= 127 - o, left(begin, o + 1), 0.0)
        for a in range(6):
            sums[a] = sums[a] + edge_ref[o * 6 + a] * shifted
    sums = [jnp.sum(x, axis=0, keepdims=True) for x in sums]
    low = lane_ids(1) < 64
    return jnp.concatenate(
        [jnp.where(low, half_turn(sums[2 * j]), sums[2 * j + 1]) for j in range(3)], axis=1
    )


def tile_products(tiles_refs, piece_of, count, pack):
    for s in range(8):
        piece = piece_of(s) * (s < count).astype(F32)
        for j in range(3):
            rows = pl.ds(j * LANES, LANES)
            tile = slot_of(tiles_refs, s)
            part = tile[rows, 0:LANES] * piece[:, 0:LANES]
            part = part + tile[rows, LANES : 2 * LANES] * piece[:, LANES : 2 * LANES]
            part = part + tile[rows, 2 * LANES : 384] * piece[:, 2 * LANES : 384]
            pack[8 * j + s : 8 * j + s + 1, :] = jnp.sum(part.T, axis=0, keepdims=True)


def cols_kernel(recv_ref, early_ref, late_ref, row_ref, edge_ref, band_ref, cols_ref, count_ref, *rest):
    extra_ref, rows_ref = rest[:2] if len(rest) == 4 else (None, None)
    send_ref, pack = rest[-2:]
    frame = lax.axis_index("frames")
    col = lax.axis_index("cols")
    total = recv_ref[0]
    for f in range(1, 32):
        total = total + recv_ref[f]
    terms = pltpu.roll(total, 4, 0) + band_ref[...]
    here = (col > 0).astype(F32)
    there = ((col == 0) & (frame < 31)).astype(F32)
    start = row_ref[col][0:1] * here + recv_ref[jnp.minimum(frame + 1, 31)][0:1] * there
    onward = onward_terms(edge_ref, start)
    for j in range(3):
        lanes = slice(j * LANES, (j + 1) * LANES)
        pack[24 + 4 * j : 28 + 4 * j, :] = terms[0:4, lanes]
        pack[36 + j : 37 + j, :] = onward[:, lanes]
    misc = jnp.zeros((1, LANES), F32)
    if extra_ref is not None:
        misc = extra_ref[48:49, :]
        for s in range(8):
            r = rows_ref[0, s]
            misc = jnp.where(lane_ids(1) == s, ((r // 4) * 8 + r % 4).astype(F32), misc)
    pack[39:40, :] = misc

    def piece_of(s):
        q = cols_ref[0, s]
        return recv_ref[q // 4, pl.ds(q % 4, 1), :]

    tile_products((early_ref, late_ref), piece_of, count_ref[0, 0], pack)
    whole = pack[...]
    for c in range(8):
        send_ref[c, 0:40, :] = whole
        if extra_ref is not None:
            send_ref[c, 40:88, :] = extra_ref[0:48, :]


def finish_kernel(
    recv_ref, early_ref, late_ref, row_ref, edge_ref, band_ref, cols_ref, count_ref, rows_ref,
    send_ref, known_ref, mine_ref, pack, columns,
):
    frame = lax.axis_index("frames")
    col = lax.axis_index("cols")
    lane = lane_ids(1)
    misc = [recv_ref[f, 39:40, :] for f in range(32)]
    total = misc[0]
    for x in misc[1:]:
        total = total + x
    known_ref[...] = jnp.broadcast_to(total, (8, LANES))
    halves = []
    for h in range(2):
        tags = jnp.zeros((1, LANES), F32)
        for i in range(16):
            tags = jnp.where(lane // 8 == i, right(misc[16 * h + i], 8 * i), tags)
        halves.append(tags)
    tags = jnp.concatenate(halves, axis=1)
    products = jnp.concatenate(
        [recv_ref[:, 8 * j : 8 * j + 8, :].reshape(256, LANES) for j in range(3)], axis=1
    )

    at = lax.broadcasted_iota(jnp.int32, (256, 256), 0)
    wanted = ((at // 8) * 4 + at % 4).astype(F32)
    sums = select_sum((wanted == jnp.broadcast_to(tags, (256, 256))).astype(F32), products)
    columns[...] = sums
    low = lax.broadcasted_iota(jnp.int32, (8, LANES), 0) < 4
    quad = jnp.zeros((8, LANES), F32)
    for f in range(32):
        here = sums[8 * f : 8 * f + 8]
        quad = quad + jnp.where(low, here[:, 0:128], here[:, 128:256]) * recv_ref[f, 24:32, :]
        quad = quad + jnp.where(low, here[:, 256:384] * recv_ref[f, 32:40, :], 0.0)
    quad = jnp.sum(quad, axis=0, keepdims=True)
    for f in range(31):
        for j in range(3):
            quad = quad + recv_ref[f, 36 + j : 37 + j, :] * recv_ref[f + 1, 24 + 4 * j : 25 + 4 * j, :]
    quad = quad + quad + jnp.where(lane == 15, total, 0.0)

    mine = columns[pl.ds(pl.multiple_of(frame * 8, 8), 8), :]
    mine_ref[...] = mine + band_ref[...]
    before = jnp.maximum(frame - 1, 0)
    for j in range(3):
        lanes = slice(j * LANES, (j + 1) * LANES)
        edge = recv_ref[before, 36 + j : 37 + j, :] * (frame > 0).astype(F32)
        mine_ref[0:1, lanes] = mine_ref[0:1, lanes] + edge
    here = (col > 0).astype(F32)
    there = ((col == 0) & (frame < 31)).astype(F32)
    after = jnp.minimum(frame + 1, 31)

    def row_of(f, i):
        return jnp.concatenate([recv_ref[f, pl.ds(24 + 4 * j + i, 1), :] for j in range(3)], axis=1)

    onward = onward_terms(edge_ref, row_ref[col][0:1] * here + row_of(after, 0) * there)
    empty = jnp.where(lax.broadcasted_iota(jnp.int32, (16, LANES), 0) == 12, quad, 0.0)
    for c in range(8):
        send_ref[c] = empty
    for j in range(3):
        send_ref[(col + 7) % 8, 4 * j + 3 : 4 * j + 4, :] = onward[:, j * LANES : (j + 1) * LANES]

    def piece_of(s):
        q = cols_ref[0, s]
        return row_of(q // 4, q % 4)

    tile_products((early_ref, late_ref), piece_of, count_ref[0, 0], pack)
    for s in range(8):
        r = rows_ref[0, s]
        for j in range(3):
            send_ref[r // 4, pl.ds(4 * j + r % 4, 1), :] += pack[8 * j + s : 8 * j + s + 1, :]


def end_kernel(
    recv_ref, mine_ref, known_ref, right_ref, v0, v1, v2, v3, w0, w1, w2, solution_ref, residual_ref, scratch
):
    col = lax.axis_index("cols")
    total = recv_ref[0]
    for c in range(1, 8):
        total = total + recv_ref[c]
    parts = [total[0:8], pltpu.roll(total[0:8], 4, 0), total[8:16]]
    last = jnp.concatenate(parts, axis=1) + mine_ref[...]
    known = known_ref[0:1, :]
    mu = [jnp.broadcast_to(known[:, 8 + i : 9 + i], (1, LANES)) for i in range(7)]
    mu.append(jnp.broadcast_to(jnp.sum(total[12:13], axis=1, keepdims=True), (1, LANES)))
    zero = jnp.zeros((1, LANES), F32)
    one = zero + 1.0

    def form(left_side, shift):
        value = zero
        for i in range(len(left_side)):
            for k in range(i, len(left_side)):
                term = left_side[i] * left_side[k]
                value = value + (term if i == k else term + term) * mu[i + k + shift]
        return value

    def ratio(top, bottom):
        return jnp.where(top == 0.0, 0.0, top / jnp.where(top == 0.0, one, bottom))

    direction, residual, solution = [one], [one], []
    gamma = mu[0]
    for it in range(ITERS):
        alpha = ratio(gamma, form(direction, 0) + form(direction, 1))
        solution = solution + [zero] * (len(direction) - len(solution))
        solution = [x + alpha * p for x, p in zip(solution, direction)]
        image = [p + q for p, q in zip(direction + [zero], [zero] + direction)]
        residual = residual + [zero] * (len(image) - len(residual))
        residual = [r - alpha * y for r, y in zip(residual, image)]
        if it + 1 < ITERS:
            fresh = form(residual, 0)
            beta = ratio(fresh, gamma)
            direction = direction + [zero] * (len(residual) - len(direction))
            direction = [r + beta * p for r, p in zip(residual, direction)]
            gamma = fresh

    def wide(x):
        return jnp.concatenate([x, x, x], axis=1)

    total = wide(solution[0]) * v0[col]
    for x, ref in zip(solution[1:], (v1, v2, v3)):
        total = total + wide(x) * ref[col]
    store_as_natural(solution_ref, total)
    total = wide(residual[4]) * last
    for x, ref in zip(residual[1:4], (w0, w1, w2)):
        total = total + wide(x) * ref[...]
    store_as_natural(scratch, total)
    residual_ref[...] = scratch[0:6, :] + jnp.concatenate([residual[0]] * 2, axis=1) * right_ref[...]


VM = pl.BlockSpec(memory_space=pltpu.VMEM)
SM = pl.BlockSpec(memory_space=pltpu.SMEM)
HB = pl.BlockSpec(memory_space=pltpu.HBM)


def shape(*dims, kind=F32):
    return jax.ShapeDtypeStruct(dims, kind)


def call(kernel, specs, outs, scratch, name):
    return pl.pallas_call(
        kernel,
        in_specs=specs,
        out_specs=[VM] * len(outs),
        out_shape=outs,
        scratch_shapes=[pltpu.VMEM(s, F32) if isinstance(s, tuple) else s for s in scratch],
        compiler_params=pltpu.CompilerParams(vmem_limit_bytes=24 * 1024 * 1024),
        name=name,
    )


def per_device(right_side, diag_blocks, band_blocks, reach, tiles, tile_rows, tile_cols, tile_count):
    def exchange(x, axis):
        return lax.all_to_all(x, axis, 0, 0, tiled=True)

    def in_hbm(x):
        return pltpu.with_memory_space_constraint(x, pltpu.HBM)

    sem = pltpu.SemaphoreType.DMA(())
    stored = in_hbm(tiles.reshape(tiles.shape[2:]))
    inputs = (right_side, diag_blocks, jnp.transpose(band_blocks, (1, 2, 0, 3)), reach.reshape(1, -1))
    inputs += (tile_rows.reshape(1, 8), tile_cols.reshape(1, 8))
    send, masked, extra, *ids = call(
        start_kernel,
        [HB] * 6,
        [shape(8, 32, LANES), shape(48, 6, 256), shape(56, LANES)]
        + [shape(1, 8, kind=jnp.int32)] * 2,
        [(6, 256), (6, 6, 256), (6, 6, 8, 256), pltpu.VMEM((1, 256), jnp.int32), (8, 384), (32, LANES)]
        + [sem] * 6,
        "start",
    )(*[in_hbm(x) for x in inputs])
    ids.append(tile_count)
    recv = exchange(send, "cols")
    (early,) = call(load_kernel, [HB], [shape(EARLY, 384, 384)], [sem] * EARLY, "load")(stored)
    frames_out = [shape(32, 8, 384), shape(8, 384), shape(8, 8, 384)]
    scratch = [(LANES, 384), (8, 256), (8, 256), (384, 512)]
    send, band, row, edges, late = call(
        first_kernel,
        [VM] * 2 + [HB, VM] + [SM] * 3,
        frames_out + [shape(48, 6, LANES), shape(8 - EARLY, 384, 384)],
        scratch + [sem] * (8 - EARLY),
        "first",
    )(recv, masked, stored, early, *ids)
    vectors, images, moments = [row], [], []
    for it in range(ITERS - 1):
        recv = exchange(send, "frames")
        (send,) = call(
            cols_kernel,
            [VM] * 6 + [SM] * 2 + ([VM, SM] if it == 0 else []),
            [shape(8, 88 if it == 0 else 40, LANES)],
            [(40, LANES)],
            "products",
        )(recv, early, late, row, edges, band, *ids[1:], *((extra, ids[0]) if it == 0 else ()))
        recv = exchange(send, "cols")
        given = (recv, row, edges, masked, early, late, *ids)
        specs = [VM] * 6 + [SM] * 3
        if it == 0:
            send, band, row, image, moment, pick, inverse = call(
                second_kernel,
                specs,
                frames_out
                + [shape(8, 384), shape(3, 8, LANES), shape(64, LANES), shape(6, 8, 8, 384)],
                scratch,
                "second",
            )(*given)
            moments.append(moment)
        elif it + 2 < ITERS:
            send, band, row, image, moment = call(
                next_kernel,
                specs + [VM] * 2,
                frames_out + [shape(8, 384), shape(2, 8, LANES)],
                scratch,
                "next",
            )(*given, pick, inverse)
            moments.append(moment)
        else:
            send, band, row, image = call(
                last_kernel,
                specs + [VM] * 4,
                [shape(32, 40, LANES), shape(8, 384), shape(8, 8, 384), shape(8, 384)],
                scratch + [(40, LANES)],
                "last",
            )(*given, pick, inverse, *moments)
        vectors.append(row)
        images.append(image)
    recv = exchange(send, "frames")
    send, known, mine = call(
        finish_kernel,
        [VM] * 6 + [SM] * 3,
        [shape(8, 16, LANES), shape(8, LANES), shape(8, 384)],
        [(24, LANES), (256, 384)],
        "finish",
    )(recv, early, late, row, edges, band, *ids[1:], ids[0])
    recv = exchange(send, "cols")
    return tuple(
        call(end_kernel, [VM] * 11, [shape(6, 256), shape(6, 256)], [(8, 256)], "end")(
            recv, mine, known, right_side, *vectors, *images
        )
    )


def solution(mesh):
    return jax.shard_map(
        per_device,
        mesh=mesh,
        in_specs=(
            P(None, ROWS),
            P(None, None, ROWS),
            P(None, None, None, ROWS),
            P(ROWS),
            P("frames", "cols", None, None, None),
            P("frames", "cols", None),
            P("frames", "cols", None),
            P("frames", "cols"),
        ),
        out_specs=(P(None, ROWS), P(None, ROWS)),
        check_vma=False,
    )
```

```python
import jax
import jax.numpy as jnp
from jax import lax
from jax.experimental import pallas as pl
from jax.experimental.pallas import tpu as pltpu
from jax.sharding import PartitionSpec as P


ITERS = 4
BAND = 8
LANES = 128
F32 = jnp.float32
ROWS = ("frames", "cols")
EARLY = 5


def lane_ids(rows):
    return lax.broadcasted_iota(jnp.int32, (rows, LANES), 1)


def half_turn(x):
    return pltpu.roll(x, 64, 1)


def left(x, by):
    return pltpu.roll(x, (x.shape[1] - by) % x.shape[1], 1) if by % x.shape[1] else x


def right(x, by):
    return pltpu.roll(x, by % x.shape[1], 1) if by % x.shape[1] else x


def store_as_tiles(ref, base, x):
    low = lane_ids(1) < 64
    for u in range(2):
        part = x[:, u * LANES : (u + 1) * LANES]
        turned = half_turn(part)
        for j in range(3):
            lanes = pl.ds(j * LANES, LANES)
            ref[pl.ds(base + 2 * u, 1), lanes] = jnp.where(
                low, part[2 * j : 2 * j + 1], turned[2 * j + 1 : 2 * j + 2]
            )
            ref[pl.ds(base + 2 * u + 1, 1), lanes] = jnp.where(
                low, turned[2 * j : 2 * j + 1], part[2 * j + 1 : 2 * j + 2]
            )


def store_as_natural(ref, t):
    low = lane_ids(1) < 64
    for j in range(3):
        part = t[:, j * LANES : (j + 1) * LANES]
        turned = half_turn(part)
        for u in range(2):
            lanes = pl.ds(u * LANES, LANES)
            ref[pl.ds(2 * j, 1), lanes] = jnp.where(
                low, part[2 * u : 2 * u + 1], turned[2 * u + 1 : 2 * u + 2]
            )
            ref[pl.ds(2 * j + 1, 1), lanes] = jnp.where(
                low, turned[2 * u : 2 * u + 1], part[2 * u + 1 : 2 * u + 2]
            )


def start_kernel(
    right_hbm, diag_hbm, band_hbm, reach_hbm, rows_hbm, cols_hbm,
    send_ref, masked_ref, extra_ref, rows_ref, cols_ref,
    right_ref, diag_ref, band_ref, reach_ref, pack, *sems,
):
    copies = [
        pltpu.make_async_copy(source, to, sem)
        for source, to, sem in zip(
            (diag_hbm, right_hbm, reach_hbm, band_hbm, rows_hbm, cols_hbm),
            (diag_ref, right_ref, reach_ref, band_ref, rows_ref, cols_ref),
            sems,
        )
    ]
    for copy in copies:
        copy.start()
    for copy in copies[:2]:
        copy.wait()
    sub = lax.broadcasted_iota(jnp.int32, (6, 256), 0)
    matrix = [diag_ref[a] for a in range(6)]
    inverse = [(sub == a).astype(F32) for a in range(6)]
    for p in range(6):
        pivot = matrix[p][p : p + 1]
        matrix[p] = matrix[p] / pivot
        inverse[p] = inverse[p] / pivot
        for a in range(6):
            if a != p:
                factor = matrix[a][p : p + 1]
                matrix[a] = matrix[a] - factor * matrix[p]
                inverse[a] = inverse[a] - factor * inverse[p]
    residual = right_ref[...]
    first = jnp.concatenate(
        [jnp.sum(inverse[a] * residual, axis=0, keepdims=True) for a in range(6)], axis=0
    )
    store_as_tiles(pack, 0, first)
    for j in range(3):
        send_ref[4 * j : 4 * j + 4, :] = pack[0:4, j * LANES : (j + 1) * LANES]
    for d in range(4):
        turned = jnp.concatenate(
            [inverse[a][(a + d) % 6 : (a + d) % 6 + 1] for a in range(6)], axis=0
        )
        store_as_tiles(pack, 0, turned)
        for j in range(3):
            at = (3 * d + j) * 4
            extra_ref[at : at + 4, :] = pack[0:4, j * LANES : (j + 1) * LANES]
    product = first * residual
    product = jnp.sum(product[:, 0:LANES] + product[:, LANES:256], axis=0, keepdims=True)
    product = jnp.sum(product, axis=1, keepdims=True)
    extra_ref[48:49, :] = jnp.where(lane_ids(1) == 8, product, 0.0)
    for copy in copies[2:6]:
        copy.wait()
    reach = reach_ref[...]
    for o in range(BAND):
        keep = (reach > o).astype(F32)
        for a in range(6):
            masked_ref[o * 6 + a] = band_ref[a, :, o, :] * keep
    ids = lane_ids(6)
    for j in range(3):
        packed = jnp.zeros((6, LANES), F32)
        for i in range(16):
            block = masked_ref[j * 16 + i, :, LANES : 2 * LANES]
            packed = jnp.where(ids // 8 == i, right(block, i * 8 + 8), packed)
        send_ref[12 + 6 * j : 18 + 6 * j, :] = packed
    send_ref[30:32, :] = jnp.zeros((2, LANES), F32)


def blocks(refs):
    col = lax.axis_index("cols")
    rows = refs[0].shape[0] // 2
    return [
        (((col // 2 + 4 - d) % 4) * 2 + (col + i) % 2, refs[d], i * rows)
        for d in range(4)
        for i in range(2)
    ]


def load_kernel(tiles_hbm, tiles_ref, *sems):
    copies = [pltpu.make_async_copy(tiles_hbm.at[s], tiles_ref.at[s], sems[s]) for s in range(EARLY)]
    for copy in copies:
        copy.start()
    for copy in copies:
        copy.wait()


def own_edge(edge_ref, row_ref, col):
    last = row_ref[(col + 7) % 8][3:4]
    values = []
    for j in range(3):
        part = last[:, j * LANES : (j + 1) * LANES]
        values += [half_turn(part), part]
    total = jnp.zeros((6, LANES), F32)
    for o in range(BAND):
        z = edge_ref[o * 6] * values[0]
        for a in range(1, 6):
            z = z + edge_ref[o * 6 + a] * values[a]
        total = total + right(z, o + 1)
    total = jnp.where(lane_ids(6) < 8, total, 0.0)
    turned = half_turn(total)
    low = lane_ids(1) < 64
    return jnp.concatenate(
        [jnp.where(low, total[2 * j : 2 * j + 1], turned[2 * j + 1 : 2 * j + 2]) for j in range(3)],
        axis=1,
    )


def bfloat16_parts(x):
    high = x.astype(jnp.bfloat16)
    rest = x - high.astype(F32)
    middle = rest.astype(jnp.bfloat16)
    return high, middle, (rest - middle.astype(F32)).astype(jnp.bfloat16)


def select_sum(pick, x):
    pick = pick.astype(jnp.bfloat16)
    high, middle, low = [
        jnp.dot(pick, part, preferred_element_type=F32) for part in bfloat16_parts(x)
    ]
    return low + middle + high


def slot_of(tiles_refs, s):
    return tiles_refs[0].at[s] if s < EARLY else tiles_refs[1].at[s - EARLY]


def transposed_products(row_ref, tiles_refs, ids_refs, picked, spread, copies=()):
    rows_ref, _, count_ref = ids_refs
    count = count_ref[0, 0]
    picked[...] = jnp.zeros((LANES, 384), F32)
    for s in range(8):
        r = rows_ref[0, s]
        picked[s : s + 1, :] = row_ref[r // 4, pl.ds(r % 4, 1), :]
    for i, part in enumerate(bfloat16_parts(picked[4:8, :])):
        picked[8 + 4 * i : 12 + 4 * i, :] = part.astype(F32)
    upright = [picked[:, j * LANES : (j + 1) * LANES].T for j in range(3)]
    at = lax.broadcasted_iota(jnp.int32, (LANES, 512), 0)
    to = lax.broadcasted_iota(jnp.int32, (LANES, 512), 1)
    ones = ((at >= 8) & (at < 20) & (at % 4 == to // LANES)).astype(jnp.bfloat16)
    for j in range(3):
        spread[j * LANES : (j + 1) * LANES, :] = jnp.dot(
            upright[j].astype(jnp.bfloat16), ones, preferred_element_type=F32
        )
    products = []
    for s in range(8):
        if copies and s >= EARLY:
            copies[s - EARLY].wait()
        tile = slot_of(tiles_refs, s)
        sums = [[None] * 3, [None] * 3]
        for i in range(48):
            if s < 4:
                column = upright[i // 16][8 * (i % 16) : 8 * (i % 16) + 8, s : s + 1]
                column = jnp.broadcast_to(column, (8, LANES))
            else:
                column = spread[8 * i : 8 * i + 8, (s - 4) * LANES : (s - 3) * LANES]
            for j in range(3):
                part = tile[8 * i : 8 * i + 8, j * LANES : (j + 1) * LANES] * column
                before = sums[i % 2][j]
                sums[i % 2][j] = part if before is None else before + part
        total = jnp.concatenate(
            [jnp.sum(x + y, axis=0, keepdims=True) for x, y in zip(*sums)], axis=1
        )
        products.append(total * (s < count).astype(F32))
    return products


def edge_terms(row_ref, edge_ref):
    frame = lax.axis_index("frames")
    col = lax.axis_index("cols")
    edge = own_edge(edge_ref, row_ref, col)
    cross = ((col == 0) & (frame < 31)).astype(F32)
    return edge * (col > 0).astype(F32), edge * cross


def band_terms(row_ref, masked_ref, edge, out_ref, natural, sums):
    col = lax.axis_index("cols")
    store_as_natural(natural, row_ref[col])
    lane = lax.broadcasted_iota(jnp.int32, (6, 256), 1)
    vector = natural[0:6, :]
    total = jnp.zeros((6, 256), F32)
    ahead = [jnp.zeros((6, 256), F32) for _ in range(6)]
    for o in range(BAND):
        shifted = jnp.where(lane < 255 - o, left(vector, o + 1), 0.0)
        z = jnp.zeros((6, 256), F32)
        for a in range(6):
            block = masked_ref[o * 6 + a]
            z = z + block * natural[a : a + 1, :]
            ahead[a] = ahead[a] + block * shifted
        total = total + jnp.where(lane > o, right(z, o + 1), 0.0)
    for a in range(6):
        sums[a : a + 1, :] = jnp.sum(ahead[a], axis=0, keepdims=True)
    out_ref[...] = jnp.zeros((8, 384), F32)
    store_as_tiles(out_ref, 0, total + sums[0:6, :])
    out_ref[0:1, :] = out_ref[0:1, :] + edge


def send_frames(row_ref, edge_ref, masked_ref, tiles_refs, ids_refs, send_ref, band_ref, scratch, copies=()):
    picked, natural, sums, spread = scratch
    col = lax.axis_index("cols")
    sub = lax.broadcasted_iota(jnp.int32, (8, 384), 0)
    chunk = jnp.where(sub < 4, row_ref[col], 0.0)
    for f in range(32):
        send_ref[f] = chunk
    mine, onward = edge_terms(row_ref, edge_ref)
    send_ref[jnp.minimum(lax.axis_index("frames") + 1, 31), 4:5, :] = onward
    band_terms(row_ref, masked_ref, mine, band_ref, natural, sums)
    for s, product in enumerate(transposed_products(row_ref, tiles_refs, ids_refs, picked, spread, copies)):
        q = ids_refs[1][0, s]
        send_ref[q // 4, pl.ds(4 + q % 4, 1), :] += product


def send_last(row_ref, edge_ref, masked_ref, tiles_refs, ids_refs, known, send_ref, band_ref, scratch):
    picked, natural, sums, spread, pack = scratch
    col = lax.axis_index("cols")
    mine, onward = edge_terms(row_ref, edge_ref)
    band_terms(row_ref, masked_ref, mine, band_ref, natural, sums)
    own = row_ref[col]
    products = transposed_products(row_ref, tiles_refs, ids_refs, picked, spread)
    for j in range(3):
        lanes = slice(j * LANES, (j + 1) * LANES)
        for s in range(8):
            pack[8 * j + s : 8 * j + s + 1, :] = products[s][:, lanes]
        pack[24 + 4 * j : 28 + 4 * j, :] = own[0:4, lanes]
        pack[36 + j : 37 + j, :] = onward[:, lanes]
    part = own * band_ref[...]
    quad = jnp.sum(part[:, 0:128] + part[:, 128:256] + part[:, 256:384], axis=0, keepdims=True)
    part = own[0:1] * mine
    quad = quad + part[:, 0:128] + part[:, 128:256] + part[:, 256:384]
    rows = [jnp.sum(x, axis=0, keepdims=True) for x in known] + [quad]
    lane = lax.broadcasted_iota(jnp.int32, (8, LANES), 1)
    sub = lax.broadcasted_iota(jnp.int32, (8, LANES), 0)
    totals = jnp.sum(jnp.concatenate(rows, axis=0), axis=1, keepdims=True)
    misc = jnp.sum(jnp.where(lane == sub + 8, totals, 0.0), axis=0, keepdims=True)
    for s in range(8):
        misc = jnp.where(lane_ids(1) == s, ids_refs[1][0, s].astype(F32), misc)
    pack[39:40, :] = misc
    whole = pack[...]
    for f in range(32):
        send_ref[f] = whole


def first_kernel(
    recv0, recv1, recv2, recv3, masked_ref, tiles_hbm, early_ref, rows_ref, cols_ref, count_ref,
    send_ref, band_ref, row_ref, edge_ref, late_ref, picked, natural, sums, spread, *sems,
):
    copies = [
        pltpu.make_async_copy(tiles_hbm.at[EARLY + s], late_ref.at[s], sems[s])
        for s in range(8 - EARLY)
    ]
    for copy in copies:
        copy.start()
    col = lax.axis_index("cols")
    row_ref[...] = jnp.zeros((8, 8, 384), F32)
    for c, ref, at in blocks((recv0, recv1, recv2, recv3)):
        for j in range(3):
            row_ref[c, 0:4, j * LANES : (j + 1) * LANES] = ref[at + 4 * j : at + 4 * j + 4, :]
    ids = lane_ids(6)
    for j in range(3):
        at = 32 + 12 + 6 * j
        part = jnp.where(col % 2 == 1, recv0[at : at + 6, :], recv1[at : at + 6, :])
        for i in range(16):
            edge_ref[j * 16 + i] = jnp.where(ids >= 120, right(part, 120 - i * 8), 0.0)
    scratch = (picked, natural, sums, spread)
    send_frames(
        row_ref, edge_ref, masked_ref, (early_ref, late_ref), (rows_ref, cols_ref, count_ref),
        send_ref, band_ref, scratch, copies,
    )


def unpack(refs, pick_ref, inverse_ref):
    lane = lane_ids(1)
    group = lane % 64 // 8
    device = jnp.zeros((1, LANES), jnp.int32)
    target = jnp.zeros((1, LANES), F32)
    low = lax.broadcasted_iota(jnp.int32, (8, LANES), 0) < 4
    for b, (c, ref, at) in enumerate(blocks(refs)):
        device = jnp.where(group == b, c, device)
        target = jnp.where(group == b, right(ref[at + 39 : at + 40, :], 8 * b), target)
        parts = []
        for g in range(12):
            first = at + 40 + 8 * (g // 2)
            part = ref[first : first + 8, :]
            part = pltpu.roll(part, 4, 0) if g % 2 else part
            parts.append(jnp.where(low, part, 0.0))
        parts = [jnp.concatenate(parts[3 * d : 3 * d + 3], axis=1) for d in range(4)]
        parts += [left(parts[2], 256), left(parts[1], 320)]
        for d in range(6):
            inverse_ref[d, c] = parts[d]
    own = (device * 8 + lane % 4).astype(F32)
    onward = ((device + 7) % 8 * 8 + 3).astype(F32)
    at = lane % 8
    none = jnp.full((1, LANES), -1.0, F32)
    index = lax.broadcasted_iota(jnp.int32, (64, LANES), 0).astype(F32)
    for j in range(3):
        three = jnp.where((at < 4) == (j == 0), own, none) if j < 2 else none
        four = jnp.where(at == 4 + j, onward, jnp.where(at < 4, own, none) if j == 2 else none)
        for half, wanted in enumerate((jnp.where(lane < 64, target, three), jnp.where(lane < 64, four, none))):
            found = (index == jnp.broadcast_to(wanted, (64, LANES))).astype(F32)
            pick_ref[j, :, half * LANES : (half + 1) * LANES] = found


def row_image(refs, pick_ref):
    parts = []
    for j in range(3):
        rows = [ref[at + first : at + first + 8, :] for first in (8 * j, 24, 32) for _, ref, at in blocks(refs)]
        parts.append(select_sum(pick_ref[j, :, 0:192], jnp.concatenate(rows, axis=0)))
    return jnp.concatenate(parts, axis=1).reshape(8, 8, 384)


def folded(x):
    x = jnp.sum(x, axis=0)
    return x[:, 0:128] + x[:, 128:256] + x[:, 256:384]


def advance(refs, pick_ref, inverse_ref, before_ref, row_ref, image_ref, moment_ref, picked):
    col = lax.axis_index("cols")
    image = row_image(refs, pick_ref)
    flat = image.reshape(64, 384)
    vector = inverse_ref[0].reshape(64, 384) * flat
    for d in range(1, 6):
        vector = vector + inverse_ref[d].reshape(64, 384) * left(flat, 64 * d)
    vector = vector.reshape(8, 8, 384)
    row_ref[...] = vector
    moments = [folded(before_ref[...] * image), folded(vector * image)]
    if moment_ref is not None:
        moment_ref[0], moment_ref[1] = moments
    picked[0:64, :] = flat
    image_ref[...] = picked[pl.ds(pl.multiple_of(col * 8, 8), 8), :]
    return moments


def second_kernel(
    recv0, recv1, recv2, recv3, before_ref, edge_ref, masked_ref, early_ref, late_ref, rows_ref, cols_ref, count_ref,
    send_ref, band_ref, row_ref, image_ref, moment_ref, pick_ref, inverse_ref, *scratch,
):
    unpack((recv0, recv1, recv2, recv3), pick_ref, inverse_ref)
    total = jnp.zeros((1, LANES), F32)
    for _, ref, at in blocks((recv0, recv1, recv2, recv3)):
        total = total + ref[at + 39 : at + 40, :]
    sub = lax.broadcasted_iota(jnp.int32, (8, LANES), 0)
    lane = lax.broadcasted_iota(jnp.int32, (8, LANES), 1)
    moment_ref[2] = jnp.where((sub == 0) & (lane == 8), jnp.broadcast_to(total, (8, LANES)), 0.0)
    advance((recv0, recv1, recv2, recv3), pick_ref, inverse_ref, before_ref, row_ref, image_ref, moment_ref, scratch[0])
    ids_refs = (rows_ref, cols_ref, count_ref)
    tiles_refs = (early_ref, late_ref)
    send_frames(row_ref, edge_ref, masked_ref, tiles_refs, ids_refs, send_ref, band_ref, scratch)


def next_kernel(
    recv0, recv1, recv2, recv3, before_ref, edge_ref, masked_ref, early_ref, late_ref, rows_ref, cols_ref, count_ref,
    pick_ref, inverse_ref, send_ref, band_ref, row_ref, image_ref, moment_ref, *scratch,
):
    advance((recv0, recv1, recv2, recv3), pick_ref, inverse_ref, before_ref, row_ref, image_ref, moment_ref, scratch[0])
    ids_refs = (rows_ref, cols_ref, count_ref)
    tiles_refs = (early_ref, late_ref)
    send_frames(row_ref, edge_ref, masked_ref, tiles_refs, ids_refs, send_ref, band_ref, scratch)


def last_kernel(
    recv0, recv1, recv2, recv3, before_ref, edge_ref, masked_ref, early_ref, late_ref, rows_ref, cols_ref, count_ref,
    pick_ref, inverse_ref, m1_ref, m2_ref, send_ref, band_ref, row_ref, image_ref, *scratch,
):
    moments = advance((recv0, recv1, recv2, recv3), pick_ref, inverse_ref, before_ref, row_ref, image_ref, None, scratch[0])
    known = [m1_ref[2], m1_ref[0], m1_ref[1], m2_ref[0], m2_ref[1]] + moments
    ids_refs = (rows_ref, cols_ref, count_ref)
    tiles_refs = (early_ref, late_ref)
    send_last(row_ref, edge_ref, masked_ref, tiles_refs, ids_refs, known, send_ref, band_ref, scratch)


def onward_terms(edge_ref, start):
    parts = []
    for j in range(3):
        part = start[:, j * LANES : (j + 1) * LANES]
        parts += [part, half_turn(part)]
    ids = lane_ids(6)
    begin = jnp.concatenate(parts, axis=0)
    sums = [jnp.zeros((6, LANES), F32) for _ in range(6)]
    for o in range(BAND):
        shifted = jnp.where(ids >= 127 - o, left(begin, o + 1), 0.0)
        for a in range(6):
            sums[a] = sums[a] + edge_ref[o * 6 + a] * shifted
    sums = [jnp.sum(x, axis=0, keepdims=True) for x in sums]
    low = lane_ids(1) < 64
    return jnp.concatenate(
        [jnp.where(low, half_turn(sums[2 * j]), sums[2 * j + 1]) for j in range(3)], axis=1
    )


def tile_products(tiles_refs, piece_of, count, pack):
    for s in range(8):
        piece = piece_of(s) * (s < count).astype(F32)
        for j in range(3):
            rows = pl.ds(j * LANES, LANES)
            tile = slot_of(tiles_refs, s)
            part = tile[rows, 0:LANES] * piece[:, 0:LANES]
            part = part + tile[rows, LANES : 2 * LANES] * piece[:, LANES : 2 * LANES]
            part = part + tile[rows, 2 * LANES : 384] * piece[:, 2 * LANES : 384]
            pack[8 * j + s : 8 * j + s + 1, :] = jnp.sum(part.T, axis=0, keepdims=True)


def cols_kernel(recv_ref, early_ref, late_ref, row_ref, edge_ref, band_ref, cols_ref, count_ref, *rest):
    extra_ref, rows_ref = rest[:2] if len(rest) == 3 else (None, None)
    pack = rest[-1]
    frame = lax.axis_index("frames")
    col = lax.axis_index("cols")
    def piece_of(s):
        q = cols_ref[0, s]
        return recv_ref[q // 4, pl.ds(q % 4, 1), :]

    tile_products((early_ref, late_ref), piece_of, count_ref[0, 0], pack)
    total = recv_ref[0]
    for f in range(1, 32):
        total = total + recv_ref[f]
    terms = pltpu.roll(total, 4, 0) + band_ref[...]
    here = (col > 0).astype(F32)
    there = ((col == 0) & (frame < 31)).astype(F32)
    start = row_ref[col][0:1] * here + recv_ref[jnp.minimum(frame + 1, 31)][0:1] * there
    onward = onward_terms(edge_ref, start)
    for j in range(3):
        lanes = slice(j * LANES, (j + 1) * LANES)
        pack[24 + 4 * j : 28 + 4 * j, :] = terms[0:4, lanes]
        pack[36 + j : 37 + j, :] = onward[:, lanes]
    misc = jnp.zeros((1, LANES), F32)
    if extra_ref is not None:
        misc = extra_ref[48:49, :]
        for s in range(8):
            r = rows_ref[0, s]
            misc = jnp.where(lane_ids(1) == s, ((r // 4) * 8 + r % 4).astype(F32), misc)
    pack[39:40, :] = misc

    if extra_ref is not None:
        pack[40:88, :] = extra_ref[0:48, :]


def finish_kernel(
    recv_ref, early_ref, late_ref, row_ref, edge_ref, band_ref, cols_ref, count_ref, rows_ref,
    send_ref, known_ref, mine_ref, pack, columns,
):
    frame = lax.axis_index("frames")
    col = lax.axis_index("cols")
    lane = lane_ids(1)
    misc = [recv_ref[f, 39:40, :] for f in range(32)]
    total = misc[0]
    for x in misc[1:]:
        total = total + x
    known_ref[...] = jnp.broadcast_to(total, (8, LANES))
    halves = []
    for h in range(2):
        tags = jnp.zeros((1, LANES), F32)
        for i in range(16):
            tags = jnp.where(lane // 8 == i, right(misc[16 * h + i], 8 * i), tags)
        halves.append(tags)
    tags = jnp.concatenate(halves, axis=1)
    products = jnp.concatenate(
        [recv_ref[:, 8 * j : 8 * j + 8, :].reshape(256, LANES) for j in range(3)], axis=1
    )

    at = lax.broadcasted_iota(jnp.int32, (256, 256), 0)
    wanted = ((at // 8) * 4 + at % 4).astype(F32)
    sums = select_sum((wanted == jnp.broadcast_to(tags, (256, 256))).astype(F32), products)
    columns[...] = sums
    low = lax.broadcasted_iota(jnp.int32, (8, LANES), 0) < 4
    quad = jnp.zeros((8, LANES), F32)
    for f in range(32):
        here = sums[8 * f : 8 * f + 8]
        quad = quad + jnp.where(low, here[:, 0:128], here[:, 128:256]) * recv_ref[f, 24:32, :]
        quad = quad + jnp.where(low, here[:, 256:384] * recv_ref[f, 32:40, :], 0.0)
    quad = jnp.sum(quad, axis=0, keepdims=True)
    for f in range(31):
        for j in range(3):
            quad = quad + recv_ref[f, 36 + j : 37 + j, :] * recv_ref[f + 1, 24 + 4 * j : 25 + 4 * j, :]
    quad = quad + quad + jnp.where(lane == 15, total, 0.0)

    mine = columns[pl.ds(pl.multiple_of(frame * 8, 8), 8), :]
    mine_ref[...] = mine + band_ref[...]
    before = jnp.maximum(frame - 1, 0)
    for j in range(3):
        lanes = slice(j * LANES, (j + 1) * LANES)
        edge = recv_ref[before, 36 + j : 37 + j, :] * (frame > 0).astype(F32)
        mine_ref[0:1, lanes] = mine_ref[0:1, lanes] + edge
    here = (col > 0).astype(F32)
    there = ((col == 0) & (frame < 31)).astype(F32)
    after = jnp.minimum(frame + 1, 31)

    def row_of(f, i):
        return jnp.concatenate([recv_ref[f, pl.ds(24 + 4 * j + i, 1), :] for j in range(3)], axis=1)

    onward = onward_terms(edge_ref, row_ref[col][0:1] * here + row_of(after, 0) * there)
    empty = jnp.where(lax.broadcasted_iota(jnp.int32, (16, LANES), 0) == 12, quad, 0.0)
    for c in range(8):
        send_ref[c] = empty
    for j in range(3):
        send_ref[(col + 7) % 8, 4 * j + 3 : 4 * j + 4, :] = onward[:, j * LANES : (j + 1) * LANES]

    def piece_of(s):
        q = cols_ref[0, s]
        return row_of(q // 4, q % 4)

    tile_products((early_ref, late_ref), piece_of, count_ref[0, 0], pack)
    for s in range(8):
        r = rows_ref[0, s]
        for j in range(3):
            send_ref[r // 4, pl.ds(4 * j + r % 4, 1), :] += pack[8 * j + s : 8 * j + s + 1, :]


def end_kernel(
    recv_ref, mine_ref, known_ref, right_ref, v0, v1, v2, v3, w0, w1, w2, solution_ref, residual_ref, scratch
):
    col = lax.axis_index("cols")
    total = recv_ref[0]
    for c in range(1, 8):
        total = total + recv_ref[c]
    parts = [total[0:8], pltpu.roll(total[0:8], 4, 0), total[8:16]]
    last = jnp.concatenate(parts, axis=1) + mine_ref[...]
    known = known_ref[0:1, :]
    mu = [jnp.broadcast_to(known[:, 8 + i : 9 + i], (1, LANES)) for i in range(7)]
    mu.append(jnp.broadcast_to(jnp.sum(total[12:13], axis=1, keepdims=True), (1, LANES)))
    zero = jnp.zeros((1, LANES), F32)
    one = zero + 1.0

    def form(left_side, shift):
        value = zero
        for i in range(len(left_side)):
            for k in range(i, len(left_side)):
                term = left_side[i] * left_side[k]
                value = value + (term if i == k else term + term) * mu[i + k + shift]
        return value

    def ratio(top, bottom):
        return jnp.where(top == 0.0, 0.0, top / jnp.where(top == 0.0, one, bottom))

    direction, residual, solution = [one], [one], []
    gamma = mu[0]
    for it in range(ITERS):
        alpha = ratio(gamma, form(direction, 0) + form(direction, 1))
        solution = solution + [zero] * (len(direction) - len(solution))
        solution = [x + alpha * p for x, p in zip(solution, direction)]
        image = [p + q for p, q in zip(direction + [zero], [zero] + direction)]
        residual = residual + [zero] * (len(image) - len(residual))
        residual = [r - alpha * y for r, y in zip(residual, image)]
        if it + 1 < ITERS:
            fresh = form(residual, 0)
            beta = ratio(fresh, gamma)
            direction = direction + [zero] * (len(residual) - len(direction))
            direction = [r + beta * p for r, p in zip(residual, direction)]
            gamma = fresh

    def wide(x):
        return jnp.concatenate([x, x, x], axis=1)

    total = wide(solution[0]) * v0[col]
    for x, ref in zip(solution[1:], (v1, v2, v3)):
        total = total + wide(x) * ref[col]
    store_as_natural(solution_ref, total)
    total = wide(residual[4]) * last
    for x, ref in zip(residual[1:4], (w0, w1, w2)):
        total = total + wide(x) * ref[...]
    store_as_natural(scratch, total)
    residual_ref[...] = scratch[0:6, :] + jnp.concatenate([residual[0]] * 2, axis=1) * right_ref[...]


VM = pl.BlockSpec(memory_space=pltpu.VMEM)
SM = pl.BlockSpec(memory_space=pltpu.SMEM)
HB = pl.BlockSpec(memory_space=pltpu.HBM)


def shape(*dims, kind=F32):
    return jax.ShapeDtypeStruct(dims, kind)


def call(kernel, specs, outs, scratch, name):
    return pl.pallas_call(
        kernel,
        in_specs=specs,
        out_specs=[VM] * len(outs),
        out_shape=outs,
        scratch_shapes=[pltpu.VMEM(s, F32) if isinstance(s, tuple) else s for s in scratch],
        compiler_params=pltpu.CompilerParams(vmem_limit_bytes=24 * 1024 * 1024),
        name=name,
    )


def per_device(right_side, diag_blocks, band_blocks, reach, tiles, tile_rows, tile_cols, tile_count):
    def exchange(x, axis):
        return lax.all_to_all(x, axis, 0, 0, tiled=True)

    def share(x):
        chips = lax.axis_size("cols") // 2
        swap = [(i, i ^ 1) for i in range(2 * chips)]
        pair = jnp.concatenate([x, lax.ppermute(x, "cols", swap)], axis=0)
        others = []
        for d in range(1, chips):
            ahead = [(i, (i + 2 * d) % (2 * chips)) for i in range(2 * chips)]
            others.append(lax.ppermute(pair, "cols", ahead))
        return [pair, *others]

    def in_hbm(x):
        return pltpu.with_memory_space_constraint(x, pltpu.HBM)

    sem = pltpu.SemaphoreType.DMA(())
    stored = in_hbm(tiles.reshape(tiles.shape[2:]))
    inputs = (right_side, diag_blocks, jnp.transpose(band_blocks, (1, 2, 0, 3)), reach.reshape(1, -1))
    inputs += (tile_rows.reshape(1, 8), tile_cols.reshape(1, 8))
    send, masked, extra, *ids = call(
        start_kernel,
        [HB] * 6,
        [shape(32, LANES), shape(48, 6, 256), shape(56, LANES)]
        + [shape(1, 8, kind=jnp.int32)] * 2,
        [(6, 256), (6, 6, 256), (6, 6, 8, 256), pltpu.VMEM((1, 256), jnp.int32), (8, 384)]
        + [sem] * 6,
        "start",
    )(*[in_hbm(x) for x in inputs])
    ids.append(tile_count)
    recv = share(send)
    (early,) = call(load_kernel, [HB], [shape(EARLY, 384, 384)], [sem] * EARLY, "load")(stored)
    frames_out = [shape(32, 8, 384), shape(8, 384), shape(8, 8, 384)]
    scratch = [(LANES, 384), (8, 256), (8, 256), (384, 512)]
    send, band, row, edges, late = call(
        first_kernel,
        [VM] * 5 + [HB, VM] + [SM] * 3,
        frames_out + [shape(48, 6, LANES), shape(8 - EARLY, 384, 384)],
        scratch + [sem] * (8 - EARLY),
        "first",
    )(*recv, masked, stored, early, *ids)
    vectors, images, moments = [row], [], []
    for it in range(ITERS - 1):
        recv = exchange(send, "frames")
        (send,) = call(
            cols_kernel,
            [VM] * 6 + [SM] * 2 + ([VM, SM] if it == 0 else []),
            [shape(88 if it == 0 else 40, LANES)],
            [],
            "products",
        )(recv, early, late, row, edges, band, *ids[1:], *((extra, ids[0]) if it == 0 else ()))
        recv = share(send)
        given = (*recv, row, edges, masked, early, late, *ids)
        specs = [VM] * 9 + [SM] * 3
        if it == 0:
            send, band, row, image, moment, pick, inverse = call(
                second_kernel,
                specs,
                frames_out
                + [shape(8, 384), shape(3, 8, LANES), shape(3, 64, 256), shape(6, 8, 8, 384)],
                scratch,
                "second",
            )(*given)
            moments.append(moment)
        elif it + 2 < ITERS:
            send, band, row, image, moment = call(
                next_kernel,
                specs + [VM] * 2,
                frames_out + [shape(8, 384), shape(2, 8, LANES)],
                scratch,
                "next",
            )(*given, pick, inverse)
            moments.append(moment)
        else:
            send, band, row, image = call(
                last_kernel,
                specs + [VM] * 4,
                [shape(32, 40, LANES), shape(8, 384), shape(8, 8, 384), shape(8, 384)],
                scratch + [(40, LANES)],
                "last",
            )(*given, pick, inverse, *moments)
        vectors.append(row)
        images.append(image)
    recv = exchange(send, "frames")
    send, known, mine = call(
        finish_kernel,
        [VM] * 6 + [SM] * 3,
        [shape(8, 16, LANES), shape(8, LANES), shape(8, 384)],
        [(24, LANES), (256, 384)],
        "finish",
    )(recv, early, late, row, edges, band, *ids[1:], ids[0])
    recv = exchange(send, "cols")
    return tuple(
        call(end_kernel, [VM] * 11, [shape(6, 256), shape(6, 256)], [(8, 256)], "end")(
            recv, mine, known, right_side, *vectors, *images
        )
    )


def solution(mesh):
    return jax.shard_map(
        per_device,
        mesh=mesh,
        in_specs=(
            P(None, ROWS),
            P(None, None, ROWS),
            P(None, None, None, ROWS),
            P(ROWS),
            P("frames", "cols", None, None, None),
            P("frames", "cols", None),
            P("frames", "cols", None),
            P("frames", "cols"),
        ),
        out_specs=(P(None, ROWS), P(None, ROWS)),
        check_vma=False,
    )
```

```python
import jax
import jax.numpy as jnp
from jax import lax
from jax.experimental import pallas as pl
from jax.experimental.pallas import tpu as pltpu
from jax.sharding import PartitionSpec as P


ITERS = 4
BAND = 8
LANES = 128
F32 = jnp.float32
ROWS = ("frames", "cols")
EARLY = 5


def lane_ids(rows):
    return lax.broadcasted_iota(jnp.int32, (rows, LANES), 1)


def half_turn(x):
    return pltpu.roll(x, 64, 1)


def left(x, by):
    return pltpu.roll(x, (x.shape[1] - by) % x.shape[1], 1) if by % x.shape[1] else x


def right(x, by):
    return pltpu.roll(x, by % x.shape[1], 1) if by % x.shape[1] else x


def store_as_tiles(ref, base, x):
    low = lane_ids(1) < 64
    for u in range(2):
        part = x[:, u * LANES : (u + 1) * LANES]
        turned = half_turn(part)
        for j in range(3):
            lanes = pl.ds(j * LANES, LANES)
            ref[pl.ds(base + 2 * u, 1), lanes] = jnp.where(
                low, part[2 * j : 2 * j + 1], turned[2 * j + 1 : 2 * j + 2]
            )
            ref[pl.ds(base + 2 * u + 1, 1), lanes] = jnp.where(
                low, turned[2 * j : 2 * j + 1], part[2 * j + 1 : 2 * j + 2]
            )


def store_as_natural(ref, t):
    low = lane_ids(1) < 64
    for j in range(3):
        part = t[:, j * LANES : (j + 1) * LANES]
        turned = half_turn(part)
        for u in range(2):
            lanes = pl.ds(u * LANES, LANES)
            ref[pl.ds(2 * j, 1), lanes] = jnp.where(
                low, part[2 * u : 2 * u + 1], turned[2 * u + 1 : 2 * u + 2]
            )
            ref[pl.ds(2 * j + 1, 1), lanes] = jnp.where(
                low, turned[2 * u : 2 * u + 1], part[2 * u + 1 : 2 * u + 2]
            )


def start_kernel(
    right_hbm, diag_hbm, band_hbm, reach_hbm, rows_hbm, cols_hbm,
    send_ref, masked_ref, rows_ref, cols_ref,
    right_ref, diag_ref, band_ref, reach_ref, pack, *sems,
):
    copies = [
        pltpu.make_async_copy(source, to, sem)
        for source, to, sem in zip(
            (diag_hbm, right_hbm, reach_hbm, band_hbm, rows_hbm, cols_hbm),
            (diag_ref, right_ref, reach_ref, band_ref, rows_ref, cols_ref),
            sems,
        )
    ]
    for copy in copies:
        copy.start()
    for copy in copies[:2]:
        copy.wait()
    sub = lax.broadcasted_iota(jnp.int32, (6, 256), 0)
    matrix = [diag_ref[a] for a in range(6)]
    inverse = [(sub == a).astype(F32) for a in range(6)]
    for p in range(6):
        pivot = matrix[p][p : p + 1]
        matrix[p] = matrix[p] / pivot
        inverse[p] = inverse[p] / pivot
        for a in range(6):
            if a != p:
                factor = matrix[a][p : p + 1]
                matrix[a] = matrix[a] - factor * matrix[p]
                inverse[a] = inverse[a] - factor * inverse[p]
    residual = right_ref[...]
    first = jnp.concatenate(
        [jnp.sum(inverse[a] * residual, axis=0, keepdims=True) for a in range(6)], axis=0
    )
    store_as_tiles(pack, 0, first)
    for j in range(3):
        send_ref[4 * j : 4 * j + 4, :] = pack[0:4, j * LANES : (j + 1) * LANES]
    for d in range(4):
        turned = jnp.concatenate(
            [inverse[a][(a + d) % 6 : (a + d) % 6 + 1] for a in range(6)], axis=0
        )
        store_as_tiles(pack, 0, turned)
        for j in range(3):
            at = 32 + (3 * d + j) * 4
            send_ref[at : at + 4, :] = pack[0:4, j * LANES : (j + 1) * LANES]
    product = first * residual
    product = jnp.sum(product[:, 0:LANES] + product[:, LANES:256], axis=0, keepdims=True)
    product = jnp.sum(product, axis=1, keepdims=True)
    moment = jnp.where(lane_ids(1) == 8, product, 0.0)
    for copy in copies[2:6]:
        copy.wait()
    reach = reach_ref[...]
    for o in range(BAND):
        keep = (reach > o).astype(F32)
        for a in range(6):
            masked_ref[o * 6 + a] = band_ref[a, :, o, :] * keep
    ids = lane_ids(6)
    for j in range(3):
        packed = jnp.zeros((6, LANES), F32)
        for i in range(16):
            block = masked_ref[j * 16 + i, :, LANES : 2 * LANES]
            packed = jnp.where(ids // 8 == i, right(block, i * 8 + 8), packed)
        send_ref[12 + 6 * j : 18 + 6 * j, :] = packed
    rows = rows_ref[...]
    send_ref[30:31, :] = moment
    send_ref[30:31, 0:8] = ((rows // 4) * 8 + rows % 4).astype(F32)
    send_ref[31:32, :] = jnp.zeros((1, LANES), F32)


def blocks(refs):
    col = lax.axis_index("cols")
    rows = refs[0].shape[0] // 2
    return [
        (((col // 2 + 4 - d) % 4) * 2 + (col + i) % 2, refs[d], i * rows)
        for d in range(4)
        for i in range(2)
    ]


def load_kernel(tiles_hbm, tiles_ref, *sems):
    copies = [pltpu.make_async_copy(tiles_hbm.at[s], tiles_ref.at[s], sems[s]) for s in range(EARLY)]
    for copy in copies:
        copy.start()
    for copy in copies:
        copy.wait()


def own_edge(edge_ref, row_ref, col):
    last = row_ref[(col + 7) % 8][3:4]
    values = []
    for j in range(3):
        part = last[:, j * LANES : (j + 1) * LANES]
        values += [half_turn(part), part]
    total = jnp.zeros((6, LANES), F32)
    for o in range(BAND):
        z = edge_ref[o * 6] * values[0]
        for a in range(1, 6):
            z = z + edge_ref[o * 6 + a] * values[a]
        total = total + right(z, o + 1)
    total = jnp.where(lane_ids(6) < 8, total, 0.0)
    turned = half_turn(total)
    low = lane_ids(1) < 64
    return jnp.concatenate(
        [jnp.where(low, total[2 * j : 2 * j + 1], turned[2 * j + 1 : 2 * j + 2]) for j in range(3)],
        axis=1,
    )


def bfloat16_parts(x):
    high = x.astype(jnp.bfloat16)
    rest = x - high.astype(F32)
    middle = rest.astype(jnp.bfloat16)
    return high, middle, (rest - middle.astype(F32)).astype(jnp.bfloat16)


def select_sum(pick, x):
    pick = pick.astype(jnp.bfloat16)
    high, middle, low = [
        jnp.dot(pick, part, preferred_element_type=F32) for part in bfloat16_parts(x)
    ]
    return low + middle + high


def slot_of(tiles_refs, s):
    return tiles_refs[0].at[s] if s < EARLY else tiles_refs[1].at[s - EARLY]


def transposed_products(row_ref, tiles_refs, ids_refs, picked, spread, copies=()):
    rows_ref, _, count_ref = ids_refs
    count = count_ref[0, 0]
    picked[...] = jnp.zeros((LANES, 384), F32)
    for s in range(8):
        r = rows_ref[0, s]
        picked[s : s + 1, :] = row_ref[r // 4, pl.ds(r % 4, 1), :]
    for i, part in enumerate(bfloat16_parts(picked[4:8, :])):
        picked[8 + 4 * i : 12 + 4 * i, :] = part.astype(F32)
    upright = [picked[:, j * LANES : (j + 1) * LANES].T for j in range(3)]
    at = lax.broadcasted_iota(jnp.int32, (LANES, 512), 0)
    to = lax.broadcasted_iota(jnp.int32, (LANES, 512), 1)
    ones = ((at >= 8) & (at < 20) & (at % 4 == to // LANES)).astype(jnp.bfloat16)
    for j in range(3):
        spread[j * LANES : (j + 1) * LANES, :] = jnp.dot(
            upright[j].astype(jnp.bfloat16), ones, preferred_element_type=F32
        )
    products = []
    for s in range(8):
        if copies and s >= EARLY:
            copies[s - EARLY].wait()
        tile = slot_of(tiles_refs, s)
        sums = [[None] * 3, [None] * 3]
        for i in range(48):
            if s < 4:
                column = upright[i // 16][8 * (i % 16) : 8 * (i % 16) + 8, s : s + 1]
                column = jnp.broadcast_to(column, (8, LANES))
            else:
                column = spread[8 * i : 8 * i + 8, (s - 4) * LANES : (s - 3) * LANES]
            for j in range(3):
                part = tile[8 * i : 8 * i + 8, j * LANES : (j + 1) * LANES] * column
                before = sums[i % 2][j]
                sums[i % 2][j] = part if before is None else before + part
        total = jnp.concatenate(
            [jnp.sum(x + y, axis=0, keepdims=True) for x, y in zip(*sums)], axis=1
        )
        products.append(total * (s < count).astype(F32))
    return products


def edge_terms(row_ref, edge_ref):
    frame = lax.axis_index("frames")
    col = lax.axis_index("cols")
    edge = own_edge(edge_ref, row_ref, col)
    cross = ((col == 0) & (frame < 31)).astype(F32)
    return edge * (col > 0).astype(F32), edge * cross


def band_terms(row_ref, masked_ref, edge, out_ref, natural, sums):
    col = lax.axis_index("cols")
    store_as_natural(natural, row_ref[col])
    lane = lax.broadcasted_iota(jnp.int32, (6, 256), 1)
    vector = natural[0:6, :]
    total = jnp.zeros((6, 256), F32)
    ahead = [jnp.zeros((6, 256), F32) for _ in range(6)]
    for o in range(BAND):
        shifted = jnp.where(lane < 255 - o, left(vector, o + 1), 0.0)
        z = jnp.zeros((6, 256), F32)
        for a in range(6):
            block = masked_ref[o * 6 + a]
            z = z + block * natural[a : a + 1, :]
            ahead[a] = ahead[a] + block * shifted
        total = total + jnp.where(lane > o, right(z, o + 1), 0.0)
    for a in range(6):
        sums[a : a + 1, :] = jnp.sum(ahead[a], axis=0, keepdims=True)
    out_ref[...] = jnp.zeros((8, 384), F32)
    store_as_tiles(out_ref, 0, total + sums[0:6, :])
    out_ref[0:1, :] = out_ref[0:1, :] + edge


def send_frames(row_ref, edge_ref, masked_ref, tiles_refs, ids_refs, send_ref, band_ref, scratch, copies=()):
    picked, natural, sums, spread = scratch
    col = lax.axis_index("cols")
    sub = lax.broadcasted_iota(jnp.int32, (8, 384), 0)
    chunk = jnp.where(sub < 4, row_ref[col], 0.0)
    for f in range(32):
        send_ref[f] = chunk
    mine, onward = edge_terms(row_ref, edge_ref)
    send_ref[jnp.minimum(lax.axis_index("frames") + 1, 31), 4:5, :] = onward
    band_terms(row_ref, masked_ref, mine, band_ref, natural, sums)
    for s, product in enumerate(transposed_products(row_ref, tiles_refs, ids_refs, picked, spread, copies)):
        q = ids_refs[1][0, s]
        send_ref[q // 4, pl.ds(4 + q % 4, 1), :] += product


def send_last(row_ref, edge_ref, masked_ref, tiles_refs, ids_refs, known, send_ref, band_ref, scratch):
    picked, natural, sums, spread, pack = scratch
    col = lax.axis_index("cols")
    mine, onward = edge_terms(row_ref, edge_ref)
    band_terms(row_ref, masked_ref, mine, band_ref, natural, sums)
    own = row_ref[col]
    products = transposed_products(row_ref, tiles_refs, ids_refs, picked, spread)
    for j in range(3):
        lanes = slice(j * LANES, (j + 1) * LANES)
        for s in range(8):
            pack[8 * j + s : 8 * j + s + 1, :] = products[s][:, lanes]
        pack[24 + 4 * j : 28 + 4 * j, :] = own[0:4, lanes]
        pack[36 + j : 37 + j, :] = onward[:, lanes]
    part = own * band_ref[...]
    quad = jnp.sum(part[:, 0:128] + part[:, 128:256] + part[:, 256:384], axis=0, keepdims=True)
    part = own[0:1] * mine
    quad = quad + part[:, 0:128] + part[:, 128:256] + part[:, 256:384]
    rows = [jnp.sum(x, axis=0, keepdims=True) for x in known] + [quad]
    lane = lax.broadcasted_iota(jnp.int32, (8, LANES), 1)
    sub = lax.broadcasted_iota(jnp.int32, (8, LANES), 0)
    totals = jnp.sum(jnp.concatenate(rows, axis=0), axis=1, keepdims=True)
    misc = jnp.sum(jnp.where(lane == sub + 8, totals, 0.0), axis=0, keepdims=True)
    for s in range(8):
        misc = jnp.where(lane_ids(1) == s, ids_refs[1][0, s].astype(F32), misc)
    pack[39:40, :] = misc
    whole = pack[...]
    for f in range(32):
        send_ref[f] = whole


def first_kernel(
    recv0, recv1, recv2, recv3, masked_ref, tiles_hbm, early_ref, rows_ref, cols_ref, count_ref,
    send_ref, band_ref, row_ref, edge_ref, late_ref, picked, natural, sums, spread, *sems,
):
    copies = [
        pltpu.make_async_copy(tiles_hbm.at[EARLY + s], late_ref.at[s], sems[s])
        for s in range(8 - EARLY)
    ]
    for copy in copies:
        copy.start()
    col = lax.axis_index("cols")
    row_ref[...] = jnp.zeros((8, 8, 384), F32)
    for c, ref, at in blocks((recv0, recv1, recv2, recv3)):
        for j in range(3):
            row_ref[c, 0:4, j * LANES : (j + 1) * LANES] = ref[at + 4 * j : at + 4 * j + 4, :]
    ids = lane_ids(6)
    for j in range(3):
        at = 80 + 12 + 6 * j
        part = jnp.where(col % 2 == 1, recv0[at : at + 6, :], recv1[at : at + 6, :])
        for i in range(16):
            edge_ref[j * 16 + i] = jnp.where(ids >= 120, right(part, 120 - i * 8), 0.0)
    scratch = (picked, natural, sums, spread)
    send_frames(
        row_ref, edge_ref, masked_ref, (early_ref, late_ref), (rows_ref, cols_ref, count_ref),
        send_ref, band_ref, scratch, copies,
    )


def layout_kernel(recv0, recv1, recv2, recv3, _, pick_ref, inverse_ref, moment_ref):
    refs = (recv0, recv1, recv2, recv3)
    total = jnp.zeros((1, LANES), F32)
    lane = lane_ids(1)
    group = lane % 64 // 8
    device = jnp.zeros((1, LANES), jnp.int32)
    target = jnp.zeros((1, LANES), F32)
    low = lax.broadcasted_iota(jnp.int32, (8, LANES), 0) < 4
    for b, (c, ref, at) in enumerate(blocks(refs)):
        device = jnp.where(group == b, c, device)
        target = jnp.where(group == b, right(ref[at + 30 : at + 31, :], 8 * b), target)
        total = total + ref[at + 30 : at + 31, :]
        parts = []
        for g in range(12):
            first = at + 32 + 8 * (g // 2)
            part = ref[first : first + 8, :]
            part = pltpu.roll(part, 4, 0) if g % 2 else part
            parts.append(jnp.where(low, part, 0.0))
        parts = [jnp.concatenate(parts[3 * d : 3 * d + 3], axis=1) for d in range(4)]
        parts += [left(parts[2], 256), left(parts[1], 320)]
        for d in range(6):
            inverse_ref[d, c] = parts[d]
    own = (device * 8 + lane % 4).astype(F32)
    onward = ((device + 7) % 8 * 8 + 3).astype(F32)
    at = lane % 8
    none = jnp.full((1, LANES), -1.0, F32)
    index = lax.broadcasted_iota(jnp.int32, (64, LANES), 0).astype(F32)
    for j in range(3):
        three = jnp.where((at < 4) == (j == 0), own, none) if j < 2 else none
        four = jnp.where(at == 4 + j, onward, jnp.where(at < 4, own, none) if j == 2 else none)
        for half, wanted in enumerate((jnp.where(lane < 64, target, three), jnp.where(lane < 64, four, none))):
            found = (index == jnp.broadcast_to(wanted, (64, LANES))).astype(F32)
            pick_ref[j, :, half * LANES : (half + 1) * LANES] = found
    sub = lax.broadcasted_iota(jnp.int32, (8, LANES), 0)
    total = jnp.where(lane == 8, total, 0.0)
    moment_ref[...] = jnp.where(sub == 0, jnp.broadcast_to(total, (8, LANES)), 0.0)


def row_image(refs, pick_ref):
    places = blocks(refs)

    def rows_from(first):
        return bfloat16_parts(
            jnp.concatenate([ref[at + first : at + first + 8, :] for _, ref, at in places], axis=0)
        )

    three, four = rows_from(24), rows_from(32)
    parts = []
    for j in range(3):
        pick = pick_ref[j, :, 0:192].astype(jnp.bfloat16)
        high, middle, low = [
            jnp.dot(pick, jnp.concatenate(x, axis=0), preferred_element_type=F32)
            for x in zip(rows_from(8 * j), three, four)
        ]
        parts.append(low + middle + high)
    return jnp.concatenate(parts, axis=1).reshape(8, 8, 384)


def folded(x):
    x = jnp.sum(x, axis=0)
    return x[:, 0:128] + x[:, 128:256] + x[:, 256:384]


def advance(refs, pick_ref, inverse_ref, before_ref, row_ref, image_ref, moment_ref, picked):
    col = lax.axis_index("cols")
    image = row_image(refs, pick_ref)
    flat = image.reshape(64, 384)
    vector = inverse_ref[0].reshape(64, 384) * flat
    for d in range(1, 6):
        vector = vector + inverse_ref[d].reshape(64, 384) * left(flat, 64 * d)
    vector = vector.reshape(8, 8, 384)
    row_ref[...] = vector
    moments = [folded(before_ref[...] * image), folded(vector * image)]
    if moment_ref is not None:
        moment_ref[0], moment_ref[1] = moments
    picked[0:64, :] = flat
    image_ref[...] = picked[pl.ds(pl.multiple_of(col * 8, 8), 8), :]
    return moments


def next_kernel(
    recv0, recv1, recv2, recv3, before_ref, edge_ref, masked_ref, early_ref, late_ref, rows_ref, cols_ref, count_ref,
    pick_ref, inverse_ref, send_ref, band_ref, row_ref, image_ref, moment_ref, *scratch,
):
    advance((recv0, recv1, recv2, recv3), pick_ref, inverse_ref, before_ref, row_ref, image_ref, moment_ref, scratch[0])
    ids_refs = (rows_ref, cols_ref, count_ref)
    tiles_refs = (early_ref, late_ref)
    send_frames(row_ref, edge_ref, masked_ref, tiles_refs, ids_refs, send_ref, band_ref, scratch)


def last_kernel(
    recv0, recv1, recv2, recv3, before_ref, edge_ref, masked_ref, early_ref, late_ref, rows_ref, cols_ref, count_ref,
    pick_ref, inverse_ref, m0_ref, m1_ref, m2_ref, send_ref, band_ref, row_ref, image_ref, *scratch,
):
    moments = advance((recv0, recv1, recv2, recv3), pick_ref, inverse_ref, before_ref, row_ref, image_ref, None, scratch[0])
    known = [m0_ref[...], m1_ref[0], m1_ref[1], m2_ref[0], m2_ref[1]] + moments
    ids_refs = (rows_ref, cols_ref, count_ref)
    tiles_refs = (early_ref, late_ref)
    send_last(row_ref, edge_ref, masked_ref, tiles_refs, ids_refs, known, send_ref, band_ref, scratch)


def onward_terms(edge_ref, start):
    parts = []
    for j in range(3):
        part = start[:, j * LANES : (j + 1) * LANES]
        parts += [part, half_turn(part)]
    ids = lane_ids(6)
    begin = jnp.concatenate(parts, axis=0)
    sums = [jnp.zeros((6, LANES), F32) for _ in range(6)]
    for o in range(BAND):
        shifted = jnp.where(ids >= 127 - o, left(begin, o + 1), 0.0)
        for a in range(6):
            sums[a] = sums[a] + edge_ref[o * 6 + a] * shifted
    sums = [jnp.sum(x, axis=0, keepdims=True) for x in sums]
    low = lane_ids(1) < 64
    return jnp.concatenate(
        [jnp.where(low, half_turn(sums[2 * j]), sums[2 * j + 1]) for j in range(3)], axis=1
    )


def tile_products(tiles_refs, piece_of, count, pack):
    for s in range(8):
        piece = piece_of(s) * (s < count).astype(F32)
        for j in range(3):
            rows = pl.ds(j * LANES, LANES)
            tile = slot_of(tiles_refs, s)
            part = tile[rows, 0:LANES] * piece[:, 0:LANES]
            part = part + tile[rows, LANES : 2 * LANES] * piece[:, LANES : 2 * LANES]
            part = part + tile[rows, 2 * LANES : 384] * piece[:, 2 * LANES : 384]
            pack[8 * j + s : 8 * j + s + 1, :] = jnp.sum(part.T, axis=0, keepdims=True)


def cols_kernel(recv_ref, early_ref, late_ref, row_ref, edge_ref, band_ref, cols_ref, count_ref, pack):
    frame = lax.axis_index("frames")
    col = lax.axis_index("cols")
    def piece_of(s):
        q = cols_ref[0, s]
        return recv_ref[q // 4, pl.ds(q % 4, 1), :]

    tile_products((early_ref, late_ref), piece_of, count_ref[0, 0], pack)
    total = recv_ref[0]
    for f in range(1, 32):
        total = total + recv_ref[f]
    terms = pltpu.roll(total, 4, 0) + band_ref[...]
    here = (col > 0).astype(F32)
    there = ((col == 0) & (frame < 31)).astype(F32)
    start = row_ref[col][0:1] * here + recv_ref[jnp.minimum(frame + 1, 31)][0:1] * there
    onward = onward_terms(edge_ref, start)
    for j in range(3):
        lanes = slice(j * LANES, (j + 1) * LANES)
        pack[24 + 4 * j : 28 + 4 * j, :] = terms[0:4, lanes]
        pack[36 + j : 37 + j, :] = onward[:, lanes]
    pack[39:40, :] = jnp.zeros((1, LANES), F32)


def finish_kernel(
    recv_ref, early_ref, late_ref, row_ref, edge_ref, band_ref, cols_ref, count_ref, rows_ref,
    send_ref, known_ref, mine_ref, pack, columns,
):
    frame = lax.axis_index("frames")
    col = lax.axis_index("cols")
    lane = lane_ids(1)
    misc = [recv_ref[f, 39:40, :] for f in range(32)]
    total = misc[0]
    for x in misc[1:]:
        total = total + x
    known_ref[...] = jnp.broadcast_to(total, (8, LANES))
    halves = []
    for h in range(2):
        tags = jnp.zeros((1, LANES), F32)
        for i in range(16):
            tags = jnp.where(lane // 8 == i, right(misc[16 * h + i], 8 * i), tags)
        halves.append(tags)
    tags = jnp.concatenate(halves, axis=1)
    products = jnp.concatenate(
        [recv_ref[:, 8 * j : 8 * j + 8, :].reshape(256, LANES) for j in range(3)], axis=1
    )

    at = lax.broadcasted_iota(jnp.int32, (256, 256), 0)
    wanted = ((at // 8) * 4 + at % 4).astype(F32)
    sums = select_sum((wanted == jnp.broadcast_to(tags, (256, 256))).astype(F32), products)
    columns[...] = sums
    low = lax.broadcasted_iota(jnp.int32, (8, LANES), 0) < 4
    quad = jnp.zeros((8, LANES), F32)
    for f in range(32):
        here = sums[8 * f : 8 * f + 8]
        quad = quad + jnp.where(low, here[:, 0:128], here[:, 128:256]) * recv_ref[f, 24:32, :]
        quad = quad + jnp.where(low, here[:, 256:384] * recv_ref[f, 32:40, :], 0.0)
    quad = jnp.sum(quad, axis=0, keepdims=True)
    for f in range(31):
        for j in range(3):
            quad = quad + recv_ref[f, 36 + j : 37 + j, :] * recv_ref[f + 1, 24 + 4 * j : 25 + 4 * j, :]
    quad = quad + quad + jnp.where(lane == 15, total, 0.0)

    mine = columns[pl.ds(pl.multiple_of(frame * 8, 8), 8), :]
    mine_ref[...] = mine + band_ref[...]
    before = jnp.maximum(frame - 1, 0)
    for j in range(3):
        lanes = slice(j * LANES, (j + 1) * LANES)
        edge = recv_ref[before, 36 + j : 37 + j, :] * (frame > 0).astype(F32)
        mine_ref[0:1, lanes] = mine_ref[0:1, lanes] + edge
    here = (col > 0).astype(F32)
    there = ((col == 0) & (frame < 31)).astype(F32)
    after = jnp.minimum(frame + 1, 31)

    def row_of(f, i):
        return jnp.concatenate([recv_ref[f, pl.ds(24 + 4 * j + i, 1), :] for j in range(3)], axis=1)

    onward = onward_terms(edge_ref, row_ref[col][0:1] * here + row_of(after, 0) * there)
    empty = jnp.where(lax.broadcasted_iota(jnp.int32, (16, LANES), 0) == 12, quad, 0.0)
    for c in range(8):
        send_ref[c] = empty
    for j in range(3):
        send_ref[(col + 7) % 8, 4 * j + 3 : 4 * j + 4, :] = onward[:, j * LANES : (j + 1) * LANES]

    def piece_of(s):
        q = cols_ref[0, s]
        return row_of(q // 4, q % 4)

    tile_products((early_ref, late_ref), piece_of, count_ref[0, 0], pack)
    for s in range(8):
        r = rows_ref[0, s]
        for j in range(3):
            send_ref[r // 4, pl.ds(4 * j + r % 4, 1), :] += pack[8 * j + s : 8 * j + s + 1, :]


def end_kernel(
    recv_ref, mine_ref, known_ref, right_ref, v0, v1, v2, v3, w0, w1, w2, solution_ref, residual_ref, scratch
):
    col = lax.axis_index("cols")
    total = recv_ref[0]
    for c in range(1, 8):
        total = total + recv_ref[c]
    parts = [total[0:8], pltpu.roll(total[0:8], 4, 0), total[8:16]]
    last = jnp.concatenate(parts, axis=1) + mine_ref[...]
    known = known_ref[0:1, :]
    mu = [jnp.broadcast_to(known[:, 8 + i : 9 + i], (1, LANES)) for i in range(7)]
    mu.append(jnp.broadcast_to(jnp.sum(total[12:13], axis=1, keepdims=True), (1, LANES)))
    zero = jnp.zeros((1, LANES), F32)
    one = zero + 1.0

    def form(left_side, shift):
        value = zero
        for i in range(len(left_side)):
            for k in range(i, len(left_side)):
                term = left_side[i] * left_side[k]
                value = value + (term if i == k else term + term) * mu[i + k + shift]
        return value

    def ratio(top, bottom):
        return jnp.where(top == 0.0, 0.0, top / jnp.where(top == 0.0, one, bottom))

    direction, residual, solution = [one], [one], []
    gamma = mu[0]
    for it in range(ITERS):
        alpha = ratio(gamma, form(direction, 0) + form(direction, 1))
        solution = solution + [zero] * (len(direction) - len(solution))
        solution = [x + alpha * p for x, p in zip(solution, direction)]
        image = [p + q for p, q in zip(direction + [zero], [zero] + direction)]
        residual = residual + [zero] * (len(image) - len(residual))
        residual = [r - alpha * y for r, y in zip(residual, image)]
        if it + 1 < ITERS:
            fresh = form(residual, 0)
            beta = ratio(fresh, gamma)
            direction = direction + [zero] * (len(residual) - len(direction))
            direction = [r + beta * p for r, p in zip(residual, direction)]
            gamma = fresh

    def wide(x):
        return jnp.concatenate([x, x, x], axis=1)

    total = wide(solution[0]) * v0[col]
    for x, ref in zip(solution[1:], (v1, v2, v3)):
        total = total + wide(x) * ref[col]
    store_as_natural(solution_ref, total)
    total = wide(residual[4]) * last
    for x, ref in zip(residual[1:4], (w0, w1, w2)):
        total = total + wide(x) * ref[...]
    store_as_natural(scratch, total)
    residual_ref[...] = scratch[0:6, :] + jnp.concatenate([residual[0]] * 2, axis=1) * right_ref[...]


VM = pl.BlockSpec(memory_space=pltpu.VMEM)
SM = pl.BlockSpec(memory_space=pltpu.SMEM)
HB = pl.BlockSpec(memory_space=pltpu.HBM)


def shape(*dims, kind=F32):
    return jax.ShapeDtypeStruct(dims, kind)


def call(kernel, specs, outs, scratch, name):
    return pl.pallas_call(
        kernel,
        in_specs=specs,
        out_specs=[VM] * len(outs),
        out_shape=outs,
        scratch_shapes=[pltpu.VMEM(s, F32) if isinstance(s, tuple) else s for s in scratch],
        compiler_params=pltpu.CompilerParams(vmem_limit_bytes=24 * 1024 * 1024),
        name=name,
    )


def per_device(right_side, diag_blocks, band_blocks, reach, tiles, tile_rows, tile_cols, tile_count):
    def exchange(x, axis):
        return lax.all_to_all(x, axis, 0, 0, tiled=True)

    def share(x):
        chips = lax.axis_size("cols") // 2
        swap = [(i, i ^ 1) for i in range(2 * chips)]
        pair = jnp.concatenate([x, lax.ppermute(x, "cols", swap)], axis=0)
        others = []
        for d in range(1, chips):
            ahead = [(i, (i + 2 * d) % (2 * chips)) for i in range(2 * chips)]
            others.append(lax.ppermute(pair, "cols", ahead))
        return [pair, *others]

    def in_hbm(x):
        return pltpu.with_memory_space_constraint(x, pltpu.HBM)

    sem = pltpu.SemaphoreType.DMA(())
    stored = in_hbm(tiles.reshape(tiles.shape[2:]))
    inputs = (right_side, diag_blocks, jnp.transpose(band_blocks, (1, 2, 0, 3)), reach.reshape(1, -1))
    inputs += (tile_rows.reshape(1, 8), tile_cols.reshape(1, 8))
    send, masked, *ids = call(
        start_kernel,
        [HB] * 6,
        [shape(80, LANES), shape(48, 6, 256)]
        + [shape(1, 8, kind=jnp.int32)] * 2,
        [(6, 256), (6, 6, 256), (6, 6, 8, 256), pltpu.VMEM((1, 256), jnp.int32), (8, 384)]
        + [sem] * 6,
        "start",
    )(*[in_hbm(x) for x in inputs])
    ids.append(tile_count)
    recv = shared = share(send)
    (early,) = call(load_kernel, [HB], [shape(EARLY, 384, 384)], [sem] * EARLY, "load")(stored)
    frames_out = [shape(32, 8, 384), shape(8, 384), shape(8, 8, 384)]
    scratch = [(LANES, 384), (8, 256), (8, 256), (384, 512)]
    send, band, row, edges, late = call(
        first_kernel,
        [VM] * 5 + [HB, VM] + [SM] * 3,
        frames_out + [shape(48, 6, LANES), shape(8 - EARLY, 384, 384)],
        scratch + [sem] * (8 - EARLY),
        "first",
    )(*recv, masked, stored, early, *ids)
    vectors, images, moments = [row], [], []
    for it in range(ITERS - 1):
        recv = exchange(send, "frames")
        (send,) = call(
            cols_kernel,
            [VM] * 6 + [SM] * 2,
            [shape(40, LANES)],
            [],
            "products",
        )(recv, early, late, row, edges, band, *ids[1:])
        recv = share(send)
        if it == 0:
            pick, inverse, moment = call(
                layout_kernel,
                [VM] * 5,
                [shape(3, 64, 256), shape(6, 8, 8, 384), shape(8, LANES)],
                [],
                "layout",
            )(*shared, send)
            moments.append(moment)
        given = (*recv, row, edges, masked, early, late, *ids)
        specs = [VM] * 9 + [SM] * 3
        if it + 2 < ITERS:
            send, band, row, image, moment = call(
                next_kernel,
                specs + [VM] * 2,
                frames_out + [shape(8, 384), shape(2, 8, LANES)],
                scratch,
                "next",
            )(*given, pick, inverse)
            moments.append(moment)
        else:
            send, band, row, image = call(
                last_kernel,
                specs + [VM] * 5,
                [shape(32, 40, LANES), shape(8, 384), shape(8, 8, 384), shape(8, 384)],
                scratch + [(40, LANES)],
                "last",
            )(*given, pick, inverse, *moments)
        vectors.append(row)
        images.append(image)
    recv = exchange(send, "frames")
    send, known, mine = call(
        finish_kernel,
        [VM] * 6 + [SM] * 3,
        [shape(8, 16, LANES), shape(8, LANES), shape(8, 384)],
        [(24, LANES), (256, 384)],
        "finish",
    )(recv, early, late, row, edges, band, *ids[1:], ids[0])
    recv = exchange(send, "cols")
    return tuple(
        call(end_kernel, [VM] * 11, [shape(6, 256), shape(6, 256)], [(8, 256)], "end")(
            recv, mine, known, right_side, *vectors, *images
        )
    )


def solution(mesh):
    return jax.shard_map(
        per_device,
        mesh=mesh,
        in_specs=(
            P(None, ROWS),
            P(None, None, ROWS),
            P(None, None, None, ROWS),
            P(ROWS),
            P("frames", "cols", None, None, None),
            P("frames", "cols", None),
            P("frames", "cols", None),
            P("frames", "cols"),
        ),
        out_specs=(P(None, ROWS), P(None, ROWS)),
        check_vma=False,
    )
```

```python
import jax
import jax.numpy as jnp
from jax import lax
from jax.experimental import pallas as pl
from jax.experimental.pallas import tpu as pltpu
from jax.sharding import PartitionSpec as P


ITERS = 4
BAND = 8
LANES = 128
F32 = jnp.float32
ROWS = ("frames", "cols")
EARLY = 7


def lane_ids(rows):
    return lax.broadcasted_iota(jnp.int32, (rows, LANES), 1)


def half_turn(x):
    return pltpu.roll(x, 64, 1)


def left(x, by):
    return pltpu.roll(x, (x.shape[1] - by) % x.shape[1], 1) if by % x.shape[1] else x


def right(x, by):
    return pltpu.roll(x, by % x.shape[1], 1) if by % x.shape[1] else x


def store_as_tiles(ref, base, x):
    low = lane_ids(1) < 64
    for u in range(2):
        part = x[:, u * LANES : (u + 1) * LANES]
        turned = half_turn(part)
        for j in range(3):
            lanes = pl.ds(j * LANES, LANES)
            ref[pl.ds(base + 2 * u, 1), lanes] = jnp.where(
                low, part[2 * j : 2 * j + 1], turned[2 * j + 1 : 2 * j + 2]
            )
            ref[pl.ds(base + 2 * u + 1, 1), lanes] = jnp.where(
                low, turned[2 * j : 2 * j + 1], part[2 * j + 1 : 2 * j + 2]
            )


def store_as_natural(ref, t):
    low = lane_ids(1) < 64
    for j in range(3):
        part = t[:, j * LANES : (j + 1) * LANES]
        turned = half_turn(part)
        for u in range(2):
            lanes = pl.ds(u * LANES, LANES)
            ref[pl.ds(2 * j, 1), lanes] = jnp.where(
                low, part[2 * u : 2 * u + 1], turned[2 * u + 1 : 2 * u + 2]
            )
            ref[pl.ds(2 * j + 1, 1), lanes] = jnp.where(
                low, turned[2 * u : 2 * u + 1], part[2 * u + 1 : 2 * u + 2]
            )


def start_kernel(
    right_hbm, diag_hbm, band_hbm, reach_hbm, rows_hbm, cols_hbm,
    send_ref, masked_ref, rows_ref, cols_ref,
    right_ref, diag_ref, band_ref, reach_ref, pack, *sems,
):
    copies = [
        pltpu.make_async_copy(source, to, sem)
        for source, to, sem in zip(
            (diag_hbm, right_hbm, reach_hbm, band_hbm, rows_hbm, cols_hbm),
            (diag_ref, right_ref, reach_ref, band_ref, rows_ref, cols_ref),
            sems,
        )
    ]
    for copy in copies:
        copy.start()
    for copy in copies[:2]:
        copy.wait()
    sub = lax.broadcasted_iota(jnp.int32, (6, 256), 0)
    matrix = [diag_ref[a] for a in range(6)]
    inverse = [(sub == a).astype(F32) for a in range(6)]
    for p in range(6):
        pivot = matrix[p][p : p + 1]
        matrix[p] = matrix[p] / pivot
        inverse[p] = inverse[p] / pivot
        for a in range(6):
            if a != p:
                factor = matrix[a][p : p + 1]
                matrix[a] = matrix[a] - factor * matrix[p]
                inverse[a] = inverse[a] - factor * inverse[p]
    residual = right_ref[...]
    first = jnp.concatenate(
        [jnp.sum(inverse[a] * residual, axis=0, keepdims=True) for a in range(6)], axis=0
    )
    store_as_tiles(pack, 0, first)
    for j in range(3):
        send_ref[4 * j : 4 * j + 4, :] = pack[0:4, j * LANES : (j + 1) * LANES]
    for d in range(4):
        turned = jnp.concatenate(
            [inverse[a][(a + d) % 6 : (a + d) % 6 + 1] for a in range(6)], axis=0
        )
        store_as_tiles(pack, 0, turned)
        for j in range(3):
            at = 32 + (3 * d + j) * 4
            send_ref[at : at + 4, :] = pack[0:4, j * LANES : (j + 1) * LANES]
    product = first * residual
    product = jnp.sum(product[:, 0:LANES] + product[:, LANES:256], axis=0, keepdims=True)
    product = jnp.sum(product, axis=1, keepdims=True)
    moment = jnp.where(lane_ids(1) == 8, product, 0.0)
    for copy in copies[2:6]:
        copy.wait()
    reach = reach_ref[...]
    for o in range(BAND):
        keep = (reach > o).astype(F32)
        for a in range(6):
            masked_ref[o * 6 + a] = band_ref[a, :, o, :] * keep
    ids = lane_ids(6)
    for j in range(3):
        packed = jnp.zeros((6, LANES), F32)
        for i in range(16):
            block = masked_ref[j * 16 + i, :, LANES : 2 * LANES]
            packed = jnp.where(ids // 8 == i, right(block, i * 8 + 8), packed)
        send_ref[12 + 6 * j : 18 + 6 * j, :] = packed
    rows = rows_ref[...]
    send_ref[30:31, :] = moment
    send_ref[30:31, 0:8] = ((rows // 4) * 8 + rows % 4).astype(F32)
    send_ref[31:32, :] = jnp.zeros((1, LANES), F32)


def blocks(refs):
    col = lax.axis_index("cols")
    rows = refs[0].shape[0] // 2
    return [
        (((col // 2 + 4 - d) % 4) * 2 + (col + i) % 2, refs[d], i * rows)
        for d in range(4)
        for i in range(2)
    ]


def load_kernel(tiles_hbm, tiles_ref, *sems):
    copies = [pltpu.make_async_copy(tiles_hbm.at[s], tiles_ref.at[s], sems[s]) for s in range(EARLY)]
    for copy in copies:
        copy.start()
    for copy in copies:
        copy.wait()


def own_edge(edge_ref, row_ref, col):
    last = row_ref[(col + 7) % 8][3:4]
    values = []
    for j in range(3):
        part = last[:, j * LANES : (j + 1) * LANES]
        values += [half_turn(part), part]
    total = jnp.zeros((6, LANES), F32)
    for o in range(BAND):
        z = edge_ref[o * 6] * values[0]
        for a in range(1, 6):
            z = z + edge_ref[o * 6 + a] * values[a]
        total = total + right(z, o + 1)
    total = jnp.where(lane_ids(6) < 8, total, 0.0)
    turned = half_turn(total)
    low = lane_ids(1) < 64
    return jnp.concatenate(
        [jnp.where(low, total[2 * j : 2 * j + 1], turned[2 * j + 1 : 2 * j + 2]) for j in range(3)],
        axis=1,
    )


def bfloat16_parts(x):
    high = x.astype(jnp.bfloat16)
    rest = x - high.astype(F32)
    middle = rest.astype(jnp.bfloat16)
    return high, middle, (rest - middle.astype(F32)).astype(jnp.bfloat16)


def select_sum(pick, x):
    pick = pick.astype(jnp.bfloat16)
    high, middle, low = [
        jnp.dot(pick, part, preferred_element_type=F32) for part in bfloat16_parts(x)
    ]
    return low + middle + high


def slot_of(tiles_refs, s):
    return tiles_refs[0].at[s] if s < EARLY else tiles_refs[1].at[s - EARLY]


def transposed_products(row_ref, tiles_refs, ids_refs, picked, spread, copies=()):
    rows_ref, _, count_ref = ids_refs
    count = count_ref[0, 0]
    picked[...] = jnp.zeros((LANES, 384), F32)
    for s in range(8):
        r = rows_ref[0, s]
        picked[s : s + 1, :] = row_ref[r // 4, pl.ds(r % 4, 1), :]
    for i, part in enumerate(bfloat16_parts(picked[4:8, :])):
        picked[8 + 4 * i : 12 + 4 * i, :] = part.astype(F32)
    upright = [picked[:, j * LANES : (j + 1) * LANES].T for j in range(3)]
    at = lax.broadcasted_iota(jnp.int32, (LANES, 512), 0)
    to = lax.broadcasted_iota(jnp.int32, (LANES, 512), 1)
    ones = ((at >= 8) & (at < 20) & (at % 4 == to // LANES)).astype(jnp.bfloat16)
    for j in range(3):
        spread[j * LANES : (j + 1) * LANES, :] = jnp.dot(
            upright[j].astype(jnp.bfloat16), ones, preferred_element_type=F32
        )
    products = []
    for s in range(8):
        if copies and s >= EARLY:
            copies[s - EARLY].wait()
        tile = slot_of(tiles_refs, s)
        sums = [[None] * 3, [None] * 3]
        for i in range(48):
            if s < 4:
                column = upright[i // 16][8 * (i % 16) : 8 * (i % 16) + 8, s : s + 1]
                column = jnp.broadcast_to(column, (8, LANES))
            else:
                column = spread[8 * i : 8 * i + 8, (s - 4) * LANES : (s - 3) * LANES]
            for j in range(3):
                part = tile[8 * i : 8 * i + 8, j * LANES : (j + 1) * LANES] * column
                before = sums[i % 2][j]
                sums[i % 2][j] = part if before is None else before + part
        total = jnp.concatenate(
            [jnp.sum(x + y, axis=0, keepdims=True) for x, y in zip(*sums)], axis=1
        )
        products.append(total * (s < count).astype(F32))
    return products


def edge_terms(row_ref, edge_ref):
    frame = lax.axis_index("frames")
    col = lax.axis_index("cols")
    edge = own_edge(edge_ref, row_ref, col)
    cross = ((col == 0) & (frame < 31)).astype(F32)
    return edge * (col > 0).astype(F32), edge * cross


def band_terms(row_ref, masked_ref, edge, out_ref, natural, sums):
    col = lax.axis_index("cols")
    store_as_natural(natural, row_ref[col])
    lane = lax.broadcasted_iota(jnp.int32, (6, 256), 1)
    vector = natural[0:6, :]
    total = jnp.zeros((6, 256), F32)
    ahead = [jnp.zeros((6, 256), F32) for _ in range(6)]
    for o in range(BAND):
        shifted = jnp.where(lane < 255 - o, left(vector, o + 1), 0.0)
        z = jnp.zeros((6, 256), F32)
        for a in range(6):
            block = masked_ref[o * 6 + a]
            z = z + block * natural[a : a + 1, :]
            ahead[a] = ahead[a] + block * shifted
        total = total + jnp.where(lane > o, right(z, o + 1), 0.0)
    for a in range(6):
        sums[a : a + 1, :] = jnp.sum(ahead[a], axis=0, keepdims=True)
    out_ref[...] = jnp.zeros((8, 384), F32)
    store_as_tiles(out_ref, 0, total + sums[0:6, :])
    out_ref[0:1, :] = out_ref[0:1, :] + edge


def send_frames(row_ref, edge_ref, masked_ref, tiles_refs, ids_refs, send_ref, band_ref, scratch, copies=()):
    picked, natural, sums, spread = scratch
    col = lax.axis_index("cols")
    sub = lax.broadcasted_iota(jnp.int32, (8, 384), 0)
    chunk = jnp.where(sub < 4, row_ref[col], 0.0)
    for f in range(32):
        send_ref[f] = chunk
    mine, onward = edge_terms(row_ref, edge_ref)
    send_ref[jnp.minimum(lax.axis_index("frames") + 1, 31), 4:5, :] = onward
    band_terms(row_ref, masked_ref, mine, band_ref, natural, sums)
    for s, product in enumerate(transposed_products(row_ref, tiles_refs, ids_refs, picked, spread, copies)):
        q = ids_refs[1][0, s]
        send_ref[q // 4, pl.ds(4 + q % 4, 1), :] += product


def send_last(row_ref, edge_ref, masked_ref, tiles_refs, ids_refs, known, send_ref, band_ref, scratch):
    picked, natural, sums, spread, pack = scratch
    col = lax.axis_index("cols")
    mine, onward = edge_terms(row_ref, edge_ref)
    band_terms(row_ref, masked_ref, mine, band_ref, natural, sums)
    own = row_ref[col]
    products = transposed_products(row_ref, tiles_refs, ids_refs, picked, spread)
    for j in range(3):
        lanes = slice(j * LANES, (j + 1) * LANES)
        for s in range(8):
            pack[8 * j + s : 8 * j + s + 1, :] = products[s][:, lanes]
        pack[24 + 4 * j : 28 + 4 * j, :] = own[0:4, lanes]
        pack[36 + j : 37 + j, :] = onward[:, lanes]
    part = own * band_ref[...]
    quad = jnp.sum(part[:, 0:128] + part[:, 128:256] + part[:, 256:384], axis=0, keepdims=True)
    part = own[0:1] * mine
    quad = quad + part[:, 0:128] + part[:, 128:256] + part[:, 256:384]
    rows = [jnp.sum(x, axis=0, keepdims=True) for x in known] + [quad]
    lane = lax.broadcasted_iota(jnp.int32, (8, LANES), 1)
    sub = lax.broadcasted_iota(jnp.int32, (8, LANES), 0)
    totals = jnp.sum(jnp.concatenate(rows, axis=0), axis=1, keepdims=True)
    misc = jnp.sum(jnp.where(lane == sub + 8, totals, 0.0), axis=0, keepdims=True)
    for s in range(8):
        misc = jnp.where(lane_ids(1) == s, ids_refs[1][0, s].astype(F32), misc)
    pack[39:40, :] = misc
    whole = pack[...]
    for f in range(32):
        send_ref[f] = whole


def first_kernel(
    recv0, recv1, recv2, recv3, masked_ref, tiles_hbm, early_ref, rows_ref, cols_ref, count_ref,
    send_ref, band_ref, row_ref, edge_ref, late_ref, picked, natural, sums, spread, *sems,
):
    copies = [
        pltpu.make_async_copy(tiles_hbm.at[EARLY + s], late_ref.at[s], sems[s])
        for s in range(8 - EARLY)
    ]
    for copy in copies:
        copy.start()
    col = lax.axis_index("cols")
    row_ref[...] = jnp.zeros((8, 8, 384), F32)
    for c, ref, at in blocks((recv0, recv1, recv2, recv3)):
        for j in range(3):
            row_ref[c, 0:4, j * LANES : (j + 1) * LANES] = ref[at + 4 * j : at + 4 * j + 4, :]
    ids = lane_ids(6)
    for j in range(3):
        at = 80 + 12 + 6 * j
        part = jnp.where(col % 2 == 1, recv0[at : at + 6, :], recv1[at : at + 6, :])
        for i in range(16):
            edge_ref[j * 16 + i] = jnp.where(ids >= 120, right(part, 120 - i * 8), 0.0)
    scratch = (picked, natural, sums, spread)
    send_frames(
        row_ref, edge_ref, masked_ref, (early_ref, late_ref), (rows_ref, cols_ref, count_ref),
        send_ref, band_ref, scratch, copies,
    )


def layout_kernel(recv0, recv1, recv2, recv3, _, pick_ref, inverse_ref, moment_ref):
    refs = (recv0, recv1, recv2, recv3)
    total = jnp.zeros((1, LANES), F32)
    lane = lane_ids(1)
    group = lane % 64 // 8
    device = jnp.zeros((1, LANES), jnp.int32)
    target = jnp.zeros((1, LANES), F32)
    low = lax.broadcasted_iota(jnp.int32, (8, LANES), 0) < 4
    for b, (c, ref, at) in enumerate(blocks(refs)):
        device = jnp.where(group == b, c, device)
        target = jnp.where(group == b, right(ref[at + 30 : at + 31, :], 8 * b), target)
        total = total + ref[at + 30 : at + 31, :]
        parts = []
        for g in range(12):
            first = at + 32 + 8 * (g // 2)
            part = ref[first : first + 8, :]
            part = pltpu.roll(part, 4, 0) if g % 2 else part
            parts.append(jnp.where(low, part, 0.0))
        parts = [jnp.concatenate(parts[3 * d : 3 * d + 3], axis=1) for d in range(4)]
        parts += [left(parts[2], 256), left(parts[1], 320)]
        for d in range(6):
            inverse_ref[d, c] = parts[d]
    own = (device * 8 + lane % 4).astype(F32)
    onward = ((device + 7) % 8 * 8 + 3).astype(F32)
    at = lane % 8
    none = jnp.full((1, LANES), -1.0, F32)
    index = lax.broadcasted_iota(jnp.int32, (64, LANES), 0).astype(F32)
    for j in range(3):
        three = jnp.where((at < 4) == (j == 0), own, none) if j < 2 else none
        four = jnp.where(at == 4 + j, onward, jnp.where(at < 4, own, none) if j == 2 else none)
        for half, wanted in enumerate((jnp.where(lane < 64, target, three), jnp.where(lane < 64, four, none))):
            found = (index == jnp.broadcast_to(wanted, (64, LANES))).astype(F32)
            pick_ref[j, :, half * LANES : (half + 1) * LANES] = found
    sub = lax.broadcasted_iota(jnp.int32, (8, LANES), 0)
    total = jnp.where(lane == 8, total, 0.0)
    moment_ref[...] = jnp.where(sub == 0, jnp.broadcast_to(total, (8, LANES)), 0.0)


def row_image(refs, pick_ref):
    places = blocks(refs)

    def rows_from(first):
        return bfloat16_parts(
            jnp.concatenate([ref[at + first : at + first + 8, :] for _, ref, at in places], axis=0)
        )

    three, four = rows_from(24), rows_from(32)
    parts = []
    for j in range(3):
        pick = pick_ref[j, :, 0:192].astype(jnp.bfloat16)
        high, middle, low = [
            jnp.dot(pick, jnp.concatenate(x, axis=0), preferred_element_type=F32)
            for x in zip(rows_from(8 * j), three, four)
        ]
        parts.append(low + middle + high)
    return jnp.concatenate(parts, axis=1).reshape(8, 8, 384)


def folded(x):
    x = jnp.sum(x, axis=0)
    return x[:, 0:128] + x[:, 128:256] + x[:, 256:384]


def advance(refs, pick_ref, inverse_ref, before_ref, row_ref, image_ref, moment_ref, picked):
    col = lax.axis_index("cols")
    image = row_image(refs, pick_ref)
    flat = image.reshape(64, 384)
    vector = inverse_ref[0].reshape(64, 384) * flat
    for d in range(1, 6):
        vector = vector + inverse_ref[d].reshape(64, 384) * left(flat, 64 * d)
    vector = vector.reshape(8, 8, 384)
    row_ref[...] = vector
    moments = [folded(before_ref[...] * image), folded(vector * image)]
    if moment_ref is not None:
        moment_ref[0], moment_ref[1] = moments
    picked[0:64, :] = flat
    image_ref[...] = picked[pl.ds(pl.multiple_of(col * 8, 8), 8), :]
    return moments


def next_kernel(
    recv0, recv1, recv2, recv3, before_ref, edge_ref, masked_ref, early_ref, late_ref, rows_ref, cols_ref, count_ref,
    pick_ref, inverse_ref, send_ref, band_ref, row_ref, image_ref, moment_ref, *scratch,
):
    advance((recv0, recv1, recv2, recv3), pick_ref, inverse_ref, before_ref, row_ref, image_ref, moment_ref, scratch[0])
    ids_refs = (rows_ref, cols_ref, count_ref)
    tiles_refs = (early_ref, late_ref)
    send_frames(row_ref, edge_ref, masked_ref, tiles_refs, ids_refs, send_ref, band_ref, scratch)


def last_kernel(
    recv0, recv1, recv2, recv3, before_ref, edge_ref, masked_ref, early_ref, late_ref, rows_ref, cols_ref, count_ref,
    pick_ref, inverse_ref, m0_ref, m1_ref, m2_ref, send_ref, band_ref, row_ref, image_ref, *scratch,
):
    moments = advance((recv0, recv1, recv2, recv3), pick_ref, inverse_ref, before_ref, row_ref, image_ref, None, scratch[0])
    known = [m0_ref[...], m1_ref[0], m1_ref[1], m2_ref[0], m2_ref[1]] + moments
    ids_refs = (rows_ref, cols_ref, count_ref)
    tiles_refs = (early_ref, late_ref)
    send_last(row_ref, edge_ref, masked_ref, tiles_refs, ids_refs, known, send_ref, band_ref, scratch)


def onward_terms(edge_ref, start):
    parts = []
    for j in range(3):
        part = start[:, j * LANES : (j + 1) * LANES]
        parts += [part, half_turn(part)]
    ids = lane_ids(6)
    begin = jnp.concatenate(parts, axis=0)
    sums = [jnp.zeros((6, LANES), F32) for _ in range(6)]
    for o in range(BAND):
        shifted = jnp.where(ids >= 127 - o, left(begin, o + 1), 0.0)
        for a in range(6):
            sums[a] = sums[a] + edge_ref[o * 6 + a] * shifted
    sums = [jnp.sum(x, axis=0, keepdims=True) for x in sums]
    low = lane_ids(1) < 64
    return jnp.concatenate(
        [jnp.where(low, half_turn(sums[2 * j]), sums[2 * j + 1]) for j in range(3)], axis=1
    )


def tile_products(tiles_refs, piece_of, count, pack):
    for s in range(8):
        piece = piece_of(s) * (s < count).astype(F32)
        for j in range(3):
            rows = pl.ds(j * LANES, LANES)
            tile = slot_of(tiles_refs, s)
            part = tile[rows, 0:LANES] * piece[:, 0:LANES]
            part = part + tile[rows, LANES : 2 * LANES] * piece[:, LANES : 2 * LANES]
            part = part + tile[rows, 2 * LANES : 384] * piece[:, 2 * LANES : 384]
            pack[8 * j + s : 8 * j + s + 1, :] = jnp.sum(part.T, axis=0, keepdims=True)


def cols_kernel(recv_ref, early_ref, late_ref, row_ref, edge_ref, band_ref, cols_ref, count_ref, pack):
    frame = lax.axis_index("frames")
    col = lax.axis_index("cols")
    def piece_of(s):
        q = cols_ref[0, s]
        return recv_ref[q // 4, pl.ds(q % 4, 1), :]

    tile_products((early_ref, late_ref), piece_of, count_ref[0, 0], pack)
    total = recv_ref[0]
    for f in range(1, 32):
        total = total + recv_ref[f]
    terms = pltpu.roll(total, 4, 0) + band_ref[...]
    here = (col > 0).astype(F32)
    there = ((col == 0) & (frame < 31)).astype(F32)
    start = row_ref[col][0:1] * here + recv_ref[jnp.minimum(frame + 1, 31)][0:1] * there
    onward = onward_terms(edge_ref, start)
    for j in range(3):
        lanes = slice(j * LANES, (j + 1) * LANES)
        pack[24 + 4 * j : 28 + 4 * j, :] = terms[0:4, lanes]
        pack[36 + j : 37 + j, :] = onward[:, lanes]
    pack[39:40, :] = jnp.zeros((1, LANES), F32)


def finish_kernel(
    recv_ref, early_ref, late_ref, row_ref, edge_ref, band_ref, cols_ref, count_ref, rows_ref,
    send_ref, known_ref, mine_ref, pack, columns,
):
    frame = lax.axis_index("frames")
    col = lax.axis_index("cols")
    lane = lane_ids(1)
    misc = [recv_ref[f, 39:40, :] for f in range(32)]
    total = misc[0]
    for x in misc[1:]:
        total = total + x
    known_ref[...] = jnp.broadcast_to(total, (8, LANES))
    halves = []
    for h in range(2):
        tags = jnp.zeros((1, LANES), F32)
        for i in range(16):
            tags = jnp.where(lane // 8 == i, right(misc[16 * h + i], 8 * i), tags)
        halves.append(tags)
    tags = jnp.concatenate(halves, axis=1)
    products = jnp.concatenate(
        [recv_ref[:, 8 * j : 8 * j + 8, :].reshape(256, LANES) for j in range(3)], axis=1
    )

    at = lax.broadcasted_iota(jnp.int32, (256, 256), 0)
    wanted = ((at // 8) * 4 + at % 4).astype(F32)
    sums = select_sum((wanted == jnp.broadcast_to(tags, (256, 256))).astype(F32), products)
    columns[...] = sums
    low = lax.broadcasted_iota(jnp.int32, (8, LANES), 0) < 4
    quad = jnp.zeros((8, LANES), F32)
    for f in range(32):
        here = sums[8 * f : 8 * f + 8]
        quad = quad + jnp.where(low, here[:, 0:128], here[:, 128:256]) * recv_ref[f, 24:32, :]
        quad = quad + jnp.where(low, here[:, 256:384] * recv_ref[f, 32:40, :], 0.0)
    quad = jnp.sum(quad, axis=0, keepdims=True)
    for f in range(31):
        for j in range(3):
            quad = quad + recv_ref[f, 36 + j : 37 + j, :] * recv_ref[f + 1, 24 + 4 * j : 25 + 4 * j, :]
    quad = quad + quad + jnp.where(lane == 15, total, 0.0)

    mine = columns[pl.ds(pl.multiple_of(frame * 8, 8), 8), :]
    mine_ref[...] = mine + band_ref[...]
    before = jnp.maximum(frame - 1, 0)
    for j in range(3):
        lanes = slice(j * LANES, (j + 1) * LANES)
        edge = recv_ref[before, 36 + j : 37 + j, :] * (frame > 0).astype(F32)
        mine_ref[0:1, lanes] = mine_ref[0:1, lanes] + edge
    here = (col > 0).astype(F32)
    there = ((col == 0) & (frame < 31)).astype(F32)
    after = jnp.minimum(frame + 1, 31)

    def row_of(f, i):
        return jnp.concatenate([recv_ref[f, pl.ds(24 + 4 * j + i, 1), :] for j in range(3)], axis=1)

    onward = onward_terms(edge_ref, row_ref[col][0:1] * here + row_of(after, 0) * there)
    empty = jnp.where(lax.broadcasted_iota(jnp.int32, (16, LANES), 0) == 12, quad, 0.0)
    for c in range(8):
        send_ref[c] = empty
    for j in range(3):
        send_ref[(col + 7) % 8, 4 * j + 3 : 4 * j + 4, :] = onward[:, j * LANES : (j + 1) * LANES]

    def piece_of(s):
        q = cols_ref[0, s]
        return row_of(q // 4, q % 4)

    tile_products((early_ref, late_ref), piece_of, count_ref[0, 0], pack)
    for s in range(8):
        r = rows_ref[0, s]
        for j in range(3):
            send_ref[r // 4, pl.ds(4 * j + r % 4, 1), :] += pack[8 * j + s : 8 * j + s + 1, :]


def end_kernel(
    recv_ref, mine_ref, known_ref, right_ref, v0, v1, v2, v3, w0, w1, w2, solution_ref, residual_ref, scratch
):
    col = lax.axis_index("cols")
    total = recv_ref[0]
    for c in range(1, 8):
        total = total + recv_ref[c]
    parts = [total[0:8], pltpu.roll(total[0:8], 4, 0), total[8:16]]
    last = jnp.concatenate(parts, axis=1) + mine_ref[...]
    known = known_ref[0:1, :]
    mu = [jnp.broadcast_to(known[:, 8 + i : 9 + i], (1, LANES)) for i in range(7)]
    mu.append(jnp.broadcast_to(jnp.sum(total[12:13], axis=1, keepdims=True), (1, LANES)))
    zero = jnp.zeros((1, LANES), F32)
    one = zero + 1.0

    def form(left_side, shift):
        value = zero
        for i in range(len(left_side)):
            for k in range(i, len(left_side)):
                term = left_side[i] * left_side[k]
                value = value + (term if i == k else term + term) * mu[i + k + shift]
        return value

    def ratio(top, bottom):
        return jnp.where(top == 0.0, 0.0, top / jnp.where(top == 0.0, one, bottom))

    direction, residual, solution = [one], [one], []
    gamma = mu[0]
    for it in range(ITERS):
        alpha = ratio(gamma, form(direction, 0) + form(direction, 1))
        solution = solution + [zero] * (len(direction) - len(solution))
        solution = [x + alpha * p for x, p in zip(solution, direction)]
        image = [p + q for p, q in zip(direction + [zero], [zero] + direction)]
        residual = residual + [zero] * (len(image) - len(residual))
        residual = [r - alpha * y for r, y in zip(residual, image)]
        if it + 1 < ITERS:
            fresh = form(residual, 0)
            beta = ratio(fresh, gamma)
            direction = direction + [zero] * (len(residual) - len(direction))
            direction = [r + beta * p for r, p in zip(residual, direction)]
            gamma = fresh

    def wide(x):
        return jnp.concatenate([x, x, x], axis=1)

    total = wide(solution[0]) * v0[col]
    for x, ref in zip(solution[1:], (v1, v2, v3)):
        total = total + wide(x) * ref[col]
    store_as_natural(solution_ref, total)
    total = wide(residual[4]) * last
    for x, ref in zip(residual[1:4], (w0, w1, w2)):
        total = total + wide(x) * ref[...]
    store_as_natural(scratch, total)
    residual_ref[...] = scratch[0:6, :] + jnp.concatenate([residual[0]] * 2, axis=1) * right_ref[...]


VM = pl.BlockSpec(memory_space=pltpu.VMEM)
SM = pl.BlockSpec(memory_space=pltpu.SMEM)
HB = pl.BlockSpec(memory_space=pltpu.HBM)


def shape(*dims, kind=F32):
    return jax.ShapeDtypeStruct(dims, kind)


def call(kernel, specs, outs, scratch, name):
    return pl.pallas_call(
        kernel,
        in_specs=specs,
        out_specs=[VM] * len(outs),
        out_shape=outs,
        scratch_shapes=[pltpu.VMEM(s, F32) if isinstance(s, tuple) else s for s in scratch],
        compiler_params=pltpu.CompilerParams(vmem_limit_bytes=24 * 1024 * 1024),
        name=name,
    )


def per_device(right_side, diag_blocks, band_blocks, reach, tiles, tile_rows, tile_cols, tile_count):
    def exchange(x, axis):
        return lax.all_to_all(x, axis, 0, 0, tiled=True)

    def share(x):
        chips = lax.axis_size("cols") // 2
        swap = [(i, i ^ 1) for i in range(2 * chips)]
        pair = jnp.concatenate([x, lax.ppermute(x, "cols", swap)], axis=0)
        others = []
        for d in range(1, chips):
            ahead = [(i, (i + 2 * d) % (2 * chips)) for i in range(2 * chips)]
            others.append(lax.ppermute(pair, "cols", ahead))
        return [pair, *others]

    def in_hbm(x):
        return pltpu.with_memory_space_constraint(x, pltpu.HBM)

    sem = pltpu.SemaphoreType.DMA(())
    stored = in_hbm(tiles.reshape(tiles.shape[2:]))
    inputs = (right_side, diag_blocks, jnp.transpose(band_blocks, (1, 2, 0, 3)), reach.reshape(1, -1))
    inputs += (tile_rows.reshape(1, 8), tile_cols.reshape(1, 8))
    send, masked, *ids = call(
        start_kernel,
        [HB] * 6,
        [shape(80, LANES), shape(48, 6, 256)]
        + [shape(1, 8, kind=jnp.int32)] * 2,
        [(6, 256), (6, 6, 256), (6, 6, 8, 256), pltpu.VMEM((1, 256), jnp.int32), (8, 384)]
        + [sem] * 6,
        "start",
    )(*[in_hbm(x) for x in inputs])
    ids.append(tile_count)
    recv = shared = share(send)
    (early,) = call(load_kernel, [HB], [shape(EARLY, 384, 384)], [sem] * EARLY, "load")(stored)
    frames_out = [shape(32, 8, 384), shape(8, 384), shape(8, 8, 384)]
    scratch = [(LANES, 384), (8, 256), (8, 256), (384, 512)]
    send, band, row, edges, late = call(
        first_kernel,
        [VM] * 5 + [HB, VM] + [SM] * 3,
        frames_out + [shape(48, 6, LANES), shape(8 - EARLY, 384, 384)],
        scratch + [sem] * (8 - EARLY),
        "first",
    )(*recv, masked, stored, early, *ids)
    vectors, images, moments = [row], [], []
    for it in range(ITERS - 1):
        recv = exchange(send, "frames")
        (send,) = call(
            cols_kernel,
            [VM] * 6 + [SM] * 2,
            [shape(40, LANES)],
            [],
            "products",
        )(recv, early, late, row, edges, band, *ids[1:])
        recv = share(send)
        if it == 0:
            pick, inverse, moment = call(
                layout_kernel,
                [VM] * 5,
                [shape(3, 64, 256), shape(6, 8, 8, 384), shape(8, LANES)],
                [],
                "layout",
            )(*shared, send)
            moments.append(moment)
        given = (*recv, row, edges, masked, early, late, *ids)
        specs = [VM] * 9 + [SM] * 3
        if it + 2 < ITERS:
            send, band, row, image, moment = call(
                next_kernel,
                specs + [VM] * 2,
                frames_out + [shape(8, 384), shape(2, 8, LANES)],
                scratch,
                "next",
            )(*given, pick, inverse)
            moments.append(moment)
        else:
            send, band, row, image = call(
                last_kernel,
                specs + [VM] * 5,
                [shape(32, 40, LANES), shape(8, 384), shape(8, 8, 384), shape(8, 384)],
                scratch + [(40, LANES)],
                "last",
            )(*given, pick, inverse, *moments)
        vectors.append(row)
        images.append(image)
    recv = exchange(send, "frames")
    send, known, mine = call(
        finish_kernel,
        [VM] * 6 + [SM] * 3,
        [shape(8, 16, LANES), shape(8, LANES), shape(8, 384)],
        [(24, LANES), (256, 384)],
        "finish",
    )(recv, early, late, row, edges, band, *ids[1:], ids[0])
    recv = exchange(send, "cols")
    return tuple(
        call(end_kernel, [VM] * 11, [shape(6, 256), shape(6, 256)], [(8, 256)], "end")(
            recv, mine, known, right_side, *vectors, *images
        )
    )


def solution(mesh):
    return jax.shard_map(
        per_device,
        mesh=mesh,
        in_specs=(
            P(None, ROWS),
            P(None, None, ROWS),
            P(None, None, None, ROWS),
            P(ROWS),
            P("frames", "cols", None, None, None),
            P("frames", "cols", None),
            P("frames", "cols", None),
            P("frames", "cols"),
        ),
        out_specs=(P(None, ROWS), P(None, ROWS)),
        check_vma=False,
    )
```

```python
import jax
import jax.numpy as jnp
from jax import lax
from jax.experimental import pallas as pl
from jax.experimental.pallas import tpu as pltpu
from jax.sharding import PartitionSpec as P


ITERS = 4
BAND = 8
LANES = 128
F32 = jnp.float32
ROWS = ("frames", "cols")
EARLY = 4


def lane_ids(rows):
    return lax.broadcasted_iota(jnp.int32, (rows, LANES), 1)


def half_turn(x):
    return pltpu.roll(x, 64, 1)


def left(x, by):
    return pltpu.roll(x, (x.shape[1] - by) % x.shape[1], 1) if by % x.shape[1] else x


def right(x, by):
    return pltpu.roll(x, by % x.shape[1], 1) if by % x.shape[1] else x


def store_as_tiles(ref, base, x):
    low = lane_ids(1) < 64
    for u in range(2):
        part = x[:, u * LANES : (u + 1) * LANES]
        turned = half_turn(part)
        for j in range(3):
            lanes = pl.ds(j * LANES, LANES)
            ref[pl.ds(base + 2 * u, 1), lanes] = jnp.where(
                low, part[2 * j : 2 * j + 1], turned[2 * j + 1 : 2 * j + 2]
            )
            ref[pl.ds(base + 2 * u + 1, 1), lanes] = jnp.where(
                low, turned[2 * j : 2 * j + 1], part[2 * j + 1 : 2 * j + 2]
            )


def store_as_natural(ref, t):
    low = lane_ids(1) < 64
    for j in range(3):
        part = t[:, j * LANES : (j + 1) * LANES]
        turned = half_turn(part)
        for u in range(2):
            lanes = pl.ds(u * LANES, LANES)
            ref[pl.ds(2 * j, 1), lanes] = jnp.where(
                low, part[2 * u : 2 * u + 1], turned[2 * u + 1 : 2 * u + 2]
            )
            ref[pl.ds(2 * j + 1, 1), lanes] = jnp.where(
                low, turned[2 * u : 2 * u + 1], part[2 * u + 1 : 2 * u + 2]
            )


def start_kernel(
    right_hbm, diag_hbm, band_hbm, reach_hbm, rows_hbm, cols_hbm,
    send_ref, masked_ref, rows_ref, cols_ref,
    right_ref, diag_ref, band_ref, reach_ref, pack, *sems,
):
    copies = [
        pltpu.make_async_copy(source, to, sem)
        for source, to, sem in zip(
            (diag_hbm, right_hbm, reach_hbm, band_hbm, rows_hbm, cols_hbm),
            (diag_ref, right_ref, reach_ref, band_ref, rows_ref, cols_ref),
            sems,
        )
    ]
    for copy in copies:
        copy.start()
    for copy in copies[:2]:
        copy.wait()
    sub = lax.broadcasted_iota(jnp.int32, (6, 256), 0)
    matrix = [diag_ref[a] for a in range(6)]
    inverse = [(sub == a).astype(F32) for a in range(6)]
    for p in range(6):
        pivot = matrix[p][p : p + 1]
        matrix[p] = matrix[p] / pivot
        inverse[p] = inverse[p] / pivot
        for a in range(6):
            if a != p:
                factor = matrix[a][p : p + 1]
                matrix[a] = matrix[a] - factor * matrix[p]
                inverse[a] = inverse[a] - factor * inverse[p]
    residual = right_ref[...]
    first = jnp.concatenate(
        [jnp.sum(inverse[a] * residual, axis=0, keepdims=True) for a in range(6)], axis=0
    )
    store_as_tiles(pack, 0, first)
    for j in range(3):
        send_ref[4 * j : 4 * j + 4, :] = pack[0:4, j * LANES : (j + 1) * LANES]
    for d in range(4):
        turned = jnp.concatenate(
            [inverse[a][(a + d) % 6 : (a + d) % 6 + 1] for a in range(6)], axis=0
        )
        store_as_tiles(pack, 0, turned)
        for j in range(3):
            at = 32 + (3 * d + j) * 4
            send_ref[at : at + 4, :] = pack[0:4, j * LANES : (j + 1) * LANES]
    product = first * residual
    product = jnp.sum(product[:, 0:LANES] + product[:, LANES:256], axis=0, keepdims=True)
    product = jnp.sum(product, axis=1, keepdims=True)
    moment = jnp.where(lane_ids(1) == 8, product, 0.0)
    for copy in copies[2:6]:
        copy.wait()
    reach = reach_ref[...]
    for o in range(BAND):
        keep = (reach > o).astype(F32)
        for a in range(6):
            masked_ref[o * 6 + a] = band_ref[a, :, o, :] * keep
    ids = lane_ids(6)
    for j in range(3):
        packed = jnp.zeros((6, LANES), F32)
        for i in range(16):
            block = masked_ref[j * 16 + i, :, LANES : 2 * LANES]
            packed = jnp.where(ids // 8 == i, right(block, i * 8 + 8), packed)
        send_ref[12 + 6 * j : 18 + 6 * j, :] = packed
    rows = rows_ref[...]
    send_ref[30:31, :] = moment
    send_ref[30:31, 0:8] = ((rows // 4) * 8 + rows % 4).astype(F32)
    send_ref[31:32, :] = jnp.zeros((1, LANES), F32)


def blocks(refs):
    col = lax.axis_index("cols")
    rows = refs[0].shape[0] // 2
    return [
        (((col // 2 + 4 - d) % 4) * 2 + (col + i) % 2, refs[d], i * rows)
        for d in range(4)
        for i in range(2)
    ]


def load_kernel(tiles_hbm, early_ref, late_ref, *sems):
    copies = [
        pltpu.make_async_copy(tiles_hbm.at[s], slot_of((early_ref, late_ref), s), sems[s])
        for s in range(8)
    ]
    for copy in copies:
        copy.start()
    for copy in copies:
        copy.wait()


def own_edge(edge_ref, row_ref, col):
    last = row_ref[(col + 7) % 8][3:4]
    values = []
    for j in range(3):
        part = last[:, j * LANES : (j + 1) * LANES]
        values += [half_turn(part), part]
    total = jnp.zeros((6, LANES), F32)
    for o in range(BAND):
        z = edge_ref[o * 6] * values[0]
        for a in range(1, 6):
            z = z + edge_ref[o * 6 + a] * values[a]
        total = total + right(z, o + 1)
    total = jnp.where(lane_ids(6) < 8, total, 0.0)
    turned = half_turn(total)
    low = lane_ids(1) < 64
    return jnp.concatenate(
        [jnp.where(low, total[2 * j : 2 * j + 1], turned[2 * j + 1 : 2 * j + 2]) for j in range(3)],
        axis=1,
    )


def bfloat16_parts(x):
    high = x.astype(jnp.bfloat16)
    rest = x - high.astype(F32)
    middle = rest.astype(jnp.bfloat16)
    return high, middle, (rest - middle.astype(F32)).astype(jnp.bfloat16)


def select_sum(pick, x):
    pick = pick.astype(jnp.bfloat16)
    high, middle, low = [
        jnp.dot(pick, part, preferred_element_type=F32) for part in bfloat16_parts(x)
    ]
    return low + middle + high


def slot_of(tiles_refs, s):
    return tiles_refs[0].at[s] if s < EARLY else tiles_refs[1].at[s - EARLY]


def transposed_products(row_ref, tiles_refs, ids_refs, picked, spread):
    rows_ref, _, count_ref = ids_refs
    count = count_ref[0, 0]
    picked[...] = jnp.zeros((LANES, 384), F32)
    for s in range(8):
        r = rows_ref[0, s]
        picked[s : s + 1, :] = row_ref[r // 4, pl.ds(r % 4, 1), :]
    for i, part in enumerate(bfloat16_parts(picked[4:8, :])):
        picked[8 + 4 * i : 12 + 4 * i, :] = part.astype(F32)
    upright = [picked[:, j * LANES : (j + 1) * LANES].T for j in range(3)]
    at = lax.broadcasted_iota(jnp.int32, (LANES, 512), 0)
    to = lax.broadcasted_iota(jnp.int32, (LANES, 512), 1)
    ones = ((at >= 8) & (at < 20) & (at % 4 == to // LANES)).astype(jnp.bfloat16)
    for j in range(3):
        spread[j * LANES : (j + 1) * LANES, :] = jnp.dot(
            upright[j].astype(jnp.bfloat16), ones, preferred_element_type=F32
        )
    products = []
    for s in range(8):
        tile = slot_of(tiles_refs, s)
        sums = [[None] * 3, [None] * 3]
        for i in range(48):
            if s < 4:
                column = upright[i // 16][8 * (i % 16) : 8 * (i % 16) + 8, s : s + 1]
                column = jnp.broadcast_to(column, (8, LANES))
            else:
                column = spread[8 * i : 8 * i + 8, (s - 4) * LANES : (s - 3) * LANES]
            for j in range(3):
                part = tile[8 * i : 8 * i + 8, j * LANES : (j + 1) * LANES] * column
                before = sums[i % 2][j]
                sums[i % 2][j] = part if before is None else before + part
        total = jnp.concatenate(
            [jnp.sum(x + y, axis=0, keepdims=True) for x, y in zip(*sums)], axis=1
        )
        products.append(total * (s < count).astype(F32))
    return products


def edge_terms(row_ref, edge_ref):
    frame = lax.axis_index("frames")
    col = lax.axis_index("cols")
    edge = own_edge(edge_ref, row_ref, col)
    cross = ((col == 0) & (frame < 31)).astype(F32)
    return edge * (col > 0).astype(F32), edge * cross


def band_terms(row_ref, masked_ref, edge, out_ref, natural, sums):
    col = lax.axis_index("cols")
    store_as_natural(natural, row_ref[col])
    lane = lax.broadcasted_iota(jnp.int32, (6, 256), 1)
    vector = natural[0:6, :]
    total = jnp.zeros((6, 256), F32)
    ahead = [jnp.zeros((6, 256), F32) for _ in range(6)]
    for o in range(BAND):
        shifted = jnp.where(lane < 255 - o, left(vector, o + 1), 0.0)
        z = jnp.zeros((6, 256), F32)
        for a in range(6):
            block = masked_ref[o * 6 + a]
            z = z + block * natural[a : a + 1, :]
            ahead[a] = ahead[a] + block * shifted
        total = total + jnp.where(lane > o, right(z, o + 1), 0.0)
    for a in range(6):
        sums[a : a + 1, :] = jnp.sum(ahead[a], axis=0, keepdims=True)
    out_ref[...] = jnp.zeros((8, 384), F32)
    store_as_tiles(out_ref, 0, total + sums[0:6, :])
    out_ref[0:1, :] = out_ref[0:1, :] + edge


def send_frames(row_ref, edge_ref, masked_ref, tiles_refs, ids_refs, send_ref, band_ref, scratch):
    picked, natural, sums, spread = scratch
    col = lax.axis_index("cols")
    sub = lax.broadcasted_iota(jnp.int32, (8, 384), 0)
    chunk = jnp.where(sub < 4, row_ref[col], 0.0)
    for f in range(32):
        send_ref[f] = chunk
    mine, onward = edge_terms(row_ref, edge_ref)
    send_ref[jnp.minimum(lax.axis_index("frames") + 1, 31), 4:5, :] = onward
    band_terms(row_ref, masked_ref, mine, band_ref, natural, sums)
    for s, product in enumerate(transposed_products(row_ref, tiles_refs, ids_refs, picked, spread)):
        q = ids_refs[1][0, s]
        send_ref[q // 4, pl.ds(4 + q % 4, 1), :] += product


def send_last(row_ref, edge_ref, masked_ref, tiles_refs, ids_refs, known, send_ref, band_ref, scratch):
    picked, natural, sums, spread, pack = scratch
    col = lax.axis_index("cols")
    mine, onward = edge_terms(row_ref, edge_ref)
    band_terms(row_ref, masked_ref, mine, band_ref, natural, sums)
    own = row_ref[col]
    products = transposed_products(row_ref, tiles_refs, ids_refs, picked, spread)
    for j in range(3):
        lanes = slice(j * LANES, (j + 1) * LANES)
        for s in range(8):
            pack[8 * j + s : 8 * j + s + 1, :] = products[s][:, lanes]
        pack[24 + 4 * j : 28 + 4 * j, :] = own[0:4, lanes]
        pack[36 + j : 37 + j, :] = onward[:, lanes]
    part = own * band_ref[...]
    quad = jnp.sum(part[:, 0:128] + part[:, 128:256] + part[:, 256:384], axis=0, keepdims=True)
    part = own[0:1] * mine
    quad = quad + part[:, 0:128] + part[:, 128:256] + part[:, 256:384]
    rows = [jnp.sum(x, axis=0, keepdims=True) for x in known] + [quad]
    lane = lax.broadcasted_iota(jnp.int32, (8, LANES), 1)
    sub = lax.broadcasted_iota(jnp.int32, (8, LANES), 0)
    totals = jnp.sum(jnp.concatenate(rows, axis=0), axis=1, keepdims=True)
    misc = jnp.sum(jnp.where(lane == sub + 8, totals, 0.0), axis=0, keepdims=True)
    for s in range(8):
        misc = jnp.where(lane_ids(1) == s, ids_refs[1][0, s].astype(F32), misc)
    pack[39:40, :] = misc
    whole = pack[...]
    for f in range(32):
        send_ref[f] = whole


def first_kernel(
    recv0, recv1, recv2, recv3, masked_ref, early_ref, late_ref, rows_ref, cols_ref, count_ref,
    send_ref, band_ref, row_ref, edge_ref, *scratch,
):
    col = lax.axis_index("cols")
    row_ref[...] = jnp.zeros((8, 8, 384), F32)
    for c, ref, at in blocks((recv0, recv1, recv2, recv3)):
        for j in range(3):
            row_ref[c, 0:4, j * LANES : (j + 1) * LANES] = ref[at + 4 * j : at + 4 * j + 4, :]
    ids = lane_ids(6)
    for j in range(3):
        at = 80 + 12 + 6 * j
        part = jnp.where(col % 2 == 1, recv0[at : at + 6, :], recv1[at : at + 6, :])
        for i in range(16):
            edge_ref[j * 16 + i] = jnp.where(ids >= 120, right(part, 120 - i * 8), 0.0)
    send_frames(
        row_ref, edge_ref, masked_ref, (early_ref, late_ref), (rows_ref, cols_ref, count_ref),
        send_ref, band_ref, scratch,
    )


def layout_kernel(recv0, recv1, recv2, recv3, _, pick_ref, inverse_ref, moment_ref):
    refs = (recv0, recv1, recv2, recv3)
    total = jnp.zeros((1, LANES), F32)
    lane = lane_ids(1)
    group = lane % 64 // 8
    device = jnp.zeros((1, LANES), jnp.int32)
    target = jnp.zeros((1, LANES), F32)
    low = lax.broadcasted_iota(jnp.int32, (8, LANES), 0) < 4
    for b, (c, ref, at) in enumerate(blocks(refs)):
        device = jnp.where(group == b, c, device)
        target = jnp.where(group == b, right(ref[at + 30 : at + 31, :], 8 * b), target)
        total = total + ref[at + 30 : at + 31, :]
        parts = []
        for g in range(12):
            first = at + 32 + 8 * (g // 2)
            part = ref[first : first + 8, :]
            part = pltpu.roll(part, 4, 0) if g % 2 else part
            parts.append(jnp.where(low, part, 0.0))
        parts = [jnp.concatenate(parts[3 * d : 3 * d + 3], axis=1) for d in range(4)]
        parts += [left(parts[2], 256), left(parts[1], 320)]
        for d in range(6):
            inverse_ref[d, c] = parts[d]
    own = (device * 8 + lane % 4).astype(F32)
    onward = ((device + 7) % 8 * 8 + 3).astype(F32)
    at = lane % 8
    none = jnp.full((1, LANES), -1.0, F32)
    index = lax.broadcasted_iota(jnp.int32, (64, LANES), 0).astype(F32)
    for j in range(3):
        three = jnp.where((at < 4) == (j == 0), own, none) if j < 2 else none
        four = jnp.where(at == 4 + j, onward, jnp.where(at < 4, own, none) if j == 2 else none)
        for half, wanted in enumerate((jnp.where(lane < 64, target, three), jnp.where(lane < 64, four, none))):
            found = (index == jnp.broadcast_to(wanted, (64, LANES))).astype(F32)
            pick_ref[j, :, half * LANES : (half + 1) * LANES] = found
    sub = lax.broadcasted_iota(jnp.int32, (8, LANES), 0)
    total = jnp.where(lane == 8, total, 0.0)
    moment_ref[...] = jnp.where(sub == 0, jnp.broadcast_to(total, (8, LANES)), 0.0)


def row_image(refs, pick_ref):
    places = blocks(refs)

    def rows_from(first):
        return bfloat16_parts(
            jnp.concatenate([ref[at + first : at + first + 8, :] for _, ref, at in places], axis=0)
        )

    three, four = rows_from(24), rows_from(32)
    parts = []
    for j in range(3):
        pick = pick_ref[j, :, 0:192].astype(jnp.bfloat16)
        high, middle, low = [
            jnp.dot(pick, jnp.concatenate(x, axis=0), preferred_element_type=F32)
            for x in zip(rows_from(8 * j), three, four)
        ]
        parts.append(low + middle + high)
    return jnp.concatenate(parts, axis=1).reshape(8, 8, 384)


def folded(x):
    x = jnp.sum(x, axis=0)
    return x[:, 0:128] + x[:, 128:256] + x[:, 256:384]


def advance(refs, pick_ref, inverse_ref, before_ref, row_ref, image_ref, moment_ref, picked):
    col = lax.axis_index("cols")
    image = row_image(refs, pick_ref)
    flat = image.reshape(64, 384)
    vector = inverse_ref[0].reshape(64, 384) * flat
    for d in range(1, 6):
        vector = vector + inverse_ref[d].reshape(64, 384) * left(flat, 64 * d)
    vector = vector.reshape(8, 8, 384)
    row_ref[...] = vector
    moments = [folded(before_ref[...] * image), folded(vector * image)]
    if moment_ref is not None:
        moment_ref[0], moment_ref[1] = moments
    picked[0:64, :] = flat
    image_ref[...] = picked[pl.ds(pl.multiple_of(col * 8, 8), 8), :]
    return moments


def next_kernel(
    recv0, recv1, recv2, recv3, before_ref, edge_ref, masked_ref, early_ref, late_ref, rows_ref, cols_ref, count_ref,
    pick_ref, inverse_ref, send_ref, band_ref, row_ref, image_ref, moment_ref, *scratch,
):
    advance((recv0, recv1, recv2, recv3), pick_ref, inverse_ref, before_ref, row_ref, image_ref, moment_ref, scratch[0])
    ids_refs = (rows_ref, cols_ref, count_ref)
    tiles_refs = (early_ref, late_ref)
    send_frames(row_ref, edge_ref, masked_ref, tiles_refs, ids_refs, send_ref, band_ref, scratch)


def last_kernel(
    recv0, recv1, recv2, recv3, before_ref, edge_ref, masked_ref, early_ref, late_ref, rows_ref, cols_ref, count_ref,
    pick_ref, inverse_ref, m0_ref, m1_ref, m2_ref, send_ref, band_ref, row_ref, image_ref, *scratch,
):
    moments = advance((recv0, recv1, recv2, recv3), pick_ref, inverse_ref, before_ref, row_ref, image_ref, None, scratch[0])
    known = [m0_ref[...], m1_ref[0], m1_ref[1], m2_ref[0], m2_ref[1]] + moments
    ids_refs = (rows_ref, cols_ref, count_ref)
    tiles_refs = (early_ref, late_ref)
    send_last(row_ref, edge_ref, masked_ref, tiles_refs, ids_refs, known, send_ref, band_ref, scratch)


def onward_terms(edge_ref, start):
    parts = []
    for j in range(3):
        part = start[:, j * LANES : (j + 1) * LANES]
        parts += [part, half_turn(part)]
    ids = lane_ids(6)
    begin = jnp.concatenate(parts, axis=0)
    sums = [jnp.zeros((6, LANES), F32) for _ in range(6)]
    for o in range(BAND):
        shifted = jnp.where(ids >= 127 - o, left(begin, o + 1), 0.0)
        for a in range(6):
            sums[a] = sums[a] + edge_ref[o * 6 + a] * shifted
    sums = [jnp.sum(x, axis=0, keepdims=True) for x in sums]
    low = lane_ids(1) < 64
    return jnp.concatenate(
        [jnp.where(low, half_turn(sums[2 * j]), sums[2 * j + 1]) for j in range(3)], axis=1
    )


def tile_products(tiles_refs, piece_of, count, pack):
    for s in range(8):
        piece = piece_of(s) * (s < count).astype(F32)
        for j in range(3):
            rows = pl.ds(j * LANES, LANES)
            tile = slot_of(tiles_refs, s)
            part = tile[rows, 0:LANES] * piece[:, 0:LANES]
            part = part + tile[rows, LANES : 2 * LANES] * piece[:, LANES : 2 * LANES]
            part = part + tile[rows, 2 * LANES : 384] * piece[:, 2 * LANES : 384]
            pack[8 * j + s : 8 * j + s + 1, :] = jnp.sum(part.T, axis=0, keepdims=True)


def cols_kernel(recv_ref, early_ref, late_ref, row_ref, edge_ref, band_ref, cols_ref, count_ref, pack):
    frame = lax.axis_index("frames")
    col = lax.axis_index("cols")
    def piece_of(s):
        q = cols_ref[0, s]
        return recv_ref[q // 4, pl.ds(q % 4, 1), :]

    tile_products((early_ref, late_ref), piece_of, count_ref[0, 0], pack)
    total = recv_ref[0]
    for f in range(1, 32):
        total = total + recv_ref[f]
    terms = pltpu.roll(total, 4, 0) + band_ref[...]
    here = (col > 0).astype(F32)
    there = ((col == 0) & (frame < 31)).astype(F32)
    start = row_ref[col][0:1] * here + recv_ref[jnp.minimum(frame + 1, 31)][0:1] * there
    onward = onward_terms(edge_ref, start)
    for j in range(3):
        lanes = slice(j * LANES, (j + 1) * LANES)
        pack[24 + 4 * j : 28 + 4 * j, :] = terms[0:4, lanes]
        pack[36 + j : 37 + j, :] = onward[:, lanes]
    pack[39:40, :] = jnp.zeros((1, LANES), F32)


def finish_kernel(
    recv_ref, early_ref, late_ref, row_ref, edge_ref, band_ref, cols_ref, count_ref, rows_ref,
    send_ref, known_ref, mine_ref, pack, columns,
):
    frame = lax.axis_index("frames")
    col = lax.axis_index("cols")
    lane = lane_ids(1)
    misc = [recv_ref[f, 39:40, :] for f in range(32)]
    total = misc[0]
    for x in misc[1:]:
        total = total + x
    known_ref[...] = jnp.broadcast_to(total, (8, LANES))
    halves = []
    for h in range(2):
        tags = jnp.zeros((1, LANES), F32)
        for i in range(16):
            tags = jnp.where(lane // 8 == i, right(misc[16 * h + i], 8 * i), tags)
        halves.append(tags)
    tags = jnp.concatenate(halves, axis=1)
    products = jnp.concatenate(
        [recv_ref[:, 8 * j : 8 * j + 8, :].reshape(256, LANES) for j in range(3)], axis=1
    )

    at = lax.broadcasted_iota(jnp.int32, (256, 256), 0)
    wanted = ((at // 8) * 4 + at % 4).astype(F32)
    sums = select_sum((wanted == jnp.broadcast_to(tags, (256, 256))).astype(F32), products)
    columns[...] = sums
    low = lax.broadcasted_iota(jnp.int32, (8, LANES), 0) < 4
    quad = jnp.zeros((8, LANES), F32)
    for f in range(32):
        here = sums[8 * f : 8 * f + 8]
        quad = quad + jnp.where(low, here[:, 0:128], here[:, 128:256]) * recv_ref[f, 24:32, :]
        quad = quad + jnp.where(low, here[:, 256:384] * recv_ref[f, 32:40, :], 0.0)
    quad = jnp.sum(quad, axis=0, keepdims=True)
    for f in range(31):
        for j in range(3):
            quad = quad + recv_ref[f, 36 + j : 37 + j, :] * recv_ref[f + 1, 24 + 4 * j : 25 + 4 * j, :]
    quad = quad + quad + jnp.where(lane == 15, total, 0.0)

    mine = columns[pl.ds(pl.multiple_of(frame * 8, 8), 8), :]
    mine_ref[...] = mine + band_ref[...]
    before = jnp.maximum(frame - 1, 0)
    for j in range(3):
        lanes = slice(j * LANES, (j + 1) * LANES)
        edge = recv_ref[before, 36 + j : 37 + j, :] * (frame > 0).astype(F32)
        mine_ref[0:1, lanes] = mine_ref[0:1, lanes] + edge
    here = (col > 0).astype(F32)
    there = ((col == 0) & (frame < 31)).astype(F32)
    after = jnp.minimum(frame + 1, 31)

    def row_of(f, i):
        return jnp.concatenate([recv_ref[f, pl.ds(24 + 4 * j + i, 1), :] for j in range(3)], axis=1)

    onward = onward_terms(edge_ref, row_ref[col][0:1] * here + row_of(after, 0) * there)
    empty = jnp.where(lax.broadcasted_iota(jnp.int32, (16, LANES), 0) == 12, quad, 0.0)
    for c in range(8):
        send_ref[c] = empty
    for j in range(3):
        send_ref[(col + 7) % 8, 4 * j + 3 : 4 * j + 4, :] = onward[:, j * LANES : (j + 1) * LANES]

    def piece_of(s):
        q = cols_ref[0, s]
        return row_of(q // 4, q % 4)

    tile_products((early_ref, late_ref), piece_of, count_ref[0, 0], pack)
    for s in range(8):
        r = rows_ref[0, s]
        for j in range(3):
            send_ref[r // 4, pl.ds(4 * j + r % 4, 1), :] += pack[8 * j + s : 8 * j + s + 1, :]


def end_kernel(
    recv_ref, mine_ref, known_ref, right_ref, v0, v1, v2, v3, w0, w1, w2, solution_ref, residual_ref, scratch
):
    col = lax.axis_index("cols")
    total = recv_ref[0]
    for c in range(1, 8):
        total = total + recv_ref[c]
    parts = [total[0:8], pltpu.roll(total[0:8], 4, 0), total[8:16]]
    last = jnp.concatenate(parts, axis=1) + mine_ref[...]
    known = known_ref[0:1, :]
    mu = [jnp.broadcast_to(known[:, 8 + i : 9 + i], (1, LANES)) for i in range(7)]
    mu.append(jnp.broadcast_to(jnp.sum(total[12:13], axis=1, keepdims=True), (1, LANES)))
    zero = jnp.zeros((1, LANES), F32)
    one = zero + 1.0

    def form(left_side, shift):
        value = zero
        for i in range(len(left_side)):
            for k in range(i, len(left_side)):
                term = left_side[i] * left_side[k]
                value = value + (term if i == k else term + term) * mu[i + k + shift]
        return value

    def ratio(top, bottom):
        return jnp.where(top == 0.0, 0.0, top / jnp.where(top == 0.0, one, bottom))

    direction, residual, solution = [one], [one], []
    gamma = mu[0]
    for it in range(ITERS):
        alpha = ratio(gamma, form(direction, 0) + form(direction, 1))
        solution = solution + [zero] * (len(direction) - len(solution))
        solution = [x + alpha * p for x, p in zip(solution, direction)]
        image = [p + q for p, q in zip(direction + [zero], [zero] + direction)]
        residual = residual + [zero] * (len(image) - len(residual))
        residual = [r - alpha * y for r, y in zip(residual, image)]
        if it + 1 < ITERS:
            fresh = form(residual, 0)
            beta = ratio(fresh, gamma)
            direction = direction + [zero] * (len(residual) - len(direction))
            direction = [r + beta * p for r, p in zip(residual, direction)]
            gamma = fresh

    def wide(x):
        return jnp.concatenate([x, x, x], axis=1)

    total = wide(solution[0]) * v0[col]
    for x, ref in zip(solution[1:], (v1, v2, v3)):
        total = total + wide(x) * ref[col]
    store_as_natural(solution_ref, total)
    total = wide(residual[4]) * last
    for x, ref in zip(residual[1:4], (w0, w1, w2)):
        total = total + wide(x) * ref[...]
    store_as_natural(scratch, total)
    residual_ref[...] = scratch[0:6, :] + jnp.concatenate([residual[0]] * 2, axis=1) * right_ref[...]


VM = pl.BlockSpec(memory_space=pltpu.VMEM)
SM = pl.BlockSpec(memory_space=pltpu.SMEM)
HB = pl.BlockSpec(memory_space=pltpu.HBM)


def shape(*dims, kind=F32):
    return jax.ShapeDtypeStruct(dims, kind)


def call(kernel, specs, outs, scratch, name):
    return pl.pallas_call(
        kernel,
        in_specs=specs,
        out_specs=[VM] * len(outs),
        out_shape=outs,
        scratch_shapes=[pltpu.VMEM(s, F32) if isinstance(s, tuple) else s for s in scratch],
        compiler_params=pltpu.CompilerParams(vmem_limit_bytes=24 * 1024 * 1024),
        name=name,
    )


def per_device(right_side, diag_blocks, band_blocks, reach, tiles, tile_rows, tile_cols, tile_count):
    def exchange(x, axis):
        return lax.all_to_all(x, axis, 0, 0, tiled=True)

    def share(x):
        chips = lax.axis_size("cols") // 2
        swap = [(i, i ^ 1) for i in range(2 * chips)]
        pair = jnp.concatenate([x, lax.ppermute(x, "cols", swap)], axis=0)
        others = []
        for d in range(1, chips):
            ahead = [(i, (i + 2 * d) % (2 * chips)) for i in range(2 * chips)]
            others.append(lax.ppermute(pair, "cols", ahead))
        return [pair, *others]

    def in_hbm(x):
        return pltpu.with_memory_space_constraint(x, pltpu.HBM)

    sem = pltpu.SemaphoreType.DMA(())
    stored = in_hbm(tiles.reshape(tiles.shape[2:]))
    inputs = (right_side, diag_blocks, jnp.transpose(band_blocks, (1, 2, 0, 3)), reach.reshape(1, -1))
    inputs += (tile_rows.reshape(1, 8), tile_cols.reshape(1, 8))
    send, masked, *ids = call(
        start_kernel,
        [HB] * 6,
        [shape(80, LANES), shape(48, 6, 256)]
        + [shape(1, 8, kind=jnp.int32)] * 2,
        [(6, 256), (6, 6, 256), (6, 6, 8, 256), pltpu.VMEM((1, 256), jnp.int32), (8, 384)]
        + [sem] * 6,
        "start",
    )(*[in_hbm(x) for x in inputs])
    ids.append(tile_count)
    recv = shared = share(send)
    early, late = call(
        load_kernel, [HB], [shape(n, 384, 384) for n in (EARLY, 8 - EARLY)], [sem] * 8, "load"
    )(stored)
    frames_out = [shape(32, 8, 384), shape(8, 384), shape(8, 8, 384)]
    scratch = [(LANES, 384), (8, 256), (8, 256), (384, 512)]
    send, band, row, edges = call(
        first_kernel,
        [VM] * 7 + [SM] * 3,
        frames_out + [shape(48, 6, LANES)],
        scratch,
        "first",
    )(*recv, masked, early, late, *ids)
    vectors, images, moments = [row], [], []
    for it in range(ITERS - 1):
        recv = exchange(send, "frames")
        (send,) = call(
            cols_kernel,
            [VM] * 6 + [SM] * 2,
            [shape(40, LANES)],
            [],
            "products",
        )(recv, early, late, row, edges, band, *ids[1:])
        recv = share(send)
        if it == 0:
            pick, inverse, moment = call(
                layout_kernel,
                [VM] * 5,
                [shape(3, 64, 256), shape(6, 8, 8, 384), shape(8, LANES)],
                [],
                "layout",
            )(*shared, send)
            moments.append(moment)
        given = (*recv, row, edges, masked, early, late, *ids)
        specs = [VM] * 9 + [SM] * 3
        if it + 2 < ITERS:
            send, band, row, image, moment = call(
                next_kernel,
                specs + [VM] * 2,
                frames_out + [shape(8, 384), shape(2, 8, LANES)],
                scratch,
                "next",
            )(*given, pick, inverse)
            moments.append(moment)
        else:
            send, band, row, image = call(
                last_kernel,
                specs + [VM] * 5,
                [shape(32, 40, LANES), shape(8, 384), shape(8, 8, 384), shape(8, 384)],
                scratch + [(40, LANES)],
                "last",
            )(*given, pick, inverse, *moments)
        vectors.append(row)
        images.append(image)
    recv = exchange(send, "frames")
    send, known, mine = call(
        finish_kernel,
        [VM] * 6 + [SM] * 3,
        [shape(8, 16, LANES), shape(8, LANES), shape(8, 384)],
        [(24, LANES), (256, 384)],
        "finish",
    )(recv, early, late, row, edges, band, *ids[1:], ids[0])
    recv = exchange(send, "cols")
    return tuple(
        call(end_kernel, [VM] * 11, [shape(6, 256), shape(6, 256)], [(8, 256)], "end")(
            recv, mine, known, right_side, *vectors, *images
        )
    )


def solution(mesh):
    return jax.shard_map(
        per_device,
        mesh=mesh,
        in_specs=(
            P(None, ROWS),
            P(None, None, ROWS),
            P(None, None, None, ROWS),
            P(ROWS),
            P("frames", "cols", None, None, None),
            P("frames", "cols", None),
            P("frames", "cols", None),
            P("frames", "cols"),
        ),
        out_specs=(P(None, ROWS), P(None, ROWS)),
        check_vma=False,
    )
```

```python
import jax
import jax.numpy as jnp
from jax import lax
from jax.experimental import pallas as pl
from jax.experimental.pallas import tpu as pltpu
from jax.sharding import PartitionSpec as P


ITERS = 4
BAND = 8
LANES = 128
F32 = jnp.float32
ROWS = ("frames", "cols")
SPREAD = 6
EARLY = 4


def lane_ids(rows):
    return lax.broadcasted_iota(jnp.int32, (rows, LANES), 1)


def half_turn(x):
    return pltpu.roll(x, 64, 1)


def left(x, by):
    return pltpu.roll(x, (x.shape[1] - by) % x.shape[1], 1) if by % x.shape[1] else x


def right(x, by):
    return pltpu.roll(x, by % x.shape[1], 1) if by % x.shape[1] else x


def store_as_tiles(ref, base, x):
    low = lane_ids(1) < 64
    for u in range(2):
        part = x[:, u * LANES : (u + 1) * LANES]
        turned = half_turn(part)
        for j in range(3):
            lanes = pl.ds(j * LANES, LANES)
            ref[pl.ds(base + 2 * u, 1), lanes] = jnp.where(
                low, part[2 * j : 2 * j + 1], turned[2 * j + 1 : 2 * j + 2]
            )
            ref[pl.ds(base + 2 * u + 1, 1), lanes] = jnp.where(
                low, turned[2 * j : 2 * j + 1], part[2 * j + 1 : 2 * j + 2]
            )


def store_as_natural(ref, t):
    low = lane_ids(1) < 64
    for j in range(3):
        part = t[:, j * LANES : (j + 1) * LANES]
        turned = half_turn(part)
        for u in range(2):
            lanes = pl.ds(u * LANES, LANES)
            ref[pl.ds(2 * j, 1), lanes] = jnp.where(
                low, part[2 * u : 2 * u + 1], turned[2 * u + 1 : 2 * u + 2]
            )
            ref[pl.ds(2 * j + 1, 1), lanes] = jnp.where(
                low, turned[2 * u : 2 * u + 1], part[2 * u + 1 : 2 * u + 2]
            )


def start_kernel(
    right_hbm, diag_hbm, band_hbm, reach_hbm, rows_hbm, cols_hbm,
    send_ref, masked_ref, rows_ref, cols_ref,
    right_ref, diag_ref, band_ref, reach_ref, pack, *sems,
):
    copies = [
        pltpu.make_async_copy(source, to, sem)
        for source, to, sem in zip(
            (diag_hbm, right_hbm, reach_hbm, band_hbm, rows_hbm, cols_hbm),
            (diag_ref, right_ref, reach_ref, band_ref, rows_ref, cols_ref),
            sems,
        )
    ]
    for copy in copies:
        copy.start()
    for copy in copies[:2]:
        copy.wait()
    sub = lax.broadcasted_iota(jnp.int32, (6, 256), 0)
    matrix = [diag_ref[a] for a in range(6)]
    inverse = [(sub == a).astype(F32) for a in range(6)]
    for p in range(6):
        pivot = matrix[p][p : p + 1]
        matrix[p] = matrix[p] / pivot
        inverse[p] = inverse[p] / pivot
        for a in range(6):
            if a != p:
                factor = matrix[a][p : p + 1]
                matrix[a] = matrix[a] - factor * matrix[p]
                inverse[a] = inverse[a] - factor * inverse[p]
    residual = right_ref[...]
    first = jnp.concatenate(
        [jnp.sum(inverse[a] * residual, axis=0, keepdims=True) for a in range(6)], axis=0
    )
    store_as_tiles(pack, 0, first)
    for j in range(3):
        send_ref[4 * j : 4 * j + 4, :] = pack[0:4, j * LANES : (j + 1) * LANES]
    for d in range(4):
        turned = jnp.concatenate(
            [inverse[a][(a + d) % 6 : (a + d) % 6 + 1] for a in range(6)], axis=0
        )
        store_as_tiles(pack, 0, turned)
        for j in range(3):
            at = 32 + (3 * d + j) * 4
            send_ref[at : at + 4, :] = pack[0:4, j * LANES : (j + 1) * LANES]
    product = first * residual
    product = jnp.sum(product[:, 0:LANES] + product[:, LANES:256], axis=0, keepdims=True)
    product = jnp.sum(product, axis=1, keepdims=True)
    moment = jnp.where(lane_ids(1) == 8, product, 0.0)
    for copy in copies[2:6]:
        copy.wait()
    reach = reach_ref[...]
    for o in range(BAND):
        keep = (reach > o).astype(F32)
        for a in range(6):
            masked_ref[o * 6 + a] = band_ref[a, :, o, :] * keep
    ids = lane_ids(6)
    for j in range(3):
        packed = jnp.zeros((6, LANES), F32)
        for i in range(16):
            block = masked_ref[j * 16 + i, :, LANES : 2 * LANES]
            packed = jnp.where(ids // 8 == i, right(block, i * 8 + 8), packed)
        send_ref[12 + 6 * j : 18 + 6 * j, :] = packed
    rows = rows_ref[...]
    send_ref[30:31, :] = moment
    send_ref[30:31, 0:8] = ((rows // 4) * 8 + rows % 4).astype(F32)
    send_ref[31:32, :] = jnp.zeros((1, LANES), F32)


def blocks(refs):
    col = lax.axis_index("cols")
    rows = refs[0].shape[0] // 2
    return [
        (((col // 2 + 4 - d) % 4) * 2 + (col + i) % 2, refs[d], i * rows)
        for d in range(4)
        for i in range(2)
    ]


def load_kernel(tiles_hbm, early_ref, late_ref, *sems):
    copies = [
        pltpu.make_async_copy(tiles_hbm.at[s], slot_of((early_ref, late_ref), s), sems[s])
        for s in range(8)
    ]
    for copy in copies:
        copy.start()
    for copy in copies:
        copy.wait()


def own_edge(edge_ref, row_ref, col):
    last = row_ref[(col + 7) % 8][3:4]
    values = []
    for j in range(3):
        part = last[:, j * LANES : (j + 1) * LANES]
        values += [half_turn(part), part]
    total = jnp.zeros((6, LANES), F32)
    for o in range(BAND):
        z = edge_ref[o * 6] * values[0]
        for a in range(1, 6):
            z = z + edge_ref[o * 6 + a] * values[a]
        total = total + right(z, o + 1)
    total = jnp.where(lane_ids(6) < 8, total, 0.0)
    turned = half_turn(total)
    low = lane_ids(1) < 64
    return jnp.concatenate(
        [jnp.where(low, total[2 * j : 2 * j + 1], turned[2 * j + 1 : 2 * j + 2]) for j in range(3)],
        axis=1,
    )


def bfloat16_parts(x):
    high = x.astype(jnp.bfloat16)
    rest = x - high.astype(F32)
    middle = rest.astype(jnp.bfloat16)
    return high, middle, (rest - middle.astype(F32)).astype(jnp.bfloat16)


def select_sum(pick, x):
    pick = pick.astype(jnp.bfloat16)
    high, middle, low = [
        jnp.dot(pick, part, preferred_element_type=F32) for part in bfloat16_parts(x)
    ]
    return low + middle + high


def slot_of(tiles_refs, s):
    return tiles_refs[0].at[s] if s < EARLY else tiles_refs[1].at[s - EARLY]


def transposed_products(row_ref, tiles_refs, ids_refs, picked, spread):
    rows_ref, _, count_ref = ids_refs
    count = count_ref[0, 0]
    picked[...] = jnp.zeros((LANES, 384), F32)
    for s in range(8):
        r = rows_ref[0, s]
        picked[s : s + 1, :] = row_ref[r // 4, pl.ds(r % 4, 1), :]
    for i, part in enumerate(bfloat16_parts(picked[8 - SPREAD : 8, :])):
        picked[8 + SPREAD * i : 8 + SPREAD * (i + 1), :] = part.astype(F32)
    upright = [picked[:, j * LANES : (j + 1) * LANES].T for j in range(3)]
    at = lax.broadcasted_iota(jnp.int32, (LANES, SPREAD * LANES), 0) - 8
    to = lax.broadcasted_iota(jnp.int32, (LANES, SPREAD * LANES), 1)
    ones = ((at >= 0) & (at < 3 * SPREAD) & (at % SPREAD == to // LANES)).astype(jnp.bfloat16)
    for j in range(3):
        spread[j * LANES : (j + 1) * LANES, :] = jnp.dot(
            upright[j].astype(jnp.bfloat16), ones, preferred_element_type=F32
        )
    products = []
    for s in range(8):
        tile = slot_of(tiles_refs, s)
        sums = [[None] * 3, [None] * 3]
        for i in range(48):
            if s < 8 - SPREAD:
                column = upright[i // 16][8 * (i % 16) : 8 * (i % 16) + 8, s : s + 1]
                column = jnp.broadcast_to(column, (8, LANES))
            else:
                column = spread[8 * i : 8 * i + 8, (s + SPREAD - 8) * LANES : (s + SPREAD - 7) * LANES]
            for j in range(3):
                part = tile[8 * i : 8 * i + 8, j * LANES : (j + 1) * LANES] * column
                before = sums[i % 2][j]
                sums[i % 2][j] = part if before is None else before + part
        total = jnp.concatenate(
            [jnp.sum(x + y, axis=0, keepdims=True) for x, y in zip(*sums)], axis=1
        )
        products.append(total * (s < count).astype(F32))
    return products


def edge_terms(row_ref, edge_ref):
    frame = lax.axis_index("frames")
    col = lax.axis_index("cols")
    edge = own_edge(edge_ref, row_ref, col)
    cross = ((col == 0) & (frame < 31)).astype(F32)
    return edge * (col > 0).astype(F32), edge * cross


def band_terms(row_ref, masked_ref, edge, out_ref, natural, sums):
    col = lax.axis_index("cols")
    store_as_natural(natural, row_ref[col])
    lane = lax.broadcasted_iota(jnp.int32, (6, 256), 1)
    vector = natural[0:6, :]
    total = jnp.zeros((6, 256), F32)
    ahead = [jnp.zeros((6, 256), F32) for _ in range(6)]
    for o in range(BAND):
        shifted = jnp.where(lane < 255 - o, left(vector, o + 1), 0.0)
        z = jnp.zeros((6, 256), F32)
        for a in range(6):
            block = masked_ref[o * 6 + a]
            z = z + block * natural[a : a + 1, :]
            ahead[a] = ahead[a] + block * shifted
        total = total + jnp.where(lane > o, right(z, o + 1), 0.0)
    for a in range(6):
        sums[a : a + 1, :] = jnp.sum(ahead[a], axis=0, keepdims=True)
    out_ref[...] = jnp.zeros((8, 384), F32)
    store_as_tiles(out_ref, 0, total + sums[0:6, :])
    out_ref[0:1, :] = out_ref[0:1, :] + edge


def send_frames(row_ref, edge_ref, masked_ref, tiles_refs, ids_refs, send_ref, band_ref, scratch):
    picked, natural, sums, spread = scratch
    col = lax.axis_index("cols")
    sub = lax.broadcasted_iota(jnp.int32, (8, 384), 0)
    chunk = jnp.where(sub < 4, row_ref[col], 0.0)
    for f in range(32):
        send_ref[f] = chunk
    mine, onward = edge_terms(row_ref, edge_ref)
    send_ref[jnp.minimum(lax.axis_index("frames") + 1, 31), 4:5, :] = onward
    band_terms(row_ref, masked_ref, mine, band_ref, natural, sums)
    for s, product in enumerate(transposed_products(row_ref, tiles_refs, ids_refs, picked, spread)):
        q = ids_refs[1][0, s]
        send_ref[q // 4, pl.ds(4 + q % 4, 1), :] += product


def send_last(row_ref, edge_ref, masked_ref, tiles_refs, ids_refs, known, send_ref, band_ref, scratch):
    picked, natural, sums, spread, pack = scratch
    col = lax.axis_index("cols")
    mine, onward = edge_terms(row_ref, edge_ref)
    band_terms(row_ref, masked_ref, mine, band_ref, natural, sums)
    own = row_ref[col]
    products = transposed_products(row_ref, tiles_refs, ids_refs, picked, spread)
    for j in range(3):
        lanes = slice(j * LANES, (j + 1) * LANES)
        for s in range(8):
            pack[8 * j + s : 8 * j + s + 1, :] = products[s][:, lanes]
        pack[24 + 4 * j : 28 + 4 * j, :] = own[0:4, lanes]
        pack[36 + j : 37 + j, :] = onward[:, lanes]
    part = own * band_ref[...]
    quad = jnp.sum(part[:, 0:128] + part[:, 128:256] + part[:, 256:384], axis=0, keepdims=True)
    part = own[0:1] * mine
    quad = quad + part[:, 0:128] + part[:, 128:256] + part[:, 256:384]
    rows = [jnp.sum(x, axis=0, keepdims=True) for x in known] + [quad]
    lane = lax.broadcasted_iota(jnp.int32, (8, LANES), 1)
    sub = lax.broadcasted_iota(jnp.int32, (8, LANES), 0)
    totals = jnp.sum(jnp.concatenate(rows, axis=0), axis=1, keepdims=True)
    misc = jnp.sum(jnp.where(lane == sub + 8, totals, 0.0), axis=0, keepdims=True)
    for s in range(8):
        misc = jnp.where(lane_ids(1) == s, ids_refs[1][0, s].astype(F32), misc)
    pack[39:40, :] = misc
    whole = pack[...]
    for f in range(32):
        send_ref[f] = whole


def first_kernel(
    recv0, recv1, recv2, recv3, masked_ref, early_ref, late_ref, rows_ref, cols_ref, count_ref,
    send_ref, band_ref, row_ref, edge_ref, *scratch,
):
    col = lax.axis_index("cols")
    row_ref[...] = jnp.zeros((8, 8, 384), F32)
    for c, ref, at in blocks((recv0, recv1, recv2, recv3)):
        for j in range(3):
            row_ref[c, 0:4, j * LANES : (j + 1) * LANES] = ref[at + 4 * j : at + 4 * j + 4, :]
    ids = lane_ids(6)
    for j in range(3):
        at = 80 + 12 + 6 * j
        part = jnp.where(col % 2 == 1, recv0[at : at + 6, :], recv1[at : at + 6, :])
        for i in range(16):
            edge_ref[j * 16 + i] = jnp.where(ids >= 120, right(part, 120 - i * 8), 0.0)
    send_frames(
        row_ref, edge_ref, masked_ref, (early_ref, late_ref), (rows_ref, cols_ref, count_ref),
        send_ref, band_ref, scratch,
    )


def layout_kernel(recv0, recv1, recv2, recv3, _, pick_ref, inverse_ref, moment_ref):
    refs = (recv0, recv1, recv2, recv3)
    total = jnp.zeros((1, LANES), F32)
    lane = lane_ids(1)
    group = lane % 64 // 8
    device = jnp.zeros((1, LANES), jnp.int32)
    target = jnp.zeros((1, LANES), F32)
    low = lax.broadcasted_iota(jnp.int32, (8, LANES), 0) < 4
    for b, (c, ref, at) in enumerate(blocks(refs)):
        device = jnp.where(group == b, c, device)
        target = jnp.where(group == b, right(ref[at + 30 : at + 31, :], 8 * b), target)
        total = total + ref[at + 30 : at + 31, :]
        parts = []
        for g in range(12):
            first = at + 32 + 8 * (g // 2)
            part = ref[first : first + 8, :]
            part = pltpu.roll(part, 4, 0) if g % 2 else part
            parts.append(jnp.where(low, part, 0.0))
        parts = [jnp.concatenate(parts[3 * d : 3 * d + 3], axis=1) for d in range(4)]
        parts += [left(parts[2], 256), left(parts[1], 320)]
        for d in range(6):
            inverse_ref[d, c] = parts[d]
    own = (device * 8 + lane % 4).astype(F32)
    onward = ((device + 7) % 8 * 8 + 3).astype(F32)
    at = lane % 8
    none = jnp.full((1, LANES), -1.0, F32)
    index = lax.broadcasted_iota(jnp.int32, (64, LANES), 0).astype(F32)
    for j in range(3):
        three = jnp.where((at < 4) == (j == 0), own, none) if j < 2 else none
        four = jnp.where(at == 4 + j, onward, jnp.where(at < 4, own, none) if j == 2 else none)
        for half, wanted in enumerate((jnp.where(lane < 64, target, three), jnp.where(lane < 64, four, none))):
            found = (index == jnp.broadcast_to(wanted, (64, LANES))).astype(F32)
            pick_ref[j, :, half * LANES : (half + 1) * LANES] = found
    sub = lax.broadcasted_iota(jnp.int32, (8, LANES), 0)
    total = jnp.where(lane == 8, total, 0.0)
    moment_ref[...] = jnp.where(sub == 0, jnp.broadcast_to(total, (8, LANES)), 0.0)


def row_image(refs, pick_ref):
    places = blocks(refs)

    def rows_from(first):
        return bfloat16_parts(
            jnp.concatenate([ref[at + first : at + first + 8, :] for _, ref, at in places], axis=0)
        )

    three, four = rows_from(24), rows_from(32)
    parts = []
    for j in range(3):
        pick = pick_ref[j, :, 0:192].astype(jnp.bfloat16)
        high, middle, low = [
            jnp.dot(pick, jnp.concatenate(x, axis=0), preferred_element_type=F32)
            for x in zip(rows_from(8 * j), three, four)
        ]
        parts.append(low + middle + high)
    return jnp.concatenate(parts, axis=1).reshape(8, 8, 384)


def folded(x):
    x = jnp.sum(x, axis=0)
    return x[:, 0:128] + x[:, 128:256] + x[:, 256:384]


def advance(refs, pick_ref, inverse_ref, before_ref, row_ref, image_ref, moment_ref, picked):
    col = lax.axis_index("cols")
    image = row_image(refs, pick_ref)
    flat = image.reshape(64, 384)
    vector = inverse_ref[0].reshape(64, 384) * flat
    for d in range(1, 6):
        vector = vector + inverse_ref[d].reshape(64, 384) * left(flat, 64 * d)
    vector = vector.reshape(8, 8, 384)
    row_ref[...] = vector
    moments = [folded(before_ref[...] * image), folded(vector * image)]
    if moment_ref is not None:
        moment_ref[0], moment_ref[1] = moments
    picked[0:64, :] = flat
    image_ref[...] = picked[pl.ds(pl.multiple_of(col * 8, 8), 8), :]
    return moments


def next_kernel(
    recv0, recv1, recv2, recv3, before_ref, edge_ref, masked_ref, early_ref, late_ref, rows_ref, cols_ref, count_ref,
    pick_ref, inverse_ref, send_ref, band_ref, row_ref, image_ref, moment_ref, *scratch,
):
    advance((recv0, recv1, recv2, recv3), pick_ref, inverse_ref, before_ref, row_ref, image_ref, moment_ref, scratch[0])
    ids_refs = (rows_ref, cols_ref, count_ref)
    tiles_refs = (early_ref, late_ref)
    send_frames(row_ref, edge_ref, masked_ref, tiles_refs, ids_refs, send_ref, band_ref, scratch)


def last_kernel(
    recv0, recv1, recv2, recv3, before_ref, edge_ref, masked_ref, early_ref, late_ref, rows_ref, cols_ref, count_ref,
    pick_ref, inverse_ref, m0_ref, m1_ref, m2_ref, send_ref, band_ref, row_ref, image_ref, *scratch,
):
    moments = advance((recv0, recv1, recv2, recv3), pick_ref, inverse_ref, before_ref, row_ref, image_ref, None, scratch[0])
    known = [m0_ref[...], m1_ref[0], m1_ref[1], m2_ref[0], m2_ref[1]] + moments
    ids_refs = (rows_ref, cols_ref, count_ref)
    tiles_refs = (early_ref, late_ref)
    send_last(row_ref, edge_ref, masked_ref, tiles_refs, ids_refs, known, send_ref, band_ref, scratch)


def onward_terms(edge_ref, start):
    parts = []
    for j in range(3):
        part = start[:, j * LANES : (j + 1) * LANES]
        parts += [part, half_turn(part)]
    ids = lane_ids(6)
    begin = jnp.concatenate(parts, axis=0)
    sums = [jnp.zeros((6, LANES), F32) for _ in range(6)]
    for o in range(BAND):
        shifted = jnp.where(ids >= 127 - o, left(begin, o + 1), 0.0)
        for a in range(6):
            sums[a] = sums[a] + edge_ref[o * 6 + a] * shifted
    sums = [jnp.sum(x, axis=0, keepdims=True) for x in sums]
    low = lane_ids(1) < 64
    return jnp.concatenate(
        [jnp.where(low, half_turn(sums[2 * j]), sums[2 * j + 1]) for j in range(3)], axis=1
    )


def tile_products(tiles_refs, piece_of, count, pack):
    for s in range(8):
        piece = piece_of(s) * (s < count).astype(F32)
        for j in range(3):
            rows = pl.ds(j * LANES, LANES)
            tile = slot_of(tiles_refs, s)
            part = tile[rows, 0:LANES] * piece[:, 0:LANES]
            part = part + tile[rows, LANES : 2 * LANES] * piece[:, LANES : 2 * LANES]
            part = part + tile[rows, 2 * LANES : 384] * piece[:, 2 * LANES : 384]
            pack[8 * j + s : 8 * j + s + 1, :] = jnp.sum(part.T, axis=0, keepdims=True)


def cols_kernel(recv_ref, early_ref, late_ref, row_ref, edge_ref, band_ref, cols_ref, count_ref, pack):
    frame = lax.axis_index("frames")
    col = lax.axis_index("cols")
    def piece_of(s):
        q = cols_ref[0, s]
        return recv_ref[q // 4, pl.ds(q % 4, 1), :]

    tile_products((early_ref, late_ref), piece_of, count_ref[0, 0], pack)
    total = recv_ref[0]
    for f in range(1, 32):
        total = total + recv_ref[f]
    terms = pltpu.roll(total, 4, 0) + band_ref[...]
    here = (col > 0).astype(F32)
    there = ((col == 0) & (frame < 31)).astype(F32)
    start = row_ref[col][0:1] * here + recv_ref[jnp.minimum(frame + 1, 31)][0:1] * there
    onward = onward_terms(edge_ref, start)
    for j in range(3):
        lanes = slice(j * LANES, (j + 1) * LANES)
        pack[24 + 4 * j : 28 + 4 * j, :] = terms[0:4, lanes]
        pack[36 + j : 37 + j, :] = onward[:, lanes]
    pack[39:40, :] = jnp.zeros((1, LANES), F32)


def finish_kernel(
    recv_ref, early_ref, late_ref, row_ref, edge_ref, band_ref, cols_ref, count_ref, rows_ref,
    send_ref, known_ref, mine_ref, pack, columns,
):
    frame = lax.axis_index("frames")
    col = lax.axis_index("cols")
    lane = lane_ids(1)
    misc = [recv_ref[f, 39:40, :] for f in range(32)]
    total = misc[0]
    for x in misc[1:]:
        total = total + x
    known_ref[...] = jnp.broadcast_to(total, (8, LANES))
    halves = []
    for h in range(2):
        tags = jnp.zeros((1, LANES), F32)
        for i in range(16):
            tags = jnp.where(lane // 8 == i, right(misc[16 * h + i], 8 * i), tags)
        halves.append(tags)
    tags = jnp.concatenate(halves, axis=1)
    products = jnp.concatenate(
        [recv_ref[:, 8 * j : 8 * j + 8, :].reshape(256, LANES) for j in range(3)], axis=1
    )

    at = lax.broadcasted_iota(jnp.int32, (256, 256), 0)
    wanted = ((at // 8) * 4 + at % 4).astype(F32)
    sums = select_sum((wanted == jnp.broadcast_to(tags, (256, 256))).astype(F32), products)
    columns[...] = sums
    low = lax.broadcasted_iota(jnp.int32, (8, LANES), 0) < 4
    quad = jnp.zeros((8, LANES), F32)
    for f in range(32):
        here = sums[8 * f : 8 * f + 8]
        quad = quad + jnp.where(low, here[:, 0:128], here[:, 128:256]) * recv_ref[f, 24:32, :]
        quad = quad + jnp.where(low, here[:, 256:384] * recv_ref[f, 32:40, :], 0.0)
    quad = jnp.sum(quad, axis=0, keepdims=True)
    for f in range(31):
        for j in range(3):
            quad = quad + recv_ref[f, 36 + j : 37 + j, :] * recv_ref[f + 1, 24 + 4 * j : 25 + 4 * j, :]
    quad = quad + quad + jnp.where(lane == 15, total, 0.0)

    mine = columns[pl.ds(pl.multiple_of(frame * 8, 8), 8), :]
    mine_ref[...] = mine + band_ref[...]
    before = jnp.maximum(frame - 1, 0)
    for j in range(3):
        lanes = slice(j * LANES, (j + 1) * LANES)
        edge = recv_ref[before, 36 + j : 37 + j, :] * (frame > 0).astype(F32)
        mine_ref[0:1, lanes] = mine_ref[0:1, lanes] + edge
    here = (col > 0).astype(F32)
    there = ((col == 0) & (frame < 31)).astype(F32)
    after = jnp.minimum(frame + 1, 31)

    def row_of(f, i):
        return jnp.concatenate([recv_ref[f, pl.ds(24 + 4 * j + i, 1), :] for j in range(3)], axis=1)

    onward = onward_terms(edge_ref, row_ref[col][0:1] * here + row_of(after, 0) * there)
    empty = jnp.where(lax.broadcasted_iota(jnp.int32, (16, LANES), 0) == 12, quad, 0.0)
    for c in range(8):
        send_ref[c] = empty
    for j in range(3):
        send_ref[(col + 7) % 8, 4 * j + 3 : 4 * j + 4, :] = onward[:, j * LANES : (j + 1) * LANES]

    def piece_of(s):
        q = cols_ref[0, s]
        return row_of(q // 4, q % 4)

    tile_products((early_ref, late_ref), piece_of, count_ref[0, 0], pack)
    for s in range(8):
        r = rows_ref[0, s]
        for j in range(3):
            send_ref[r // 4, pl.ds(4 * j + r % 4, 1), :] += pack[8 * j + s : 8 * j + s + 1, :]


def end_kernel(
    recv_ref, mine_ref, known_ref, right_ref, v0, v1, v2, v3, w0, w1, w2, solution_ref, residual_ref, scratch
):
    col = lax.axis_index("cols")
    total = recv_ref[0]
    for c in range(1, 8):
        total = total + recv_ref[c]
    parts = [total[0:8], pltpu.roll(total[0:8], 4, 0), total[8:16]]
    last = jnp.concatenate(parts, axis=1) + mine_ref[...]
    known = known_ref[0:1, :]
    mu = [jnp.broadcast_to(known[:, 8 + i : 9 + i], (1, LANES)) for i in range(7)]
    mu.append(jnp.broadcast_to(jnp.sum(total[12:13], axis=1, keepdims=True), (1, LANES)))
    zero = jnp.zeros((1, LANES), F32)
    one = zero + 1.0

    def form(left_side, shift):
        value = zero
        for i in range(len(left_side)):
            for k in range(i, len(left_side)):
                term = left_side[i] * left_side[k]
                value = value + (term if i == k else term + term) * mu[i + k + shift]
        return value

    def ratio(top, bottom):
        return jnp.where(top == 0.0, 0.0, top / jnp.where(top == 0.0, one, bottom))

    direction, residual, solution = [one], [one], []
    gamma = mu[0]
    for it in range(ITERS):
        alpha = ratio(gamma, form(direction, 0) + form(direction, 1))
        solution = solution + [zero] * (len(direction) - len(solution))
        solution = [x + alpha * p for x, p in zip(solution, direction)]
        image = [p + q for p, q in zip(direction + [zero], [zero] + direction)]
        residual = residual + [zero] * (len(image) - len(residual))
        residual = [r - alpha * y for r, y in zip(residual, image)]
        if it + 1 < ITERS:
            fresh = form(residual, 0)
            beta = ratio(fresh, gamma)
            direction = direction + [zero] * (len(residual) - len(direction))
            direction = [r + beta * p for r, p in zip(residual, direction)]
            gamma = fresh

    def wide(x):
        return jnp.concatenate([x, x, x], axis=1)

    total = wide(solution[0]) * v0[col]
    for x, ref in zip(solution[1:], (v1, v2, v3)):
        total = total + wide(x) * ref[col]
    store_as_natural(solution_ref, total)
    total = wide(residual[4]) * last
    for x, ref in zip(residual[1:4], (w0, w1, w2)):
        total = total + wide(x) * ref[...]
    store_as_natural(scratch, total)
    residual_ref[...] = scratch[0:6, :] + jnp.concatenate([residual[0]] * 2, axis=1) * right_ref[...]


VM = pl.BlockSpec(memory_space=pltpu.VMEM)
SM = pl.BlockSpec(memory_space=pltpu.SMEM)
HB = pl.BlockSpec(memory_space=pltpu.HBM)


def shape(*dims, kind=F32):
    return jax.ShapeDtypeStruct(dims, kind)


def call(kernel, specs, outs, scratch, name):
    return pl.pallas_call(
        kernel,
        in_specs=specs,
        out_specs=[VM] * len(outs),
        out_shape=outs,
        scratch_shapes=[pltpu.VMEM(s, F32) if isinstance(s, tuple) else s for s in scratch],
        compiler_params=pltpu.CompilerParams(vmem_limit_bytes=24 * 1024 * 1024),
        name=name,
    )


def per_device(right_side, diag_blocks, band_blocks, reach, tiles, tile_rows, tile_cols, tile_count):
    def exchange(x, axis):
        return lax.all_to_all(x, axis, 0, 0, tiled=True)

    def share(x):
        chips = lax.axis_size("cols") // 2
        swap = [(i, i ^ 1) for i in range(2 * chips)]
        pair = jnp.concatenate([x, lax.ppermute(x, "cols", swap)], axis=0)
        others = []
        for d in range(1, chips):
            ahead = [(i, (i + 2 * d) % (2 * chips)) for i in range(2 * chips)]
            others.append(lax.ppermute(pair, "cols", ahead))
        return [pair, *others]

    def in_hbm(x):
        return pltpu.with_memory_space_constraint(x, pltpu.HBM)

    sem = pltpu.SemaphoreType.DMA(())
    stored = in_hbm(tiles.reshape(tiles.shape[2:]))
    inputs = (right_side, diag_blocks, jnp.transpose(band_blocks, (1, 2, 0, 3)), reach.reshape(1, -1))
    inputs += (tile_rows.reshape(1, 8), tile_cols.reshape(1, 8))
    send, masked, *ids = call(
        start_kernel,
        [HB] * 6,
        [shape(80, LANES), shape(48, 6, 256)]
        + [shape(1, 8, kind=jnp.int32)] * 2,
        [(6, 256), (6, 6, 256), (6, 6, 8, 256), pltpu.VMEM((1, 256), jnp.int32), (8, 384)]
        + [sem] * 6,
        "start",
    )(*[in_hbm(x) for x in inputs])
    ids.append(tile_count)
    recv = shared = share(send)
    early, late = call(
        load_kernel, [HB], [shape(n, 384, 384) for n in (EARLY, 8 - EARLY)], [sem] * 8, "load"
    )(stored)
    frames_out = [shape(32, 8, 384), shape(8, 384), shape(8, 8, 384)]
    scratch = [(LANES, 384), (8, 256), (8, 256), (384, SPREAD * LANES)]
    send, band, row, edges = call(
        first_kernel,
        [VM] * 7 + [SM] * 3,
        frames_out + [shape(48, 6, LANES)],
        scratch,
        "first",
    )(*recv, masked, early, late, *ids)
    vectors, images, moments = [row], [], []
    for it in range(ITERS - 1):
        recv = exchange(send, "frames")
        (send,) = call(
            cols_kernel,
            [VM] * 6 + [SM] * 2,
            [shape(40, LANES)],
            [],
            "products",
        )(recv, early, late, row, edges, band, *ids[1:])
        recv = share(send)
        if it == 0:
            pick, inverse, moment = call(
                layout_kernel,
                [VM] * 5,
                [shape(3, 64, 256), shape(6, 8, 8, 384), shape(8, LANES)],
                [],
                "layout",
            )(*shared, send)
            moments.append(moment)
        given = (*recv, row, edges, masked, early, late, *ids)
        specs = [VM] * 9 + [SM] * 3
        if it + 2 < ITERS:
            send, band, row, image, moment = call(
                next_kernel,
                specs + [VM] * 2,
                frames_out + [shape(8, 384), shape(2, 8, LANES)],
                scratch,
                "next",
            )(*given, pick, inverse)
            moments.append(moment)
        else:
            send, band, row, image = call(
                last_kernel,
                specs + [VM] * 5,
                [shape(32, 40, LANES), shape(8, 384), shape(8, 8, 384), shape(8, 384)],
                scratch + [(40, LANES)],
                "last",
            )(*given, pick, inverse, *moments)
        vectors.append(row)
        images.append(image)
    recv = exchange(send, "frames")
    send, known, mine = call(
        finish_kernel,
        [VM] * 6 + [SM] * 3,
        [shape(8, 16, LANES), shape(8, LANES), shape(8, 384)],
        [(24, LANES), (256, 384)],
        "finish",
    )(recv, early, late, row, edges, band, *ids[1:], ids[0])
    recv = exchange(send, "cols")
    return tuple(
        call(end_kernel, [VM] * 11, [shape(6, 256), shape(6, 256)], [(8, 256)], "end")(
            recv, mine, known, right_side, *vectors, *images
        )
    )


def solution(mesh):
    return jax.shard_map(
        per_device,
        mesh=mesh,
        in_specs=(
            P(None, ROWS),
            P(None, None, ROWS),
            P(None, None, None, ROWS),
            P(ROWS),
            P("frames", "cols", None, None, None),
            P("frames", "cols", None),
            P("frames", "cols", None),
            P("frames", "cols"),
        ),
        out_specs=(P(None, ROWS), P(None, ROWS)),
        check_vma=False,
    )
```
